16 devices in a mesh: rep: 4 (over y, z, core), dp: 4 (over x).
Axes of the slice: x: 4, y: 2, z: 1, core: 2. Of those that a mesh axis runs over, the one named last changes fastest.
The devices are a block of a 4x4x8 slice.
Arguments:
- x: bfloat16 [16, 4096, 512], P(('rep', 'dp')), parts along dimension 0
- dy: bfloat16 [16, 4096, 512], P(('rep', 'dp')), parts along dimension 0
- w_gate: bfloat16 [2, 512, 2048], replicated
- w_up: bfloat16 [2, 512, 2048], replicated
- w_down: bfloat16 [2, 2048, 512], replicated
- m_w_gate: float32 [2, 512, 2048], replicated
- m_w_up: float32 [2, 512, 2048], replicated
- m_w_down: float32 [2, 2048, 512], replicated
- v_w_gate: float32 [2, 512, 2048], replicated
- v_w_up: float32 [2, 512, 2048], replicated
- v_w_down: float32 [2, 2048, 512], replicated
Outputs:
- output 1: bfloat16 [8, 512, 2048], P('rep'), parts along dimension 0
- output 2: bfloat16 [8, 512, 2048], P('rep'), parts along dimension 0
- output 3: bfloat16 [8, 2048, 512], P('rep'), parts along dimension 0
- output 4: float32 [8, 512, 2048], P('rep'), parts along dimension 0
- output 5: float32 [8, 512, 2048], P('rep'), parts along dimension 0
- output 6: float32 [8, 2048, 512], P('rep'), parts along dimension 0
- output 7: float32 [8, 512, 2048], P('rep'), parts along dimension 0
- output 8: float32 [8, 512, 2048], P('rep'), parts along dimension 0
- output 9: float32 [8, 2048, 512], P('rep'), parts along dimension 0
There are 4 independent parts. The reference program is written for one: setup_inputs(seed, part) draws one part's arguments, and reference() takes and returns one part's arrays. A program takes and returns all parts, laid end to end along the dimension named above; an argument that names none is the same for every part.
All inputs are finite; a program needn't handle non-finite values.
Results may differ from the reference program's by a relative error of at most 0.022.
Values are sent between devices in bfloat16 or wider.
A program may use at most 768 MiB of HBM per device.

```python
import jax
import jax.numpy as jnp
from jax import lax

SEQUENCES = 4
TOKENS = 4096
D = 512
FF = 2048
LAYERS = 2
NAMES = ("w_gate", "w_up", "w_down")
SHAPES = {"w_gate": (LAYERS, D, FF), "w_up": (LAYERS, D, FF), "w_down": (LAYERS, FF, D)}


def bump(key, n, height):
    away = (jnp.arange(n, dtype=jnp.int32) - jax.random.randint(key, (), 0, n, jnp.int32)) % n
    return jnp.where(away < n // 8, height, 1.0)


def together(key, own, strength):
    shared = jax.random.normal(key, own.shape[1:], jnp.float32)
    return (own + strength * shared) * lax.rsqrt(1 + strength * strength)


def setup_inputs(seed: int = 0, part: int = 0) -> dict:
    kx, kdy, ka, kb, kz, kf, kh, kl, *keys = jax.random.split(jax.random.key(seed), 8 + 3 * len(NAMES))
    kx, kdy, ka, kb = (jax.random.fold_in(k, part) for k in (kx, kdy, ka, kb))
    kw, km, kv = (keys[i::3] for i in range(3))
    shape = (SEQUENCES, TOKENS, D)
    much_x, much_dy = jax.random.uniform(kz, (2,), jnp.float32, 0.0, 1.0)
    loud = 2.0 ** jax.random.uniform(jax.random.fold_in(kz, 1), (), jnp.float32, -1.0, 2.0)
    layers = 2.0 ** jax.random.uniform(kl, (LAYERS, 1, 1), jnp.float32, -1.0, 1.0)
    x = together(ka, jax.random.normal(kx, shape, jnp.float32), much_x) * bump(kf, D, 4.0)
    dy = together(kb, jax.random.normal(kdy, shape, jnp.float32), much_dy)
    drawn = {"x": x.astype(jnp.bfloat16), "dy": (loud * dy * (SEQUENCES * TOKENS) ** -0.5).astype(jnp.bfloat16)}
    for key, name in zip(kw, NAMES, strict=True):
        w = jax.random.normal(key, SHAPES[name], jnp.float32) * SHAPES[name][1] ** -0.5
        drawn[name] = (w * {"w_gate": 1.0, "w_up": bump(kh, FF, 4.0), "w_down": layers}[name]).astype(jnp.bfloat16)
    for key, name in zip(km, NAMES, strict=True):
        drawn[f"m_{name}"] = 0.1 * jax.random.normal(key, SHAPES[name], jnp.float32)
    for key, name in zip(kv, NAMES, strict=True):
        drawn[f"v_{name}"] = jax.random.uniform(key, SHAPES[name], jnp.float32, 0.005, 0.015)
    return drawn


def matmul(a, w):
    return jnp.dot(a, w, preferred_element_type=jnp.float32).astype(jnp.bfloat16)


def normed(h):
    wide = h.astype(jnp.float32)
    scale = lax.rsqrt(jnp.mean(wide**2, -1, keepdims=True) + 1e-6)
    return (wide * scale).astype(jnp.bfloat16)


def layer(h, w):
    a = normed(h)
    gate = jnp.dot(a, w["w_gate"], preferred_element_type=jnp.float32)
    up = jnp.dot(a, w["w_up"], preferred_element_type=jnp.float32)
    return h + matmul((jax.nn.silu(gate) * up).astype(jnp.bfloat16), w["w_down"])


def adamw(w, m, v, g):
    m = 0.9 * m + 0.1 * g
    v = 0.95 * v + 0.05 * g * g
    step = m * lax.rsqrt(v + 1e-8) + 0.1 * w
    return (w - 0.02 * step).astype(jnp.bfloat16), m, v


def clipped(gradients, sum_of_squares, count):
    factor = jnp.minimum(1.0, 0.5 * lax.rsqrt(sum_of_squares / count + 1e-30))
    return [g * factor for g in gradients]


def stack(weights, h):
    return lax.scan(lambda h, w: (layer(h, w), None), h, weights)[0]


def reference(x, dy, w_gate, w_up, w_down, m_w_gate, m_w_up, m_w_down, v_w_gate, v_w_up, v_w_down):
    weights = dict(zip(NAMES, (w_gate, w_up, w_down), strict=True))

    def take(so_far, sequence):
        h, by_y = sequence
        _, back = jax.vjp(lambda w: stack(w, h), weights)
        return jax.tree.map(lambda total, term: total + term.astype(jnp.float32), so_far, back(by_y)[0]), None

    none_yet = {name: jnp.zeros(w.shape, jnp.float32) for name, w in weights.items()}
    by_weights, _ = lax.scan(take, none_yet, (x, dy))
    gradients = [by_weights[name].astype(jnp.bfloat16).astype(jnp.float32) for name in NAMES]
    gradients = clipped(gradients, sum(jnp.sum(g * g) for g in gradients), sum(g.size for g in gradients))
    new = [
        adamw(w.astype(jnp.float32), m, v, g)
        for w, m, v, g in zip((w_gate, w_up, w_down), (m_w_gate, m_w_up, m_w_down), (v_w_gate, v_w_up, v_w_down), gradients, strict=True)
    ]
    return tuple(one[which] for which in range(3) for one in new)
```

```python
import functools

import jax
import jax.numpy as jnp
from jax import lax
from jax.experimental import pallas as pl
from jax.experimental.pallas import tpu as pltpu
from jax.sharding import PartitionSpec as P

F32, BF16 = jnp.float32, jnp.bfloat16
CHUNK = 256
TILE = 1024
FTILE = 512
OWN = 4
VMEM_LIMIT = 67_043_328
MESH_ID = pl.DeviceIdType.MESH


def dot(a, b):
    return jnp.dot(a, b, preferred_element_type=F32)


def dot_t(a, b):
    return lax.dot_general(a, b, (((1,), (1,)), ((), ())), preferred_element_type=F32)


def sigmoid(x):
    return 0.5 * jnp.tanh(0.5 * x) + 0.5


def scale_of(wide):
    return lax.rsqrt(jnp.mean(wide * wide, -1, keepdims=True) + 1e-6)


def normed(h):
    wide = h.astype(F32)
    return (wide * scale_of(wide)).astype(BF16)


def forward_kernel(x_ref, wg_ref, wu_ref, wd_ref, h_ref):
    x = x_ref[...]
    a = normed(x)
    ff = wg_ref.shape[2]
    part = 512
    total = None
    for f in range(0, ff, part):
        gate = dot(a, wg_ref[0, :, f : f + part])
        up = dot(a, wu_ref[0, :, f : f + part])
        p = (gate * sigmoid(gate) * up).astype(BF16)
        term = dot(p, wd_ref[0, f : f + part, :])
        total = term if total is None else total + term
    h_ref[...] = (x.astype(F32) + total.astype(BF16).astype(F32)).astype(BF16)


def forward(x, wg, wu, wd):
    tokens, d = x.shape
    ff = wg.shape[2]
    return pl.pallas_call(
        forward_kernel,
        grid=(tokens // FTILE,),
        out_shape=jax.ShapeDtypeStruct((tokens, d), BF16),
        in_specs=[
            pl.BlockSpec((FTILE, d), lambda i: (i, 0)),
            pl.BlockSpec((1, d, ff), lambda i: (0, 0, 0)),
            pl.BlockSpec((1, d, ff), lambda i: (0, 0, 0)),
            pl.BlockSpec((1, ff, d), lambda i: (0, 0, 0)),
        ],
        out_specs=pl.BlockSpec((FTILE, d), lambda i: (i, 0)),
        compiler_params=pltpu.CompilerParams(vmem_limit_bytes=VMEM_LIMIT),
        cost_estimate=pl.CostEstimate(flops=6 * tokens * d * ff, bytes_accessed=4 * tokens * d + 6 * d * ff, transcendentals=tokens * ff),
        name="forward",
    )(x, wg, wu, wd)


def train_kernel(n, h_hbm, x_hbm, dy_hbm, wg_hbm, wu_hbm, wd_hbm, g_out, sa_out, sb_out, ss_out,
                 h_v, a_v, at_v, dy_v, dyt_v, da_v, w_v, wd_v, gu_v, gd_v, own_v, all_v, left_v, ss_v, ssall_v,
                 in_sem, w_sem, send_sem, recv_sem, out_sem, ss_send, ss_recv):
    tokens, d = h_v.shape
    chunks = wg_hbm.shape[2] // CHUNK
    total = 2 * chunks
    rows = own_v.shape[1]
    shard, half = rows // n, rows // n // 2
    pr, pd = d // n, CHUNK // n
    me = lax.axis_index("dp")
    right, left, opposite = lax.rem(me + 1, n), lax.rem(me + n - 1, n), lax.rem(me + 2, n)

    barrier = pltpu.get_barrier_semaphore()
    for peer in (left, right, opposite):
        pl.semaphore_signal(barrier, inc=1, device_id={"dp": peer}, device_id_type=MESH_ID)
    pl.semaphore_wait(barrier, 3)

    def part(j, which=None):
        if which is None:
            return pl.ds(pl.multiple_of(j * shard, half), shard)
        return pl.ds(pl.multiple_of(j * shard + which * half, half), half)

    def weights(k):
        layer, c, slot = 1 - k // chunks, lax.rem(k, chunks), lax.rem(k, 2)
        cols = pl.ds(pl.multiple_of(c * CHUNK, CHUNK), CHUNK)
        return (
            pltpu.make_async_copy(wg_hbm.at[layer, :, cols], w_v.at[slot, :, pl.ds(0, CHUNK)], w_sem.at[slot, 0]),
            pltpu.make_async_copy(wu_hbm.at[layer, :, cols], w_v.at[slot, :, pl.ds(CHUNK, CHUNK)], w_sem.at[slot, 1]),
            pltpu.make_async_copy(wd_hbm.at[layer, cols, :], wd_v.at[slot], w_sem.at[slot, 2]),
        )

    def remote(kind, way, k, src, dst):
        return pltpu.make_async_remote_copy(
            src_ref=src, dst_ref=dst, send_sem=send_sem.at[kind, way, k], recv_sem=recv_sem.at[kind, way, k],
            device_id={"dp": (left, right)[way]}, device_id_type=MESH_ID,
        )

    def first(way, k):
        where = part(opposite, way)
        return remote(0, way, k, own_v.at[lax.rem(k, OWN), where], all_v.at[k, where])

    def second(way, k):
        where = part((left, right)[way])
        return remote(1, way, k, own_v.at[lax.rem(k, OWN), where], all_v.at[k, where] if way == 0 else left_v.at[k])

    def third(way, k):
        return remote(2, way, k, all_v.at[k, part(me)], all_v.at[k, part(me)])

    def fourth(way, k):
        where = part((right, left)[way], way)
        return remote(3, way, k, all_v.at[k, where], all_v.at[k, where])

    def out(k):
        return pltpu.make_async_copy(all_v.at[k], g_out.at[k], out_sem.at[0, k])

    def out_shard(k, which):
        return pltpu.make_async_copy(all_v.at[k, part(me, which)], (sa_out, sb_out)[which].at[k - chunks], out_sem.at[which, k])

    def gathered(k):
        return (k >= 0) & (k < chunks)

    def alive(k):
        return (k >= 0) & (k < total)

    def exchange(k):
        @pl.when(alive(k - 1))
        def _():
            q, slot = k - 1, lax.rem(k - 1 + OWN, OWN)
            for way in range(2):
                first(way, q).wait_recv()
            for j, which in ((left, 0), (right, 1)):
                where = part(j, which)
                own_v[slot, where, :] = (own_v[slot, where, :].astype(F32) + all_v[q, where, :].astype(F32)).astype(BF16)

        @pl.when(alive(k))
        def _():
            for way in range(2):
                first(way, k).start()

        @pl.when(alive(k - 2))
        def _():
            q, slot = k - 2, lax.rem(k - 2 + OWN, OWN)
            for way in range(2):
                second(way, q).wait_recv()
            mine = part(me)
            g = own_v[slot, mine, :].astype(F32) + all_v[q, mine, :].astype(F32) + left_v[q].astype(F32)
            g = g.astype(BF16)
            all_v[q, mine, :] = g
            wide = g.astype(F32)
            ss_v[...] += jnp.sum((wide * wide).reshape(shard // 8, 8, CHUNK), 0)

        @pl.when(alive(k - 1))
        def _():
            for way in range(2):
                second(way, k - 1).start()

        @pl.when(gathered(k - 4))
        def _():
            for way in range(2):
                third(way, k - 4).wait_recv()
            for way in range(2):
                fourth(way, k - 4).start()

        @pl.when(gathered(k - 2))
        def _():
            for way in range(2):
                third(way, k - 2).start()

        @pl.when(alive(k - 2) & (k - 2 >= chunks))
        def _():
            for which in range(2):
                out_shard(k - 2, which).start()

        @pl.when(alive(k - 3))
        def _():
            for way in range(2):
                first(way, k - 3).wait_send()
                second(way, k - 3).wait_send()

        @pl.when(gathered(k - 6))
        def _():
            for way in range(2):
                third(way, k - 6).wait_send()
                fourth(way, k - 6).wait_send()
                fourth(way, k - 6).wait_recv()
            out(k - 6).start()

    def chunk(k, last_layer):
        slot = lax.rem(k, 2)

        @pl.when(k + 1 < total)
        def _():
            for copy in weights(k + 1):
                copy.start()

        for copy in weights(k):
            copy.wait()
        gu_v[...] = jnp.zeros_like(gu_v)
        gd_v[...] = jnp.zeros_like(gd_v)

        def tile(t, _):
            where = pl.ds(pl.multiple_of(t * TILE, TILE), TILE)
            w = w_v[slot]
            both = dot(a_v[where, :], w)
            dp = dot_t(dy_v[where, :], wd_v[slot]).astype(BF16).astype(F32)
            gate, up = both[:, :CHUNK], both[:, CHUNK:]
            s = sigmoid(gate)
            act = gate * s
            p = (act * up).astype(BF16)
            gd_v[...] += dot(dyt_v[:, where], p)
            dgate = (dp * up * (s + act * (1.0 - s))).astype(BF16)
            dup = (dp * act).astype(BF16)
            dboth = jnp.concatenate([dgate, dup], 1)
            gu_v[...] += dot(at_v[:, where], dboth)
            if last_layer:
                da_v[where, :] += dot_t(dboth, w)
            return 0

        lax.fori_loop(0, tokens // TILE, tile, 0)
        o = lax.rem(k, OWN)
        down = gd_v[...].T
        for j in range(n):
            own_v[o, j * shard : j * shard + pr, :] = gu_v[j * pr : (j + 1) * pr, :CHUNK].astype(BF16)
            own_v[o, j * shard + pr : j * shard + 2 * pr, :] = gu_v[j * pr : (j + 1) * pr, CHUNK:].astype(BF16)
            for i in range(d // CHUNK):
                at = j * shard + 2 * pr + i * pd
                own_v[o, at : at + pd, :] = down[j * pd : (j + 1) * pd, i * CHUNK : (i + 1) * CHUNK].astype(BF16)
        exchange(k)
        return 0

    loads = (
        pltpu.make_async_copy(h_hbm, h_v, in_sem.at[0]),
        pltpu.make_async_copy(dy_hbm, dy_v, in_sem.at[1]),
    )
    for copy in loads:
        copy.start()
    for copy in weights(0):
        copy.start()
    ss_v[...] = jnp.zeros_like(ss_v)
    for copy in loads:
        copy.wait()

    def prepare(t, _):
        where = pl.ds(pl.multiple_of(t * FTILE, FTILE), FTILE)
        a = normed(h_v[where, :])
        a_v[where, :] = a
        at_v[:, where] = a.T
        dyt_v[:, where] = dy_v[where, :].T
        da_v[where, :] = jnp.zeros((FTILE, d), F32)
        return 0

    lax.fori_loop(0, tokens // FTILE, prepare, 0)
    lax.fori_loop(0, chunks, lambda k, _: chunk(k, True), 0)

    load = pltpu.make_async_copy(x_hbm, a_v, in_sem.at[2])
    load.start()

    def through_norm(t, _):
        where = pl.ds(pl.multiple_of(t * FTILE, FTILE), FTILE)
        wide = h_v[where, :].astype(F32)
        scale = scale_of(wide)
        g = da_v[where, :].astype(BF16).astype(F32)
        along = jnp.sum(g * wide, -1, keepdims=True)
        dh = (scale * g - wide * (scale * scale * scale * along * (1.0 / d))).astype(BF16)
        dy = (dy_v[where, :].astype(F32) + dh.astype(F32)).astype(BF16)
        dy_v[where, :] = dy
        dyt_v[:, where] = dy.T
        return 0

    lax.fori_loop(0, tokens // FTILE, through_norm, 0)
    load.wait()

    def prepare_first(t, _):
        where = pl.ds(pl.multiple_of(t * FTILE, FTILE), FTILE)
        a = normed(a_v[where, :])
        a_v[where, :] = a
        at_v[:, where] = a.T
        return 0

    lax.fori_loop(0, tokens // FTILE, prepare_first, 0)
    lax.fori_loop(chunks, total, lambda k, _: chunk(k, False), 0)

    def drain(k, _):
        exchange(k)
        return 0

    lax.fori_loop(total, total + 4, drain, 0)

    ssall_v[me] = ss_v[...]

    def squares(i, peer):
        return pltpu.make_async_remote_copy(
            src_ref=ss_v, dst_ref=ssall_v.at[me], send_sem=ss_send.at[i], recv_sem=ss_recv.at[i],
            device_id={"dp": peer}, device_id_type=MESH_ID,
        )

    sends = [squares(i, peer) for i, peer in enumerate((right, left, opposite))]
    for copy in sends:
        copy.start()

    def finish(k, _):
        out(k).wait()
        for which in range(2):
            out_shard(k + chunks, which).wait()
        return 0

    lax.fori_loop(0, chunks, finish, 0)
    for copy in sends:
        copy.wait()
    squares_sum = ssall_v[0]
    for j in range(1, n):
        squares_sum = squares_sum + ssall_v[j]
    ss_out[...] = squares_sum


def train(n, h, x, dy, wg, wu, wd):
    tokens, d = x.shape
    ff = wg.shape[2]
    chunks = ff // CHUNK
    rows = 3 * d
    anywhere = pl.BlockSpec(memory_space=pl.ANY)
    dma = pltpu.SemaphoreType.DMA
    return pl.pallas_call(
        functools.partial(train_kernel, n),
        out_shape=(
            jax.ShapeDtypeStruct((chunks, rows, CHUNK), BF16),
            jax.ShapeDtypeStruct((chunks, rows // n // 2, CHUNK), BF16),
            jax.ShapeDtypeStruct((chunks, rows // n // 2, CHUNK), BF16),
            jax.ShapeDtypeStruct((8, CHUNK), F32),
        ),
        in_specs=[anywhere] * 6,
        out_specs=(anywhere, anywhere, anywhere, pl.BlockSpec(memory_space=pltpu.VMEM)),
        scratch_shapes=[
            pltpu.VMEM((tokens, d), BF16),
            pltpu.VMEM((tokens, d), BF16),
            pltpu.VMEM((d, tokens), BF16),
            pltpu.VMEM((tokens, d), BF16),
            pltpu.VMEM((d, tokens), BF16),
            pltpu.VMEM((tokens, d), F32),
            pltpu.VMEM((2, d, 2 * CHUNK), BF16),
            pltpu.VMEM((2, CHUNK, d), BF16),
            pltpu.VMEM((d, 2 * CHUNK), F32),
            pltpu.VMEM((d, CHUNK), F32),
            pltpu.VMEM((OWN, rows, CHUNK), BF16),
            pltpu.VMEM((2 * chunks, rows, CHUNK), BF16),
            pltpu.VMEM((2 * chunks, rows // n, CHUNK), BF16),
            pltpu.VMEM((8, CHUNK), F32),
            pltpu.VMEM((n, 8, CHUNK), F32),
            dma((3,)),
            dma((2, 3)),
            dma((4, 2, 2 * chunks)),
            dma((4, 2, 2 * chunks)),
            dma((2, 2 * chunks)),
            dma((3,)),
            dma((3,)),
        ],
        compiler_params=pltpu.CompilerParams(collective_id=0, has_side_effects=True, vmem_limit_bytes=VMEM_LIMIT),
        cost_estimate=pl.CostEstimate(flops=28 * tokens * d * ff, bytes_accessed=12 * tokens * d + 24 * d * ff, transcendentals=2 * tokens * ff),
        name="train",
    )(h, x, dy, wg, wu, wd)


def update_kernel(split, count, first, j_ref, ss_ref, *refs):
    g_refs, refs = (refs[:2], refs[2:]) if split else (refs[:1], refs[1:])
    w_refs, m_refs, v_refs = refs[:3], refs[3:6], refs[6:9]
    outs = refs[9:] if first else refs[18:]
    factor = jnp.minimum(1.0, 0.5 * lax.rsqrt(jnp.sum(ss_ref[...], keepdims=True) / count + 1e-30))
    block = g_refs[0].shape[0]
    pr = w_refs[0].shape[1]
    pd = w_refs[2].shape[3]

    def g_rows(i, lo, hi):
        if not split:
            return g_refs[0][i, lo:hi, :]
        half = g_refs[0].shape[1]
        if hi <= half:
            return g_refs[0][i, lo:hi, :]
        if lo >= half:
            return g_refs[1][i, lo - half : hi - half, :]
        return jnp.concatenate([g_refs[0][i, lo:half, :], g_refs[1][i, 0 : hi - half, :]], 0)

    def step(which, at, g):
        g = g.astype(F32) * factor
        m = 0.9 * m_refs[which][at] + 0.1 * g
        v = 0.95 * v_refs[which][at] + 0.05 * g * g
        w = w_refs[which][at].astype(F32)
        outs[which][at] = (w - 0.02 * (m * lax.rsqrt(v + 1e-8) + 0.1 * w)).astype(BF16)
        outs[3 + which][at] = m
        outs[6 + which][at] = v

    for i in range(block):
        cols = slice(i * CHUNK, (i + 1) * CHUNK)
        for which in range(2):
            step(which, (0, slice(None), cols), g_rows(i, which * pr, (which + 1) * pr))
        for h in range(w_refs[2].shape[4] // CHUNK):
            at = (0, i, 0, slice(None), slice(h * CHUNK, (h + 1) * CHUNK))
            step(2, at, g_rows(i, 2 * pr + h * pd, 2 * pr + (h + 1) * pd))


def update(n, layer, j, ss, gs, arrays, outs, block):
    chunks = gs[0].shape[0]
    d, ff = arrays[0].shape[1:]
    split, first = j is not None, outs is None
    pr, pd = d // n, CHUNK // n
    count = sum(a.size for a in arrays[:3])
    if split:
        grid = (chunks // block,)
        g_specs = [pl.BlockSpec((block,) + gs[0].shape[1:], lambda c, j: (c, 0, 0))] * 2
        side = pl.BlockSpec((1, pr, block * CHUNK), lambda c, j: (layer, j[0], c))
        down = pl.BlockSpec((1, block, 1, pd, d), lambda c, j: (layer, c, j[0], 0, 0))
        whole = pl.BlockSpec(ss.shape, lambda c, j: (0, 0))
    else:
        grid = (chunks // block, n)
        g_specs = [pl.BlockSpec((block, gs[0].shape[1] // n, CHUNK), lambda c, s, j: (c, s, 0))]
        side = pl.BlockSpec((1, pr, block * CHUNK), lambda c, s, j: (layer, s, c))
        down = pl.BlockSpec((1, block, 1, pd, d), lambda c, s, j: (layer, c, s, 0, 0))
        whole = pl.BlockSpec(ss.shape, lambda c, s, j: (0, 0))
        j = jnp.zeros((1,), jnp.int32)
    specs = [side, side, down] * 3
    size = d * ff // (n if split else 1)
    operands = [j, ss, *gs, *arrays] + ([] if first else list(outs))
    return pl.pallas_call(
        functools.partial(update_kernel, split, count, first),
        out_shape=tuple(jax.ShapeDtypeStruct(a.shape, a.dtype) for a in arrays),
        grid_spec=pltpu.PrefetchScalarGridSpec(
            num_scalar_prefetch=1,
            grid=grid,
            in_specs=[whole, *g_specs, *specs] + ([] if first else [pl.BlockSpec(memory_space=pl.ANY)] * 9),
            out_specs=tuple(specs),
        ),
        input_output_aliases={} if first else {2 + len(gs) + 9 + i: i for i in range(9)},
        compiler_params=pltpu.CompilerParams(vmem_limit_bytes=VMEM_LIMIT),
        cost_estimate=pl.CostEstimate(flops=45 * size, bytes_accessed=66 * size, transcendentals=3 * size),
        name="update",
    )(*operands)


def solution(mesh):
    n = mesh.shape["dp"]
    assert n == 4

    def step(x, dy, *arrays):
        x, dy = x.reshape(x.shape[1:]), dy.reshape(dy.shape[1:])
        wg, wu, wd = arrays[:3]
        h = forward(x, wg, wu, wd)
        gathered, half_a, half_b, ss = train(n, h, x, dy, wg, wu, wd)

        to_right = [(i, (i + 1) % n) for i in range(n)]
        to_left = [(i, (i + n - 1) % n) for i in range(n)]
        left_b = lax.ppermute(half_b, "dp", to_right)
        right_a = lax.ppermute(half_a, "dp", to_left)
        left_a = lax.ppermute(half_a, "dp", to_right)
        right_b = lax.ppermute(half_b, "dp", to_left)

        layers, ff, d = wd.shape
        cut = (layers, ff // CHUNK, n, CHUNK // n, d)
        views = [a.reshape(cut) if i % 3 == 2 else a for i, a in enumerate(arrays)]
        me = lax.axis_index("dp").astype(jnp.int32)

        def shard(by):
            return lax.rem(me + by, n).reshape(1)

        outs = update(n, 1, None, ss, (gathered,), views, None, 4)
        left_b, right_a, outs = lax.optimization_barrier((left_b, right_a, outs))
        far_b = lax.ppermute(left_b, "dp", to_right)
        far_a = lax.ppermute(right_a, "dp", to_left)
        outs = update(n, 0, shard(0), ss, (half_a, half_b), views, outs, 2)
        outs = update(n, 0, shard(n - 1), ss, (left_a, left_b), views, outs, 2)
        outs = update(n, 0, shard(1), ss, (right_a, right_b), views, outs, 2)
        outs = update(n, 0, shard(2), ss, (far_a, far_b), views, outs, 2)
        return tuple(o.reshape(a.shape) for o, a in zip(outs, arrays, strict=True))

    return jax.shard_map(
        step,
        mesh=mesh,
        in_specs=(P(("rep", "dp"), None, None),) * 2 + (P(None, None, None),) * 9,
        out_specs=(P("rep", None, None),) * 9,
        check_vma=False,
    )
```

```python
import functools

import jax
import jax.numpy as jnp
from jax import lax
from jax.experimental import pallas as pl
from jax.experimental.pallas import tpu as pltpu
from jax.sharding import PartitionSpec as P

F32, BF16 = jnp.float32, jnp.bfloat16
CHUNK = 256
TILE = 1024
FTILE = 512
OWN = 4
VMEM_LIMIT = 67_043_328
MESH_ID = pl.DeviceIdType.MESH


def dot(a, b):
    return jnp.dot(a, b, preferred_element_type=F32)


def dot_t(a, b):
    return lax.dot_general(a, b, (((1,), (1,)), ((), ())), preferred_element_type=F32)


def sigmoid(x):
    return 0.5 * jnp.tanh(0.5 * x) + 0.5


def scale_of(wide):
    return lax.rsqrt(jnp.mean(wide * wide, -1, keepdims=True) + 1e-6)


def normed(h):
    wide = h.astype(F32)
    return (wide * scale_of(wide)).astype(BF16)


def forward_kernel(x_ref, wg_ref, wu_ref, wd_ref, h_ref):
    x = x_ref[...]
    a = normed(x)
    ff = wg_ref.shape[2]
    part = 512
    total = None
    for f in range(0, ff, part):
        gate = dot(a, wg_ref[0, :, f : f + part])
        up = dot(a, wu_ref[0, :, f : f + part])
        p = (gate * sigmoid(gate) * up).astype(BF16)
        term = dot(p, wd_ref[0, f : f + part, :])
        total = term if total is None else total + term
    h_ref[...] = (x.astype(F32) + total.astype(BF16).astype(F32)).astype(BF16)


def forward(x, wg, wu, wd):
    tokens, d = x.shape
    ff = wg.shape[2]
    return pl.pallas_call(
        forward_kernel,
        grid=(tokens // FTILE,),
        out_shape=jax.ShapeDtypeStruct((tokens, d), BF16),
        in_specs=[
            pl.BlockSpec((FTILE, d), lambda i: (i, 0)),
            pl.BlockSpec((1, d, ff), lambda i: (0, 0, 0)),
            pl.BlockSpec((1, d, ff), lambda i: (0, 0, 0)),
            pl.BlockSpec((1, ff, d), lambda i: (0, 0, 0)),
        ],
        out_specs=pl.BlockSpec((FTILE, d), lambda i: (i, 0)),
        compiler_params=pltpu.CompilerParams(vmem_limit_bytes=VMEM_LIMIT),
        cost_estimate=pl.CostEstimate(flops=6 * tokens * d * ff, bytes_accessed=4 * tokens * d + 6 * d * ff, transcendentals=tokens * ff),
        name="forward",
    )(x, wg, wu, wd)


def train_kernel(n, h_hbm, x_hbm, dy_hbm, wg_hbm, wu_hbm, wd_hbm, g_out, sa_out, sb_out, ss_out,
                 h_v, a_v, at_v, dy_v, dyt_v, da_v, w_v, wd_v, gu_v, gd_v, own_v, all_v, left_v, ss_v, ssall_v,
                 in_sem, w_sem, send_sem, recv_sem, out_sem, ss_send, ss_recv):
    tokens, d = h_v.shape
    chunks = wg_hbm.shape[2] // CHUNK
    total = 2 * chunks
    rows = own_v.shape[1]
    shard, half = rows // n, rows // n // 2
    pr, pd = d // n, CHUNK // n
    me = lax.axis_index("dp")
    right, left, opposite = lax.rem(me + 1, n), lax.rem(me + n - 1, n), lax.rem(me + 2, n)

    barrier = pltpu.get_barrier_semaphore()
    for peer in (left, right, opposite):
        pl.semaphore_signal(barrier, inc=1, device_id={"dp": peer}, device_id_type=MESH_ID)
    pl.semaphore_wait(barrier, 3)

    def part(j, which=None):
        if which is None:
            return pl.ds(pl.multiple_of(j * shard, half), shard)
        return pl.ds(pl.multiple_of(j * shard + which * half, half), half)

    def weights(k):
        layer, c, slot = 1 - k // chunks, lax.rem(k, chunks), lax.rem(k, 2)
        cols = pl.ds(pl.multiple_of(c * CHUNK, CHUNK), CHUNK)
        return (
            pltpu.make_async_copy(wg_hbm.at[layer, :, cols], w_v.at[slot, :, pl.ds(0, CHUNK)], w_sem.at[slot, 0]),
            pltpu.make_async_copy(wu_hbm.at[layer, :, cols], w_v.at[slot, :, pl.ds(CHUNK, CHUNK)], w_sem.at[slot, 1]),
            pltpu.make_async_copy(wd_hbm.at[layer, cols, :], wd_v.at[slot], w_sem.at[slot, 2]),
        )

    def remote(kind, way, k, src, dst):
        return pltpu.make_async_remote_copy(
            src_ref=src, dst_ref=dst, send_sem=send_sem.at[kind, way, k], recv_sem=recv_sem.at[kind, way, k],
            device_id={"dp": (left, right)[way]}, device_id_type=MESH_ID,
        )

    def first(way, k):
        where = part(opposite, way)
        return remote(0, way, k, own_v.at[lax.rem(k, OWN), where], all_v.at[k, where])

    def second(way, k):
        where = part((left, right)[way])
        return remote(1, way, k, own_v.at[lax.rem(k, OWN), where], all_v.at[k, where] if way == 0 else left_v.at[k])

    def third(way, k):
        return remote(2, way, k, all_v.at[k, part(me)], all_v.at[k, part(me)])

    def fourth(way, k):
        where = part((right, left)[way], way)
        return remote(3, way, k, all_v.at[k, where], all_v.at[k, where])

    def out(k):
        return pltpu.make_async_copy(all_v.at[k], g_out.at[k], out_sem.at[0, k])

    def out_mine(k):
        return pltpu.make_async_copy(all_v.at[k, part(me)], g_out.at[k, part(me)], out_sem.at[0, k])

    def out_shard(k, which):
        return pltpu.make_async_copy(all_v.at[k, part(me, which)], (sa_out, sb_out)[which].at[k - chunks], out_sem.at[1 + which, k])

    def chunk_at(i):
        return jnp.where(i > chunks, i - 1, i)

    def alive(i):
        return (i >= 0) & (i <= total) & (i != chunks)

    def gather_at(i):
        i = i - 2
        k = 2 * (i // 3) + lax.rem(jnp.maximum(i, 0), 3) // 2
        return k, (i >= 0) & (lax.rem(jnp.maximum(i, 0), 3) != 1) & (k < chunks)

    def exchange(i):
        @pl.when(alive(i - 1))
        def _():
            q = chunk_at(i - 1)
            slot = lax.rem(q, OWN)
            for way in range(2):
                first(way, q).wait_recv()
            for j, which in ((left, 0), (right, 1)):
                where = part(j, which)
                own_v[slot, where, :] = (own_v[slot, where, :].astype(F32) + all_v[q, where, :].astype(F32)).astype(BF16)

        @pl.when(alive(i))
        def _():
            for way in range(2):
                first(way, chunk_at(i)).start()

        @pl.when(alive(i - 2))
        def _():
            q = chunk_at(i - 2)
            slot = lax.rem(q, OWN)
            for way in range(2):
                second(way, q).wait_recv()
            mine = part(me)
            g = own_v[slot, mine, :].astype(F32) + all_v[q, mine, :].astype(F32) + left_v[q].astype(F32)
            g = g.astype(BF16)
            all_v[q, mine, :] = g
            wide = g.astype(F32)
            ss_v[...] += jnp.sum((wide * wide).reshape(shard // 8, 8, CHUNK), 0)

        @pl.when(alive(i - 1))
        def _():
            for way in range(2):
                second(way, chunk_at(i - 1)).start()

        g2, go2 = gather_at(i - 1)

        @pl.when(go2)
        def _():
            for way in range(2):
                third(way, g2).wait_recv()
            for way in range(2):
                fourth(way, g2).start()

        g1, go1 = gather_at(i)

        @pl.when(go1)
        def _():
            for way in range(2):
                third(way, g1).start()

        @pl.when(alive(i - 2) & (chunk_at(i - 2) >= chunks))
        def _():
            q = chunk_at(i - 2)
            for which in range(2):
                out_shard(q, which).start()
            out_mine(q).start()

        @pl.when(alive(i - 3))
        def _():
            for way in range(2):
                first(way, chunk_at(i - 3)).wait_send()
                second(way, chunk_at(i - 3)).wait_send()

        g3, go3 = gather_at(i - 3)

        @pl.when(go3)
        def _():
            for way in range(2):
                third(way, g3).wait_send()
                fourth(way, g3).wait_send()
                fourth(way, g3).wait_recv()
            out(g3).start()

    def chunk(i, last_layer):
        k = i if last_layer else i - 1
        slot = lax.rem(k, 2)

        @pl.when(k + 1 < total)
        def _():
            for copy in weights(k + 1):
                copy.start()

        for copy in weights(k):
            copy.wait()
        gu_v[...] = jnp.zeros_like(gu_v)
        gd_v[...] = jnp.zeros_like(gd_v)

        def tile(t, _):
            where = pl.ds(pl.multiple_of(t * TILE, TILE), TILE)
            w = w_v[slot]
            both = dot(a_v[where, :], w)
            dp = dot_t(dy_v[where, :], wd_v[slot]).astype(BF16).astype(F32)
            gate, up = both[:, :CHUNK], both[:, CHUNK:]
            s = sigmoid(gate)
            act = gate * s
            p = (act * up).astype(BF16)
            gd_v[...] += dot(dyt_v[:, where], p)
            dgate = (dp * up * (s + act * (1.0 - s))).astype(BF16)
            dup = (dp * act).astype(BF16)
            dboth = jnp.concatenate([dgate, dup], 1)
            gu_v[...] += dot(at_v[:, where], dboth)
            if last_layer:
                da_v[where, :] += dot_t(dboth, w)
            return 0

        lax.fori_loop(0, tokens // TILE, tile, 0)
        o = lax.rem(k, OWN)
        down = gd_v[...].T
        for j in range(n):
            own_v[o, j * shard : j * shard + pr, :] = gu_v[j * pr : (j + 1) * pr, :CHUNK].astype(BF16)
            own_v[o, j * shard + pr : j * shard + 2 * pr, :] = gu_v[j * pr : (j + 1) * pr, CHUNK:].astype(BF16)
            for b in range(d // CHUNK):
                at = j * shard + 2 * pr + b * pd
                own_v[o, at : at + pd, :] = down[j * pd : (j + 1) * pd, b * CHUNK : (b + 1) * CHUNK].astype(BF16)
        exchange(i)
        return 0

    def drain(i, _):
        exchange(i)
        return 0

    loads = (
        pltpu.make_async_copy(h_hbm, h_v, in_sem.at[0]),
        pltpu.make_async_copy(dy_hbm, dy_v, in_sem.at[1]),
    )
    for copy in loads:
        copy.start()
    for copy in weights(0):
        copy.start()
    ss_v[...] = jnp.zeros_like(ss_v)
    for copy in loads:
        copy.wait()

    def prepare(t, _):
        where = pl.ds(pl.multiple_of(t * FTILE, FTILE), FTILE)
        a = normed(h_v[where, :])
        a_v[where, :] = a
        at_v[:, where] = a.T
        dyt_v[:, where] = dy_v[where, :].T
        da_v[where, :] = jnp.zeros((FTILE, d), F32)
        return 0

    lax.fori_loop(0, tokens // FTILE, prepare, 0)
    lax.fori_loop(0, chunks, lambda i, _: chunk(i, True), 0)

    load = pltpu.make_async_copy(x_hbm, a_v, in_sem.at[2])
    load.start()

    def through_norm(t, _):
        where = pl.ds(pl.multiple_of(t * FTILE, FTILE), FTILE)
        wide = h_v[where, :].astype(F32)
        scale = scale_of(wide)
        g = da_v[where, :].astype(BF16).astype(F32)
        along = jnp.sum(g * wide, -1, keepdims=True)
        dh = (scale * g - wide * (scale * scale * scale * along * (1.0 / d))).astype(BF16)
        dy = (dy_v[where, :].astype(F32) + dh.astype(F32)).astype(BF16)
        dy_v[where, :] = dy
        dyt_v[:, where] = dy.T
        return 0

    lax.fori_loop(0, tokens // FTILE, through_norm, 0)
    lax.fori_loop(chunks, chunks + 1, drain, 0)
    load.wait()

    def prepare_first(t, _):
        where = pl.ds(pl.multiple_of(t * FTILE, FTILE), FTILE)
        a = normed(a_v[where, :])
        a_v[where, :] = a
        at_v[:, where] = a.T
        return 0

    lax.fori_loop(0, tokens // FTILE, prepare_first, 0)
    lax.fori_loop(chunks + 1, total + 1, lambda i, _: chunk(i, False), 0)

    lax.fori_loop(total + 1, total + 4, drain, 0)

    ssall_v[me] = ss_v[...]

    def squares(i, peer):
        return pltpu.make_async_remote_copy(
            src_ref=ss_v, dst_ref=ssall_v.at[me], send_sem=ss_send.at[i], recv_sem=ss_recv.at[i],
            device_id={"dp": peer}, device_id_type=MESH_ID,
        )

    sends = [squares(i, peer) for i, peer in enumerate((right, left, opposite))]
    for copy in sends:
        copy.start()

    def finish(k, _):
        out(k).wait()
        out_mine(k + chunks).wait()
        for which in range(2):
            out_shard(k + chunks, which).wait()
        return 0

    lax.fori_loop(0, chunks, finish, 0)
    for copy in sends:
        copy.wait()
    squares_sum = ssall_v[0]
    for j in range(1, n):
        squares_sum = squares_sum + ssall_v[j]
    ss_out[...] = squares_sum


def train(n, h, x, dy, wg, wu, wd):
    tokens, d = x.shape
    ff = wg.shape[2]
    chunks = ff // CHUNK
    rows = 3 * d
    anywhere = pl.BlockSpec(memory_space=pl.ANY)
    dma = pltpu.SemaphoreType.DMA
    return pl.pallas_call(
        functools.partial(train_kernel, n),
        out_shape=(
            jax.ShapeDtypeStruct((2 * chunks, rows, CHUNK), BF16),
            jax.ShapeDtypeStruct((chunks, rows // n // 2, CHUNK), BF16),
            jax.ShapeDtypeStruct((chunks, rows // n // 2, CHUNK), BF16),
            jax.ShapeDtypeStruct((8, CHUNK), F32),
        ),
        in_specs=[anywhere] * 6,
        out_specs=(anywhere, anywhere, anywhere, pl.BlockSpec(memory_space=pltpu.VMEM)),
        scratch_shapes=[
            pltpu.VMEM((tokens, d), BF16),
            pltpu.VMEM((tokens, d), BF16),
            pltpu.VMEM((d, tokens), BF16),
            pltpu.VMEM((tokens, d), BF16),
            pltpu.VMEM((d, tokens), BF16),
            pltpu.VMEM((tokens, d), F32),
            pltpu.VMEM((2, d, 2 * CHUNK), BF16),
            pltpu.VMEM((2, CHUNK, d), BF16),
            pltpu.VMEM((d, 2 * CHUNK), F32),
            pltpu.VMEM((d, CHUNK), F32),
            pltpu.VMEM((OWN, rows, CHUNK), BF16),
            pltpu.VMEM((2 * chunks, rows, CHUNK), BF16),
            pltpu.VMEM((2 * chunks, rows // n, CHUNK), BF16),
            pltpu.VMEM((8, CHUNK), F32),
            pltpu.VMEM((n, 8, CHUNK), F32),
            dma((3,)),
            dma((2, 3)),
            dma((4, 2, 2 * chunks)),
            dma((4, 2, 2 * chunks)),
            dma((3, 2 * chunks)),
            dma((3,)),
            dma((3,)),
        ],
        compiler_params=pltpu.CompilerParams(collective_id=0, has_side_effects=True, vmem_limit_bytes=VMEM_LIMIT),
        cost_estimate=pl.CostEstimate(flops=28 * tokens * d * ff, bytes_accessed=12 * tokens * d + 24 * d * ff, transcendentals=2 * tokens * ff),
        name="train",
    )(h, x, dy, wg, wu, wd)


def update_kernel(count, sources, first, table_ref, ss_ref, *refs):
    unit = pl.program_id(0)
    g_refs = []
    for parts in sources:
        g_refs.append(refs[:parts])
        refs = refs[parts:]
    w_refs, m_refs, v_refs = refs[:3], refs[3:6], refs[6:9]
    outs = refs[9:] if first else refs[18:]
    factor = jnp.minimum(1.0, 0.5 * lax.rsqrt(jnp.sum(ss_ref[...], keepdims=True) / count + 1e-30))
    pr, pd = w_refs[0].shape[1], w_refs[2].shape[3]

    def rows(halves, i, lo, hi):
        half = halves[0].shape[1]
        if hi <= half:
            return halves[0][i, lo:hi, :]
        if lo >= half:
            return halves[1][i, lo - half : hi - half, :]
        return jnp.concatenate([halves[0][i, lo:half, :], halves[1][i, 0 : hi - half, :]], 0)

    def step(which, at, g):
        g = g.astype(F32) * factor
        m = 0.9 * m_refs[which][at] + 0.1 * g
        v = 0.95 * v_refs[which][at] + 0.05 * g * g
        w = w_refs[which][at].astype(F32)
        outs[which][at] = (w - 0.02 * (m * lax.rsqrt(v + 1e-8) + 0.1 * w)).astype(BF16)
        outs[3 + which][at] = m
        outs[6 + which][at] = v

    for number, halves in enumerate(g_refs):

        @pl.when(table_ref[3 + len(g_refs), unit] == number)
        def _(halves=halves):
            for i in range(halves[0].shape[0]):
                cols = slice(i * CHUNK, (i + 1) * CHUNK)
                for which in range(2):
                    step(which, (0, slice(None), cols), rows(halves, i, which * pr, (which + 1) * pr))
                for h in range(w_refs[2].shape[4] // CHUNK):
                    at = (0, i, 0, slice(None), slice(h * CHUNK, (h + 1) * CHUNK))
                    step(2, at, rows(halves, i, 2 * pr + h * pd, 2 * pr + (h + 1) * pd))


def update(n, me, units, block, ss, sources, arrays, outs):
    d, ff = arrays[0].shape[1:]
    first = outs is None
    pr, pd = d // n, CHUNK // n
    count = sum(a.size for a in arrays[:3])
    fixed = jnp.array([[u[0], u[1], u[2], *u[5], u[4]] for u in units], jnp.int32).T
    moving = jnp.array([[0, 0, int(u[3]), *(0 for _ in u[5]), 0] for u in units], jnp.int32).T
    table = jnp.where(moving == 1, lax.rem(fixed + me, n), fixed)
    specs = [
        pl.BlockSpec((1, pr, block * CHUNK), lambda u, t: (t[0, u], t[2, u], t[1, u])),
        pl.BlockSpec((1, pr, block * CHUNK), lambda u, t: (t[0, u], t[2, u], t[1, u])),
        pl.BlockSpec((1, block, 1, pd, d), lambda u, t: (t[0, u], t[1, u], t[2, u], 0, 0)),
    ] * 3
    g_specs = []
    for s, source in enumerate(sources):
        if len(source) == 1:
            g_specs.append(pl.BlockSpec((block, source[0].shape[1] // n, CHUNK), lambda u, t, s=s: (t[3 + s, u], t[2, u], 0)))
        else:
            g_specs += [pl.BlockSpec((block, *a.shape[1:]), lambda u, t, s=s: (t[3 + s, u], 0, 0)) for a in source]
    gs = [a for source in sources for a in source]
    size = len(units) * 3 * pr * block * CHUNK
    return pl.pallas_call(
        functools.partial(update_kernel, count, tuple(len(source) for source in sources), first),
        out_shape=tuple(jax.ShapeDtypeStruct(a.shape, a.dtype) for a in arrays),
        grid_spec=pltpu.PrefetchScalarGridSpec(
            num_scalar_prefetch=1,
            grid=(len(units),),
            in_specs=[pl.BlockSpec(ss.shape, lambda u, t: (0, 0)), *g_specs, *specs]
            + ([] if first else [pl.BlockSpec(memory_space=pl.ANY)] * 9),
            out_specs=tuple(specs),
        ),
        input_output_aliases={} if first else {2 + len(gs) + 9 + i: i for i in range(9)},
        compiler_params=pltpu.CompilerParams(vmem_limit_bytes=VMEM_LIMIT),
        cost_estimate=pl.CostEstimate(flops=15 * size, bytes_accessed=22 * size, transcendentals=size),
        name="update",
    )(table, ss, *gs, *arrays, *([] if first else outs))


def solution(mesh):
    n = mesh.shape["dp"]
    assert n == 4

    def step(x, dy, *arrays):
        x, dy = x.reshape(x.shape[1:]), dy.reshape(dy.shape[1:])
        wg, wu, wd = arrays[:3]
        h = forward(x, wg, wu, wd)
        gathered, half_a, half_b, ss = train(n, h, x, dy, wg, wu, wd)

        to_right = [(i, (i + 1) % n) for i in range(n)]
        to_left = [(i, (i + n - 1) % n) for i in range(n)]
        left_b = lax.ppermute(half_b, "dp", to_right)
        right_a = lax.ppermute(half_a, "dp", to_left)
        left_a = lax.ppermute(half_a, "dp", to_right)
        right_b = lax.ppermute(half_b, "dp", to_left)

        layers, ff, d = wd.shape
        chunks = ff // CHUNK
        cut = (layers, chunks, n, CHUNK // n, d)
        views = [a.reshape(cut) if i % 3 == 2 else a for i, a in enumerate(arrays)]
        me = lax.axis_index("dp").astype(jnp.int32)

        block = 4
        blocks = chunks // block
        units = [(1, b, s, False, 0, (b,)) for b in range(blocks) for s in range(n)]
        units += [(0, b, 0, True, 0, (blocks + b,)) for b in range(blocks)]
        outs = update(n, me, units, block, ss, ((gathered,),), views, None)
        left_b, right_a, outs = lax.optimization_barrier((left_b, right_a, outs))
        far_b = lax.ppermute(left_b, "dp", to_right)
        far_a = lax.ppermute(right_a, "dp", to_left)
        units = [(0, b, n - 1, True, 0, (b, 0)) for b in range(blocks)] + [(0, b, 1, True, 1, (blocks - 1, b)) for b in range(blocks)]
        outs = update(n, me, units, block, ss, ((left_a, left_b), (right_a, right_b)), views, outs)
        block = 2
        blocks = chunks // block
        units = [(0, b, 2, True, 0, (b,)) for b in range(blocks)]
        outs = update(n, me, units, block, ss, ((far_a, far_b),), views, outs)
        return tuple(o.reshape(a.shape) for o, a in zip(outs, arrays, strict=True))

    return jax.shard_map(
        step,
        mesh=mesh,
        in_specs=(P(("rep", "dp"), None, None),) * 2 + (P(None, None, None),) * 9,
        out_specs=(P("rep", None, None),) * 9,
        check_vma=False,
    )
```

```python
import functools

import jax
import jax.numpy as jnp
from jax import lax
from jax.experimental import pallas as pl
from jax.experimental.pallas import tpu as pltpu
from jax.sharding import PartitionSpec as P

F32, BF16 = jnp.float32, jnp.bfloat16
CHUNK = 256
TILE = 1024
FTILE = 512
OWN = 4
VMEM_LIMIT = 67_043_328
MESH_ID = pl.DeviceIdType.MESH


def dot(a, b):
    return jnp.dot(a, b, preferred_element_type=F32)


def dot_t(a, b):
    return lax.dot_general(a, b, (((1,), (1,)), ((), ())), preferred_element_type=F32)


def sigmoid(x):
    return 0.5 * jnp.tanh(0.5 * x) + 0.5


def scale_of(wide):
    return lax.rsqrt(jnp.mean(wide * wide, -1, keepdims=True) + 1e-6)


def normed(h):
    wide = h.astype(F32)
    return (wide * scale_of(wide)).astype(BF16)


def train_kernel(n, x_hbm, dy_hbm, wg_hbm, wu_hbm, wd_hbm, g_out, sa_out, sb_out, ss_out,
                 h_v, a_v, at_v, dy_v, dyt_v, da_v, w_v, wd_v, gu_v, gd_v, own_v, all_v, left_v, ss_v, ssall_v,
                 in_sem, again_sem, first_sem, w_sem, send_sem, recv_sem, out_sem, ss_send, ss_recv):
    tokens, d = h_v.shape
    chunks = wg_hbm.shape[2] // CHUNK
    total = 2 * chunks
    rows = own_v.shape[1]
    shard, half = rows // n, rows // n // 2
    pr, pd = d // n, CHUNK // n
    me = lax.axis_index("dp")
    right, left, opposite = lax.rem(me + 1, n), lax.rem(me + n - 1, n), lax.rem(me + 2, n)

    barrier = pltpu.get_barrier_semaphore()
    for peer in (left, right, opposite):
        pl.semaphore_signal(barrier, inc=1, device_id={"dp": peer}, device_id_type=MESH_ID)
    pl.semaphore_wait(barrier, 3)

    def part(j, which=None):
        if which is None:
            return pl.ds(pl.multiple_of(j * shard, half), shard)
        return pl.ds(pl.multiple_of(j * shard + which * half, half), half)

    def weights(k):
        layer, c, slot = 1 - k // chunks, lax.rem(k, chunks), lax.rem(k, 2)
        cols = pl.ds(pl.multiple_of(c * CHUNK, CHUNK), CHUNK)
        return (
            pltpu.make_async_copy(wg_hbm.at[layer, :, cols], w_v.at[slot, :, pl.ds(0, CHUNK)], w_sem.at[slot, 0]),
            pltpu.make_async_copy(wu_hbm.at[layer, :, cols], w_v.at[slot, :, pl.ds(CHUNK, CHUNK)], w_sem.at[slot, 1]),
            pltpu.make_async_copy(wd_hbm.at[layer, cols, :], wd_v.at[slot], w_sem.at[slot, 2]),
        )

    def remote(kind, way, k, src, dst):
        return pltpu.make_async_remote_copy(
            src_ref=src, dst_ref=dst, send_sem=send_sem.at[kind, way, k], recv_sem=recv_sem.at[kind, way, k],
            device_id={"dp": (left, right)[way]}, device_id_type=MESH_ID,
        )

    def first(way, k):
        where = part(opposite, way)
        return remote(0, way, k, own_v.at[lax.rem(k, OWN), where], all_v.at[k, where])

    def second(way, k):
        where = part((left, right)[way])
        return remote(1, way, k, own_v.at[lax.rem(k, OWN), where], all_v.at[k, where] if way == 0 else left_v.at[k])

    def third(way, p):
        where = pl.ds(2 * p, 2)
        return remote(2, way, p, all_v.at[where, part(me)], all_v.at[where, part(me)])

    def fourth(way, p):
        where = pl.ds(2 * p, 2)
        half_of = part((right, left)[way], way)
        return remote(3, way, p, all_v.at[where, half_of], all_v.at[where, half_of])

    def out(p):
        where = pl.ds(2 * p, 2)
        return pltpu.make_async_copy(all_v.at[where], g_out.at[where], out_sem.at[0, p])

    def out_mine(k):
        return pltpu.make_async_copy(all_v.at[k, part(me)], g_out.at[k, part(me)], out_sem.at[0, k])

    def out_shard(k, which):
        return pltpu.make_async_copy(all_v.at[k, part(me, which)], (sa_out, sb_out)[which].at[k - chunks], out_sem.at[1 + which, k])

    def chunk_at(i):
        return jnp.where(i > chunks, i - 1, i)

    def alive(i):
        return (i >= 0) & (i <= total) & (i != chunks)

    def gather_at(i):
        i = i - 4
        p = i // 3
        return p, (i >= 0) & (i % 3 == 0) & (2 * p < chunks)

    lag = 3

    def exchange(i):
        @pl.when(alive(i - 1))
        def _():
            q = chunk_at(i - 1)
            slot = lax.rem(q, OWN)
            for way in range(2):
                first(way, q).wait_recv()
            for j, which in ((left, 0), (right, 1)):
                where = part(j, which)
                own_v[slot, where, :] = (own_v[slot, where, :].astype(F32) + all_v[q, where, :].astype(F32)).astype(BF16)

        @pl.when(alive(i))
        def _():
            for way in range(2):
                first(way, chunk_at(i)).start()

        @pl.when(alive(i - lag))
        def _():
            q = chunk_at(i - lag)
            slot = lax.rem(q, OWN)
            for way in range(2):
                second(way, q).wait_recv()
            mine = part(me)
            g = own_v[slot, mine, :].astype(F32) + all_v[q, mine, :].astype(F32) + left_v[q].astype(F32)
            g = g.astype(BF16)
            all_v[q, mine, :] = g
            wide = g.astype(F32)
            ss_v[...] += jnp.sum((wide * wide).reshape(shard // 8, 8, CHUNK), 0)

        @pl.when(alive(i - 1))
        def _():
            for way in range(2):
                second(way, chunk_at(i - 1)).start()

        g2, go2 = gather_at(i - 2)

        @pl.when(go2)
        def _():
            for way in range(2):
                third(way, g2).wait_recv()
            for way in range(2):
                fourth(way, g2).start()

        g1, go1 = gather_at(i)

        @pl.when(go1)
        def _():
            for way in range(2):
                third(way, g1).start()

        @pl.when(alive(i - lag) & (chunk_at(i - lag) >= chunks))
        def _():
            q = chunk_at(i - lag)
            for which in range(2):
                out_shard(q, which).start()
            out_mine(q).start()

        @pl.when(alive(i - lag))
        def _():
            for way in range(2):
                first(way, chunk_at(i - lag)).wait_send()
                second(way, chunk_at(i - lag)).wait_send()

        g3, go3 = gather_at(i - 5)

        @pl.when(go3)
        def _():
            for way in range(2):
                third(way, g3).wait_send()
                fourth(way, g3).wait_send()
                fourth(way, g3).wait_recv()
            out(g3).start()

    def chunk(i, last_layer):
        k = i if last_layer else i - 1
        slot = lax.rem(k, 2)

        @pl.when(k + 1 < total)
        def _():
            for copy in weights(k + 1):
                copy.start()

        for copy in weights(k):
            copy.wait()
        gu_v[...] = jnp.zeros_like(gu_v)
        gd_v[...] = jnp.zeros_like(gd_v)

        def tile(t, _):
            where = pl.ds(pl.multiple_of(t * TILE, TILE), TILE)
            w = w_v[slot]
            both = dot(a_v[where, :], w)
            dp = dot_t(dy_v[where, :], wd_v[slot]).astype(BF16).astype(F32)
            gate, up = both[:, :CHUNK], both[:, CHUNK:]
            s = sigmoid(gate)
            act = gate * s
            p = (act * up).astype(BF16)
            gd_v[...] += dot(dyt_v[:, where], p)
            dgate = (dp * up * (s + act * (1.0 - s))).astype(BF16)
            dup = (dp * act).astype(BF16)
            dboth = jnp.concatenate([dgate, dup], 1)
            gu_v[...] += dot(at_v[:, where], dboth)
            if last_layer:
                da_v[where, :] += dot_t(dboth, w)
            return 0

        lax.fori_loop(0, tokens // TILE, tile, 0)
        o = lax.rem(k, OWN)
        down = gd_v[...].T
        for j in range(n):
            own_v[o, j * shard : j * shard + pr, :] = gu_v[j * pr : (j + 1) * pr, :CHUNK].astype(BF16)
            own_v[o, j * shard + pr : j * shard + 2 * pr, :] = gu_v[j * pr : (j + 1) * pr, CHUNK:].astype(BF16)
            for b in range(d // CHUNK):
                at = j * shard + 2 * pr + b * pd
                own_v[o, at : at + pd, :] = down[j * pd : (j + 1) * pd, b * CHUNK : (b + 1) * CHUNK].astype(BF16)
        exchange(i)
        return 0

    def drain(i, _):
        exchange(i)
        return 0

    def first_weights(c):
        cols = pl.ds(pl.multiple_of(c * CHUNK, CHUNK), CHUNK)
        held = all_v.at[chunks + c]
        copies = [
            pltpu.make_async_copy(wg_hbm.at[0, :, cols], held.at[pl.ds(0, d)], first_sem.at[0, c]),
            pltpu.make_async_copy(wu_hbm.at[0, :, cols], held.at[pl.ds(d, d)], first_sem.at[1, c]),
        ]
        for b in range(d // CHUNK):
            to = held.at[pl.ds(2 * d + b * CHUNK, CHUNK)]
            copies.append(pltpu.make_async_copy(wd_hbm.at[0, cols, pl.ds(b * CHUNK, CHUNK)], to, first_sem.at[2 + b, c]))
        return copies

    def x_tile(t):
        where = pl.ds(pl.multiple_of(t * FTILE, FTILE), FTILE)
        return pltpu.make_async_copy(x_hbm.at[where], h_v.at[where], in_sem.at[0, t])

    def dy_tile(t):
        where = pl.ds(pl.multiple_of(t * FTILE, FTILE), FTILE)
        return pltpu.make_async_copy(dy_hbm.at[where], dy_v.at[where], in_sem.at[1, t])

    steps = tokens // FTILE
    for t in range(steps):
        dy_tile(t).start()
    x_tile(0).start()
    for c in range(chunks):
        for copy in first_weights(c):
            copy.start()
    for t in range(1, steps):
        x_tile(t).start()
    for copy in weights(0):
        copy.start()
    ss_v[...] = jnp.zeros_like(ss_v)

    def turn(t, _):
        where = pl.ds(pl.multiple_of(t * FTILE, FTILE), FTILE)
        dy_tile(t).wait()
        dyt_v[:, where] = dy_v[where, :].T
        return 0

    lax.fori_loop(0, steps, turn, 0)
    for c in range(chunks):
        for copy in first_weights(c):
            copy.wait()

    def forward(t, _):
        where = pl.ds(pl.multiple_of(t * FTILE, FTILE), FTILE)
        x_tile(t).wait()
        x = h_v[where, :]
        a = normed(x)
        sums = [None] * (d // CHUNK)
        for c in range(chunks, total, 2):
            ps = []
            for b in range(2):
                gate = dot(a, all_v[c + b, :d, :])
                up = dot(a, all_v[c + b, d : 2 * d, :])
                ps.append((gate * sigmoid(gate) * up).astype(BF16))
            p = jnp.concatenate(ps, 1)
            for b in range(d // CHUNK):
                at = 2 * d + b * CHUNK
                term = dot(p, all_v[c : c + 2, at : at + CHUNK, :].reshape(2 * CHUNK, CHUNK))
                sums[b] = term if sums[b] is None else sums[b] + term
        out = jnp.concatenate(sums, 1).astype(BF16)
        h = (x.astype(F32) + out.astype(F32)).astype(BF16)
        h_v[where, :] = h
        a = normed(h)
        a_v[where, :] = a
        at_v[:, where] = a.T
        da_v[where, :] = jnp.zeros((FTILE, d), F32)
        return 0

    lax.fori_loop(0, steps, forward, 0)
    lax.fori_loop(0, chunks, lambda i, _: chunk(i, True), 0)

    load = pltpu.make_async_copy(x_hbm, a_v, again_sem)
    load.start()

    def through_norm(t, _):
        where = pl.ds(pl.multiple_of(t * FTILE, FTILE), FTILE)
        wide = h_v[where, :].astype(F32)
        scale = scale_of(wide)
        g = da_v[where, :].astype(BF16).astype(F32)
        along = jnp.sum(g * wide, -1, keepdims=True)
        dh = (scale * g - wide * (scale * scale * scale * along * (1.0 / d))).astype(BF16)
        dy = (dy_v[where, :].astype(F32) + dh.astype(F32)).astype(BF16)
        dy_v[where, :] = dy
        dyt_v[:, where] = dy.T
        return 0

    lax.fori_loop(0, tokens // FTILE, through_norm, 0)
    lax.fori_loop(chunks, chunks + 1, drain, 0)
    load.wait()

    def prepare_first(t, _):
        where = pl.ds(pl.multiple_of(t * FTILE, FTILE), FTILE)
        a = normed(a_v[where, :])
        a_v[where, :] = a
        at_v[:, where] = a.T
        return 0

    lax.fori_loop(0, tokens // FTILE, prepare_first, 0)
    lax.fori_loop(chunks + 1, total + 1, lambda i, _: chunk(i, False), 0)

    lax.fori_loop(total + 1, total + lag + 1, drain, 0)

    ssall_v[me] = ss_v[...]

    def squares(i, peer):
        return pltpu.make_async_remote_copy(
            src_ref=ss_v, dst_ref=ssall_v.at[me], send_sem=ss_send.at[i], recv_sem=ss_recv.at[i],
            device_id={"dp": peer}, device_id_type=MESH_ID,
        )

    sends = [squares(i, peer) for i, peer in enumerate((right, left, opposite))]
    for copy in sends:
        copy.start()

    def finish(k, _):
        out_mine(k + chunks).wait()
        for which in range(2):
            out_shard(k + chunks, which).wait()
        return 0

    lax.fori_loop(0, chunks, finish, 0)

    def finish_pair(p, _):
        out(p).wait()
        return 0

    lax.fori_loop(0, chunks // 2, finish_pair, 0)
    for copy in sends:
        copy.wait()
    squares_sum = ssall_v[0]
    for j in range(1, n):
        squares_sum = squares_sum + ssall_v[j]
    ss_out[...] = squares_sum


def train(n, x, dy, wg, wu, wd):
    tokens, d = x.shape
    ff = wg.shape[2]
    chunks = ff // CHUNK
    rows = 3 * d
    anywhere = pl.BlockSpec(memory_space=pl.ANY)
    dma = pltpu.SemaphoreType.DMA
    return pl.pallas_call(
        functools.partial(train_kernel, n),
        out_shape=(
            jax.ShapeDtypeStruct((2 * chunks, rows, CHUNK), BF16),
            jax.ShapeDtypeStruct((chunks, rows // n // 2, CHUNK), BF16),
            jax.ShapeDtypeStruct((chunks, rows // n // 2, CHUNK), BF16),
            jax.ShapeDtypeStruct((8, CHUNK), F32),
        ),
        in_specs=[anywhere] * 5,
        out_specs=(anywhere, anywhere, anywhere, pl.BlockSpec(memory_space=pltpu.VMEM)),
        scratch_shapes=[
            pltpu.VMEM((tokens, d), BF16),
            pltpu.VMEM((tokens, d), BF16),
            pltpu.VMEM((d, tokens), BF16),
            pltpu.VMEM((tokens, d), BF16),
            pltpu.VMEM((d, tokens), BF16),
            pltpu.VMEM((tokens, d), F32),
            pltpu.VMEM((2, d, 2 * CHUNK), BF16),
            pltpu.VMEM((2, CHUNK, d), BF16),
            pltpu.VMEM((d, 2 * CHUNK), F32),
            pltpu.VMEM((d, CHUNK), F32),
            pltpu.VMEM((OWN, rows, CHUNK), BF16),
            pltpu.VMEM((2 * chunks, rows, CHUNK), BF16),
            pltpu.VMEM((2 * chunks, rows // n, CHUNK), BF16),
            pltpu.VMEM((8, CHUNK), F32),
            pltpu.VMEM((n, 8, CHUNK), F32),
            dma((2, tokens // FTILE)),
            dma,
            dma((2 + d // CHUNK, chunks)),
            dma((2, 3)),
            dma((4, 2, 2 * chunks)),
            dma((4, 2, 2 * chunks)),
            dma((3, 2 * chunks)),
            dma((3,)),
            dma((3,)),
        ],
        compiler_params=pltpu.CompilerParams(collective_id=0, has_side_effects=True, vmem_limit_bytes=VMEM_LIMIT),
        cost_estimate=pl.CostEstimate(flops=34 * tokens * d * ff, bytes_accessed=12 * tokens * d + 24 * d * ff, transcendentals=3 * tokens * ff),
        name="train",
    )(x, dy, wg, wu, wd)


def update_kernel(count, sources, first, unit, me_ref, ss_ref, *refs):
    source = unit(pl.program_id(0), me_ref[0])[3]
    g_refs = []
    for parts in sources:
        g_refs.append(refs[:parts])
        refs = refs[parts:]
    w_refs, m_refs, v_refs = refs[:3], refs[3:6], refs[6:9]
    outs = refs[9:] if first else refs[18:]
    factor = jnp.minimum(1.0, 0.5 * lax.rsqrt(jnp.sum(ss_ref[...], keepdims=True) / count + 1e-30))
    pr, pd = w_refs[0].shape[1], w_refs[2].shape[3]

    def rows(halves, i, lo, hi):
        half = halves[0].shape[1]
        if hi <= half:
            return halves[0][i, lo:hi, :]
        if lo >= half:
            return halves[1][i, lo - half : hi - half, :]
        return jnp.concatenate([halves[0][i, lo:half, :], halves[1][i, 0 : hi - half, :]], 0)

    def step(which, at, g):
        g = g.astype(F32) * factor
        m = 0.9 * m_refs[which][at] + 0.1 * g
        v = 0.95 * v_refs[which][at] + 0.05 * g * g
        w = w_refs[which][at].astype(F32)
        outs[which][at] = (w - 0.02 * (m * lax.rsqrt(v + 1e-8) + 0.1 * w)).astype(BF16)
        outs[3 + which][at] = m
        outs[6 + which][at] = v

    for number, halves in enumerate(g_refs):

        @pl.when(source == number)
        def _(halves=halves):
            for i in range(halves[0].shape[0]):
                cols = slice(i * CHUNK, (i + 1) * CHUNK)
                for which in range(2):
                    step(which, (0, slice(None), cols), rows(halves, i, which * pr, (which + 1) * pr))
                for h in range(w_refs[2].shape[4] // CHUNK):
                    at = (0, i, 0, slice(None), slice(h * CHUNK, (h + 1) * CHUNK))
                    step(2, at, rows(halves, i, 2 * pr + h * pd, 2 * pr + (h + 1) * pd))


def update(n, me, units, unit, block, ss, sources, arrays, outs):
    d, ff = arrays[0].shape[1:]
    first = outs is None
    pr, pd = d // n, CHUNK // n
    count = sum(a.size for a in arrays[:3])

    def side(u, me_ref):
        layer, b, s, _, _ = unit(u, me_ref[0])
        return layer, s, b

    def down(u, me_ref):
        layer, b, s, _, _ = unit(u, me_ref[0])
        return layer, b, s, 0, 0

    def whole_g(u, me_ref):
        _, _, s, _, at = unit(u, me_ref[0])
        return at[0], s, 0

    specs = [pl.BlockSpec((1, pr, block * CHUNK), side)] * 2 + [pl.BlockSpec((1, block, 1, pd, d), down)]
    specs = specs * 3
    g_specs = []
    for i, source in enumerate(sources):
        if len(source) == 1:
            g_specs.append(pl.BlockSpec((block, source[0].shape[1] // n, CHUNK), whole_g))
        else:
            g_specs += [pl.BlockSpec((block, *a.shape[1:]), lambda u, me_ref, i=i: (unit(u, me_ref[0])[4][i], 0, 0)) for a in source]
    gs = [a for source in sources for a in source]
    size = units * 3 * pr * block * CHUNK
    return pl.pallas_call(
        functools.partial(update_kernel, count, tuple(len(source) for source in sources), first, unit),
        out_shape=tuple(jax.ShapeDtypeStruct(a.shape, a.dtype) for a in arrays),
        grid_spec=pltpu.PrefetchScalarGridSpec(
            num_scalar_prefetch=1,
            grid=(units,),
            in_specs=[pl.BlockSpec(ss.shape, lambda u, me_ref: (0, 0)), *g_specs, *specs]
            + ([] if first else [pl.BlockSpec(memory_space=pl.ANY)] * 9),
            out_specs=tuple(specs),
        ),
        input_output_aliases={} if first else {2 + len(gs) + 9 + i: i for i in range(9)},
        compiler_params=pltpu.CompilerParams(vmem_limit_bytes=VMEM_LIMIT),
        cost_estimate=pl.CostEstimate(flops=15 * size, bytes_accessed=22 * size, transcendentals=size),
        name="update",
    )(me, ss, *gs, *arrays, *([] if first else outs))


def solution(mesh):
    n = mesh.shape["dp"]
    assert n == 4

    def step(x, dy, *arrays):
        x, dy = x.reshape(x.shape[1:]), dy.reshape(dy.shape[1:])
        wg, wu, wd = arrays[:3]
        gathered, half_a, half_b, ss = train(n, x, dy, wg, wu, wd)

        to_right = [(i, (i + 1) % n) for i in range(n)]
        to_left = [(i, (i + n - 1) % n) for i in range(n)]
        left_b = lax.ppermute(half_b, "dp", to_right)
        right_a = lax.ppermute(half_a, "dp", to_left)
        left_a = lax.ppermute(half_a, "dp", to_right)
        right_b = lax.ppermute(half_b, "dp", to_left)

        layers, ff, d = wd.shape
        chunks = ff // CHUNK
        cut = (layers, chunks, n, CHUNK // n, d)
        views = [a.reshape(cut) if i % 3 == 2 else a for i, a in enumerate(arrays)]
        me = lax.axis_index("dp").astype(jnp.int32).reshape(1)

        blocks = chunks // 4

        def unit(u, me, blocks=blocks):
            mine = u >= blocks * n
            b = jnp.where(mine, u - blocks * n, u // n)
            return jnp.where(mine, 0, 1), b, jnp.where(mine, me, u % n), 0, (jnp.where(mine, blocks + b, b),)

        outs = update(n, me, blocks * (n + 1), unit, 4, ss, ((gathered,),), views, None)
        left_b, right_a, outs = lax.optimization_barrier((left_b, right_a, outs))
        far_b = lax.ppermute(left_b, "dp", to_right)
        far_a = lax.ppermute(right_a, "dp", to_left)

        def unit(u, me, blocks=blocks):
            on_right = u >= blocks
            b = jnp.where(on_right, u - blocks, u)
            shard = (me + jnp.where(on_right, 1, n - 1)) % n
            return 0, b, shard, jnp.where(on_right, 1, 0), (jnp.where(on_right, blocks - 1, b), jnp.where(on_right, b, 0))

        outs = update(n, me, 2 * blocks, unit, 4, ss, ((left_a, left_b), (right_a, right_b)), views, outs)

        def unit(u, me):
            return 0, u, (me + 2) % n, 0, (u,)

        outs = update(n, me, chunks // 2, unit, 2, ss, ((far_a, far_b),), views, outs)
        return tuple(o.reshape(a.shape) for o, a in zip(outs, arrays, strict=True))

    return jax.shard_map(
        step,
        mesh=mesh,
        in_specs=(P(("rep", "dp"), None, None),) * 2 + (P(None, None, None),) * 9,
        out_specs=(P("rep", None, None),) * 9,
        check_vma=False,
    )
```

```python
import functools

import jax
import jax.numpy as jnp
from jax import lax
from jax.experimental import pallas as pl
from jax.experimental.pallas import tpu as pltpu
from jax.sharding import PartitionSpec as P

F32, BF16 = jnp.float32, jnp.bfloat16
CHUNK = 256
TILE = 1024
FWD = 256
FTILE = 512
AHEAD = 3
OWN = 4
VMEM_LIMIT = 67_043_328
MESH_ID = pl.DeviceIdType.MESH


def dot(a, b):
    return jnp.dot(a, b, preferred_element_type=F32)


def dot_t(a, b):
    return lax.dot_general(a, b, (((1,), (1,)), ((), ())), preferred_element_type=F32)


def sigmoid(x):
    return 0.5 * jnp.tanh(0.5 * x) + 0.5


def scale_of(wide):
    return lax.rsqrt(jnp.mean(wide * wide, -1, keepdims=True) + 1e-6)


def normed(h):
    wide = h.astype(F32)
    return (wide * scale_of(wide)).astype(BF16)


def train_kernel(n, x_hbm, dy_hbm, wg_hbm, wu_hbm, wd_hbm, g_out, sa_out, sb_out, ss_out, kept_hbm,
                 h_v, a_v, at_v, dy_v, dyt_v, da_v, w_v, wd_v, gu_v, gd_v, own_v, all_v, left_v, ss_v, ssall_v,
                 in_sem, again_sem, kept_sem, first_sem, w_sem, send_sem, recv_sem, out_sem, ss_send, ss_recv):
    tokens, d = h_v.shape
    chunks = wg_hbm.shape[2] // CHUNK
    total = 2 * chunks
    rows = own_v.shape[1]
    shard, half = rows // n, rows // n // 2
    pr, pd = d // n, CHUNK // n
    me = lax.axis_index("dp")
    right, left, opposite = lax.rem(me + 1, n), lax.rem(me + n - 1, n), lax.rem(me + 2, n)

    barrier = pltpu.get_barrier_semaphore()
    for peer in (left, right, opposite):
        pl.semaphore_signal(barrier, inc=1, device_id={"dp": peer}, device_id_type=MESH_ID)
    pl.semaphore_wait(barrier, 3)

    def part(j, which=None):
        if which is None:
            return pl.ds(pl.multiple_of(j * shard, half), shard)
        return pl.ds(pl.multiple_of(j * shard + which * half, half), half)

    def weights(k):
        layer, c, slot = 1 - k // chunks, lax.rem(k, chunks), lax.rem(k, 2)
        cols = pl.ds(pl.multiple_of(c * CHUNK, CHUNK), CHUNK)
        return (
            pltpu.make_async_copy(wg_hbm.at[layer, :, cols], w_v.at[slot, :, pl.ds(0, CHUNK)], w_sem.at[slot, 0]),
            pltpu.make_async_copy(wu_hbm.at[layer, :, cols], w_v.at[slot, :, pl.ds(CHUNK, CHUNK)], w_sem.at[slot, 1]),
            pltpu.make_async_copy(wd_hbm.at[layer, cols, :], wd_v.at[slot], w_sem.at[slot, 2]),
        )

    def remote(kind, way, k, src, dst):
        return pltpu.make_async_remote_copy(
            src_ref=src, dst_ref=dst, send_sem=send_sem.at[kind, way, k], recv_sem=recv_sem.at[kind, way, k],
            device_id={"dp": (left, right)[way]}, device_id_type=MESH_ID,
        )

    def first(way, k):
        where = part(opposite, way)
        return remote(0, way, k, own_v.at[lax.rem(k, OWN), where], all_v.at[k, where])

    def second(way, k):
        where = part((left, right)[way])
        return remote(1, way, k, own_v.at[lax.rem(k, OWN), where], all_v.at[k, where] if way == 0 else left_v.at[k])

    def third(way, p):
        where = pl.ds(2 * p, 2)
        return remote(2, way, p, all_v.at[where, part(me)], all_v.at[where, part(me)])

    def fourth(way, p):
        where = pl.ds(2 * p, 2)
        half_of = part((right, left)[way], way)
        return remote(3, way, p, all_v.at[where, half_of], all_v.at[where, half_of])

    def out(p):
        where = pl.ds(2 * p, 2)
        return pltpu.make_async_copy(all_v.at[where], g_out.at[where], out_sem.at[0, p])

    def out_mine(k):
        return pltpu.make_async_copy(all_v.at[k, part(me)], g_out.at[k, part(me)], out_sem.at[0, k])

    def out_shard(k, which):
        return pltpu.make_async_copy(all_v.at[k, part(me, which)], (sa_out, sb_out)[which].at[k - chunks], out_sem.at[1 + which, k])

    def chunk_at(i):
        return jnp.where(i > chunks, i - 1, i)

    def alive(i):
        return (i >= 0) & (i <= total) & (i != chunks)

    def gather_at(i):
        i = i - 4
        p = i // 3
        return p, (i >= 0) & (i % 3 == 0) & (2 * p < chunks)

    lag = 3

    def exchange(i):
        @pl.when(alive(i - 1))
        def _():
            q = chunk_at(i - 1)
            slot = lax.rem(q, OWN)
            for way in range(2):
                first(way, q).wait_recv()
            for j, which in ((left, 0), (right, 1)):
                where = part(j, which)
                own_v[slot, where, :] = (own_v[slot, where, :].astype(F32) + all_v[q, where, :].astype(F32)).astype(BF16)

        @pl.when(alive(i))
        def _():
            for way in range(2):
                first(way, chunk_at(i)).start()

        @pl.when(alive(i - lag))
        def _():
            q = chunk_at(i - lag)
            slot = lax.rem(q, OWN)
            for way in range(2):
                second(way, q).wait_recv()
            mine = part(me)
            g = own_v[slot, mine, :].astype(F32) + all_v[q, mine, :].astype(F32) + left_v[q].astype(F32)
            g = g.astype(BF16)
            all_v[q, mine, :] = g
            wide = g.astype(F32)
            ss_v[...] += jnp.sum((wide * wide).reshape(shard // 8, 8, CHUNK), 0)

        @pl.when(alive(i - 1))
        def _():
            for way in range(2):
                second(way, chunk_at(i - 1)).start()

        g2, go2 = gather_at(i - 2)

        @pl.when(go2)
        def _():
            for way in range(2):
                third(way, g2).wait_recv()
            for way in range(2):
                fourth(way, g2).start()

        g1, go1 = gather_at(i)

        @pl.when(go1)
        def _():
            for way in range(2):
                third(way, g1).start()

        @pl.when(alive(i - lag) & (chunk_at(i - lag) >= chunks))
        def _():
            q = chunk_at(i - lag)
            for which in range(2):
                out_shard(q, which).start()
            out_mine(q).start()

        @pl.when(alive(i - lag))
        def _():
            for way in range(2):
                first(way, chunk_at(i - lag)).wait_send()
                second(way, chunk_at(i - lag)).wait_send()

        g3, go3 = gather_at(i - 5)

        @pl.when(go3)
        def _():
            for way in range(2):
                third(way, g3).wait_send()
                fourth(way, g3).wait_send()
                fourth(way, g3).wait_recv()
            out(g3).start()

    tiles, per = tokens // TILE, TILE // FWD

    def keep(t):
        slot = lax.rem(t, 2) * chunks
        return pltpu.make_async_copy(da_v.at[pl.ds(slot, chunks)], kept_hbm.at[t], kept_sem.at[lax.rem(t, 2)])

    def kept(at):
        slot = lax.rem(at, AHEAD + 1)
        where = pl.ds(lax.rem(at, tiles) * per, per)
        return pltpu.make_async_copy(kept_hbm.at[where, at // tiles], da_v.at[pl.ds(slot * per, per)], kept_sem.at[2 + slot])

    def chunk(i, last_layer):
        k = i if last_layer else i - 1
        slot = lax.rem(k, 2)

        @pl.when(k + 1 < total)
        def _():
            for copy in weights(k + 1):
                copy.start()

        for copy in weights(k):
            copy.wait()
        gu_v[...] = jnp.zeros_like(gu_v)
        gd_v[...] = jnp.zeros_like(gd_v)

        def tile(t, _):
            where = pl.ds(pl.multiple_of(t * TILE, TILE), TILE)
            if last_layer:
                w = w_v[slot]
                both = dot(a_v[where, :], w)
            else:
                at = (k - chunks) * tiles + t

                @pl.when(at + AHEAD < chunks * tiles)
                def _():
                    kept(at + AHEAD).start()

                kept(at).wait()
                both = da_v[pl.ds(lax.rem(at, AHEAD + 1) * per, per)].reshape(TILE, 2 * CHUNK)
            dp = dot_t(dy_v[where, :], wd_v[slot]).astype(BF16).astype(F32)
            gate, up = both[:, :CHUNK], both[:, CHUNK:]
            s = sigmoid(gate)
            act = gate * s
            p = (act * up).astype(BF16)
            gd_v[...] += dot(dyt_v[:, where], p)
            dgate = (dp * up * (s + act * (1.0 - s))).astype(BF16)
            dup = (dp * act).astype(BF16)
            dboth = jnp.concatenate([dgate, dup], 1)
            gu_v[...] += dot(at_v[:, where], dboth)
            if last_layer:
                da_v[pl.ds(t * per, per)] += dot_t(dboth, w).reshape(per, FWD, d)
            return 0

        lax.fori_loop(0, tokens // TILE, tile, 0)
        o = lax.rem(k, OWN)
        down = gd_v[...].T
        for j in range(n):
            own_v[o, j * shard : j * shard + pr, :] = gu_v[j * pr : (j + 1) * pr, :CHUNK].astype(BF16)
            own_v[o, j * shard + pr : j * shard + 2 * pr, :] = gu_v[j * pr : (j + 1) * pr, CHUNK:].astype(BF16)
            for b in range(d // CHUNK):
                at = j * shard + 2 * pr + b * pd
                own_v[o, at : at + pd, :] = down[j * pd : (j + 1) * pd, b * CHUNK : (b + 1) * CHUNK].astype(BF16)
        exchange(i)
        return 0

    def drain(i, _):
        exchange(i)
        return 0

    def first_weights(c):
        cols = pl.ds(pl.multiple_of(c * CHUNK, CHUNK), CHUNK)
        held = all_v.at[chunks + c]
        copies = [
            pltpu.make_async_copy(wg_hbm.at[0, :, cols], held.at[pl.ds(0, d)], first_sem.at[0, c]),
            pltpu.make_async_copy(wu_hbm.at[0, :, cols], held.at[pl.ds(d, d)], first_sem.at[1, c]),
        ]
        for b in range(d // CHUNK):
            to = held.at[pl.ds(2 * d + b * CHUNK, CHUNK)]
            copies.append(pltpu.make_async_copy(wd_hbm.at[0, cols, pl.ds(b * CHUNK, CHUNK)], to, first_sem.at[2 + b, c]))
        return copies

    def x_tile(t):
        where = pl.ds(pl.multiple_of(t * FWD, FWD), FWD)
        return pltpu.make_async_copy(x_hbm.at[where], h_v.at[where], in_sem.at[0, t])

    def dy_tile(t):
        where = pl.ds(pl.multiple_of(t * FWD, FWD), FWD)
        return pltpu.make_async_copy(dy_hbm.at[where], dy_v.at[where], in_sem.at[1, t])

    steps = tokens // FWD
    x_tile(0).start()
    for c in range(chunks):
        for copy in first_weights(c):
            copy.start()

    def load_tiles(t, _):
        dy_tile(t).start()

        @pl.when(t > 0)
        def _():
            x_tile(t).start()

        return 0

    lax.fori_loop(0, steps, load_tiles, 0)
    for copy in weights(0):
        copy.start()
    ss_v[...] = jnp.zeros_like(ss_v)

    def tile_at(t):
        return pl.ds(pl.multiple_of(t * FWD, FWD), FWD)

    def after_forward(t):
        a = normed(h_v[tile_at(t), :])
        a_v[tile_at(t), :] = a
        at_v[:, tile_at(t)] = a.T
        dyt_v[:, tile_at(t)] = dy_v[tile_at(t), :].T

    def forward(t, _):
        after = jnp.minimum(t + 1, steps - 1)
        slot = lax.rem(t, 2) * chunks
        dy_tile(t).wait()

        @pl.when(t + 1 < steps)
        def _():
            x_tile(after).wait()

        @pl.when(t >= 2)
        def _():
            keep(t - 2).wait()

        a = a_v[tile_at(t), :]
        after_forward(jnp.maximum(t - 1, 0))
        a_v[tile_at(after), :] = normed(h_v[tile_at(after), :])
        sums = [None] * (d // CHUNK)
        for c in range(0, chunks, 2):
            ps = []
            for b in range(2):
                gate = dot(a, all_v[chunks + c + b, :d, :])
                up = dot(a, all_v[chunks + c + b, d : 2 * d, :])
                da_v[slot + c + b, :, :CHUNK] = gate
                da_v[slot + c + b, :, CHUNK:] = up
                ps.append((gate * sigmoid(gate) * up).astype(BF16))
            p = jnp.concatenate(ps, 1)
            for b in range(d // CHUNK):
                at = 2 * d + b * CHUNK
                term = dot(p, all_v[chunks + c : chunks + c + 2, at : at + CHUNK, :].reshape(2 * CHUNK, CHUNK))
                sums[b] = term if sums[b] is None else sums[b] + term
        out = jnp.concatenate(sums, 1).astype(BF16)
        h_v[tile_at(t), :] = (h_v[tile_at(t), :].astype(F32) + out.astype(F32)).astype(BF16)
        keep(t).start()
        return 0

    x_tile(0).wait()
    a_v[tile_at(0), :] = normed(h_v[tile_at(0), :])
    for c in range(chunks):
        for copy in first_weights(c):
            copy.wait()
    lax.fori_loop(0, steps, forward, 0)
    after_forward(steps - 1)
    for t in (steps - 2, steps - 1):
        keep(t).wait()

    def clear(t, _):
        da_v[t] = jnp.zeros((FWD, d), F32)
        return 0

    lax.fori_loop(0, steps, clear, 0)
    lax.fori_loop(0, chunks, lambda i, _: chunk(i, True), 0)

    load = pltpu.make_async_copy(x_hbm, a_v, again_sem)
    load.start()

    def through_norm(t, _):
        where = pl.ds(pl.multiple_of(t * FTILE, FTILE), FTILE)
        wide = h_v[where, :].astype(F32)
        scale = scale_of(wide)
        g = da_v[pl.ds(t * (FTILE // FWD), FTILE // FWD)].reshape(FTILE, d).astype(BF16).astype(F32)
        along = jnp.sum(g * wide, -1, keepdims=True)
        dh = (scale * g - wide * (scale * scale * scale * along * (1.0 / d))).astype(BF16)
        dy = (dy_v[where, :].astype(F32) + dh.astype(F32)).astype(BF16)
        dy_v[where, :] = dy
        dyt_v[:, where] = dy.T
        return 0

    lax.fori_loop(0, tokens // FTILE, through_norm, 0)
    for at in range(AHEAD):
        kept(at).start()
    lax.fori_loop(chunks, chunks + 1, drain, 0)
    load.wait()

    def prepare_first(t, _):
        where = pl.ds(pl.multiple_of(t * FTILE, FTILE), FTILE)
        at_v[:, where] = normed(a_v[where, :]).T
        return 0

    lax.fori_loop(0, tokens // FTILE, prepare_first, 0)
    lax.fori_loop(chunks + 1, total + 1, lambda i, _: chunk(i, False), 0)

    lax.fori_loop(total + 1, total + lag + 1, drain, 0)

    ssall_v[me] = ss_v[...]

    def squares(i, peer):
        return pltpu.make_async_remote_copy(
            src_ref=ss_v, dst_ref=ssall_v.at[me], send_sem=ss_send.at[i], recv_sem=ss_recv.at[i],
            device_id={"dp": peer}, device_id_type=MESH_ID,
        )

    sends = [squares(i, peer) for i, peer in enumerate((right, left, opposite))]
    for copy in sends:
        copy.start()

    def finish(k, _):
        out_mine(k + chunks).wait()
        for which in range(2):
            out_shard(k + chunks, which).wait()
        return 0

    lax.fori_loop(0, chunks, finish, 0)

    def finish_pair(p, _):
        out(p).wait()
        return 0

    lax.fori_loop(0, chunks // 2, finish_pair, 0)
    for copy in sends:
        copy.wait()
    squares_sum = ssall_v[0]
    for j in range(1, n):
        squares_sum = squares_sum + ssall_v[j]
    ss_out[...] = squares_sum


def train(n, x, dy, wg, wu, wd):
    tokens, d = x.shape
    ff = wg.shape[2]
    chunks = ff // CHUNK
    rows = 3 * d
    assert d == 2 * CHUNK and tokens % TILE == 0 and TILE // FWD * (AHEAD + 1) <= tokens // FWD
    anywhere = pl.BlockSpec(memory_space=pl.ANY)
    dma = pltpu.SemaphoreType.DMA
    return pl.pallas_call(
        functools.partial(train_kernel, n),
        out_shape=(
            jax.ShapeDtypeStruct((2 * chunks, rows, CHUNK), BF16),
            jax.ShapeDtypeStruct((chunks, rows // n // 2, CHUNK), BF16),
            jax.ShapeDtypeStruct((chunks, rows // n // 2, CHUNK), BF16),
            jax.ShapeDtypeStruct((8, CHUNK), F32),
            jax.ShapeDtypeStruct((tokens // FWD, chunks, FWD, 2 * CHUNK), F32),
        ),
        in_specs=[anywhere] * 5,
        out_specs=(anywhere, anywhere, anywhere, pl.BlockSpec(memory_space=pltpu.VMEM), anywhere),
        scratch_shapes=[
            pltpu.VMEM((tokens, d), BF16),
            pltpu.VMEM((tokens, d), BF16),
            pltpu.VMEM((d, tokens), BF16),
            pltpu.VMEM((tokens, d), BF16),
            pltpu.VMEM((d, tokens), BF16),
            pltpu.VMEM((tokens // FWD, FWD, d), F32),
            pltpu.VMEM((2, d, 2 * CHUNK), BF16),
            pltpu.VMEM((2, CHUNK, d), BF16),
            pltpu.VMEM((d, 2 * CHUNK), F32),
            pltpu.VMEM((d, CHUNK), F32),
            pltpu.VMEM((OWN, rows, CHUNK), BF16),
            pltpu.VMEM((2 * chunks, rows, CHUNK), BF16),
            pltpu.VMEM((2 * chunks, rows // n, CHUNK), BF16),
            pltpu.VMEM((8, CHUNK), F32),
            pltpu.VMEM((n, 8, CHUNK), F32),
            dma((2, tokens // FWD)),
            dma,
            dma((2 + AHEAD + 1,)),
            dma((2 + d // CHUNK, chunks)),
            dma((2, 3)),
            dma((4, 2, 2 * chunks)),
            dma((4, 2, 2 * chunks)),
            dma((3, 2 * chunks)),
            dma((3,)),
            dma((3,)),
        ],
        compiler_params=pltpu.CompilerParams(collective_id=0, has_side_effects=True, vmem_limit_bytes=VMEM_LIMIT),
        cost_estimate=pl.CostEstimate(flops=30 * tokens * d * ff, bytes_accessed=12 * tokens * d + 16 * tokens * ff + 24 * d * ff, transcendentals=3 * tokens * ff),
        name="train",
    )(x, dy, wg, wu, wd)


def update_kernel(count, sources, first, unit, me_ref, ss_ref, *refs):
    source = unit(pl.program_id(0), me_ref[0])[3]
    g_refs = []
    for parts in sources:
        g_refs.append(refs[:parts])
        refs = refs[parts:]
    w_refs, m_refs, v_refs = refs[:3], refs[3:6], refs[6:9]
    outs = refs[9:] if first else refs[18:]
    factor = jnp.minimum(1.0, 0.5 * lax.rsqrt(jnp.sum(ss_ref[...], keepdims=True) / count + 1e-30))
    pr, pd = w_refs[0].shape[1], w_refs[2].shape[3]

    def rows(halves, i, lo, hi):
        half = halves[0].shape[1]
        if hi <= half:
            return halves[0][i, lo:hi, :]
        if lo >= half:
            return halves[1][i, lo - half : hi - half, :]
        return jnp.concatenate([halves[0][i, lo:half, :], halves[1][i, 0 : hi - half, :]], 0)

    def step(which, at, g):
        g = g.astype(F32) * factor
        m = 0.9 * m_refs[which][at] + 0.1 * g
        v = 0.95 * v_refs[which][at] + 0.05 * g * g
        w = w_refs[which][at].astype(F32)
        outs[which][at] = (w - 0.02 * (m * lax.rsqrt(v + 1e-8) + 0.1 * w)).astype(BF16)
        outs[3 + which][at] = m
        outs[6 + which][at] = v

    for number, halves in enumerate(g_refs):

        @pl.when(source == number)
        def _(halves=halves):
            for i in range(halves[0].shape[0]):
                cols = slice(i * CHUNK, (i + 1) * CHUNK)
                for which in range(2):
                    step(which, (0, slice(None), cols), rows(halves, i, which * pr, (which + 1) * pr))
                for h in range(w_refs[2].shape[4] // CHUNK):
                    at = (0, i, 0, slice(None), slice(h * CHUNK, (h + 1) * CHUNK))
                    step(2, at, rows(halves, i, 2 * pr + h * pd, 2 * pr + (h + 1) * pd))


def update(n, me, units, unit, block, ss, sources, arrays, outs):
    d, ff = arrays[0].shape[1:]
    first = outs is None
    pr, pd = d // n, CHUNK // n
    count = sum(a.size for a in arrays[:3])

    def side(u, me_ref):
        layer, b, s, _, _ = unit(u, me_ref[0])
        return layer, s, b

    def down(u, me_ref):
        layer, b, s, _, _ = unit(u, me_ref[0])
        return layer, b, s, 0, 0

    def whole_g(u, me_ref):
        _, _, s, _, at = unit(u, me_ref[0])
        return at[0], s, 0

    specs = [pl.BlockSpec((1, pr, block * CHUNK), side)] * 2 + [pl.BlockSpec((1, block, 1, pd, d), down)]
    specs = specs * 3
    g_specs = []
    for i, source in enumerate(sources):
        if len(source) == 1:
            g_specs.append(pl.BlockSpec((block, source[0].shape[1] // n, CHUNK), whole_g))
        else:
            g_specs += [pl.BlockSpec((block, *a.shape[1:]), lambda u, me_ref, i=i: (unit(u, me_ref[0])[4][i], 0, 0)) for a in source]
    gs = [a for source in sources for a in source]
    size = units * 3 * pr * block * CHUNK
    return pl.pallas_call(
        functools.partial(update_kernel, count, tuple(len(source) for source in sources), first, unit),
        out_shape=tuple(jax.ShapeDtypeStruct(a.shape, a.dtype) for a in arrays),
        grid_spec=pltpu.PrefetchScalarGridSpec(
            num_scalar_prefetch=1,
            grid=(units,),
            in_specs=[pl.BlockSpec(ss.shape, lambda u, me_ref: (0, 0)), *g_specs, *specs]
            + ([] if first else [pl.BlockSpec(memory_space=pl.ANY)] * 9),
            out_specs=tuple(specs),
        ),
        input_output_aliases={} if first else {2 + len(gs) + 9 + i: i for i in range(9)},
        compiler_params=pltpu.CompilerParams(vmem_limit_bytes=VMEM_LIMIT),
        cost_estimate=pl.CostEstimate(flops=15 * size, bytes_accessed=22 * size, transcendentals=size),
        name="update",
    )(me, ss, *gs, *arrays, *([] if first else outs))


def solution(mesh):
    n = mesh.shape["dp"]
    assert n == 4

    def step(x, dy, *arrays):
        x, dy = x.reshape(x.shape[1:]), dy.reshape(dy.shape[1:])
        wg, wu, wd = arrays[:3]
        gathered, half_a, half_b, ss, _ = train(n, x, dy, wg, wu, wd)

        to_right = [(i, (i + 1) % n) for i in range(n)]
        to_left = [(i, (i + n - 1) % n) for i in range(n)]
        left_b = lax.ppermute(half_b, "dp", to_right)
        right_a = lax.ppermute(half_a, "dp", to_left)
        left_a = lax.ppermute(half_a, "dp", to_right)
        right_b = lax.ppermute(half_b, "dp", to_left)

        layers, ff, d = wd.shape
        chunks = ff // CHUNK
        cut = (layers, chunks, n, CHUNK // n, d)
        views = [a.reshape(cut) if i % 3 == 2 else a for i, a in enumerate(arrays)]
        me = lax.axis_index("dp").astype(jnp.int32).reshape(1)

        blocks = chunks // 4

        def unit(u, me, blocks=blocks):
            mine = u >= blocks * n
            b = jnp.where(mine, u - blocks * n, u // n)
            return jnp.where(mine, 0, 1), b, jnp.where(mine, me, u % n), 0, (jnp.where(mine, blocks + b, b),)

        outs = update(n, me, blocks * (n + 1), unit, 4, ss, ((gathered,),), views, None)
        left_b, right_a, outs = lax.optimization_barrier((left_b, right_a, outs))
        far_b = lax.ppermute(left_b, "dp", to_right)
        far_a = lax.ppermute(right_a, "dp", to_left)

        def unit(u, me, blocks=blocks):
            on_right = u >= blocks
            b = jnp.where(on_right, u - blocks, u)
            shard = (me + jnp.where(on_right, 1, n - 1)) % n
            return 0, b, shard, jnp.where(on_right, 1, 0), (jnp.where(on_right, blocks - 1, b), jnp.where(on_right, b, 0))

        outs = update(n, me, 2 * blocks, unit, 4, ss, ((left_a, left_b), (right_a, right_b)), views, outs)

        def unit(u, me):
            return 0, u, (me + 2) % n, 0, (u,)

        outs = update(n, me, chunks // 2, unit, 2, ss, ((far_a, far_b),), views, outs)
        return tuple(o.reshape(a.shape) for o, a in zip(outs, arrays, strict=True))

    return jax.shard_map(
        step,
        mesh=mesh,
        in_specs=(P(("rep", "dp"), None, None),) * 2 + (P(None, None, None),) * 9,
        out_specs=(P("rep", None, None),) * 9,
        check_vma=False,
    )
```

```python
import functools

import jax
import jax.numpy as jnp
from jax import lax
from jax.experimental import pallas as pl
from jax.experimental.pallas import tpu as pltpu
from jax.sharding import PartitionSpec as P

F32, BF16 = jnp.float32, jnp.bfloat16
CHUNK = 256
TILE = 1024
FWD = 256
FTILE = 512
AHEAD = 3
OWN = 4
VMEM_LIMIT = 67_043_328
MESH_ID = pl.DeviceIdType.MESH


def dot(a, b):
    return jnp.dot(a, b, preferred_element_type=F32)


def dot_t(a, b):
    return lax.dot_general(a, b, (((1,), (1,)), ((), ())), preferred_element_type=F32)


def sigmoid(x):
    return 0.5 * jnp.tanh(0.5 * x) + 0.5


def scale_of(wide):
    return lax.rsqrt(jnp.mean(wide * wide, -1, keepdims=True) + 1e-6)


def normed(h):
    wide = h.astype(F32)
    return (wide * scale_of(wide)).astype(BF16)


def train_kernel(n, x_hbm, dy_hbm, wg_hbm, wu_hbm, wd_hbm, g_out, sa_out, sb_out, ss_out, kept_hbm,
                 h_v, a_v, at_v, dy_v, dyt_v, da_v, w_v, wd_v, gu_v, gd_v, own_v, all_v, left_v, ss_v, ssall_v,
                 in_sem, again_sem, kept_sem, first_sem, w_sem, send_sem, recv_sem, out_sem, ss_send, ss_recv):
    tokens, d = h_v.shape
    chunks = wg_hbm.shape[2] // CHUNK
    total = 2 * chunks
    rows = own_v.shape[1]
    shard, half = rows // n, rows // n // 2
    pr, pd = d // n, CHUNK // n
    me = lax.axis_index("dp")
    right, left, opposite = lax.rem(me + 1, n), lax.rem(me + n - 1, n), lax.rem(me + 2, n)

    barrier = pltpu.get_barrier_semaphore()
    for peer in (left, right, opposite):
        pl.semaphore_signal(barrier, inc=1, device_id={"dp": peer}, device_id_type=MESH_ID)
    pl.semaphore_wait(barrier, 3)

    def part(j, which=None):
        if which is None:
            return pl.ds(pl.multiple_of(j * shard, half), shard)
        return pl.ds(pl.multiple_of(j * shard + which * half, half), half)

    def weights(k):
        layer, c, slot = 1 - k // chunks, lax.rem(k, chunks), lax.rem(k, 2)
        cols = pl.ds(pl.multiple_of(c * CHUNK, CHUNK), CHUNK)
        return (
            pltpu.make_async_copy(wg_hbm.at[layer, :, cols], w_v.at[slot, :, pl.ds(0, CHUNK)], w_sem.at[slot, 0]),
            pltpu.make_async_copy(wu_hbm.at[layer, :, cols], w_v.at[slot, :, pl.ds(CHUNK, CHUNK)], w_sem.at[slot, 1]),
            pltpu.make_async_copy(wd_hbm.at[layer, cols, :], wd_v.at[slot], w_sem.at[slot, 2]),
        )

    def remote(kind, way, k, src, dst):
        return pltpu.make_async_remote_copy(
            src_ref=src, dst_ref=dst, send_sem=send_sem.at[kind, way, k], recv_sem=recv_sem.at[kind, way, k],
            device_id={"dp": (left, right)[way]}, device_id_type=MESH_ID,
        )

    def first(way, k):
        where = part(opposite, way)
        return remote(0, way, k, own_v.at[lax.rem(k, OWN), where], all_v.at[k, where])

    def second(way, k):
        where = part((left, right)[way])
        return remote(1, way, k, own_v.at[lax.rem(k, OWN), where], all_v.at[k, where] if way == 0 else left_v.at[k])

    def third(way, k):
        return remote(2, way, k, all_v.at[k, part(me)], all_v.at[k, part(me)])

    def fourth(way, k):
        where = part((right, left)[way], way)
        return remote(3, way, k, all_v.at[k, where], all_v.at[k, where])

    def out(k):
        return pltpu.make_async_copy(all_v.at[k], g_out.at[k], out_sem.at[0, k])

    def out_mine(k):
        return pltpu.make_async_copy(all_v.at[k, part(me)], g_out.at[k, part(me)], out_sem.at[0, k])

    def out_shard(k, which):
        return pltpu.make_async_copy(all_v.at[k, part(me, which)], (sa_out, sb_out)[which].at[k - chunks], out_sem.at[1 + which, k])

    def chunk_at(i):
        return jnp.where(i > chunks, i - 1, i)

    def alive(i):
        return (i >= 0) & (i <= total) & (i != chunks)

    def gather_at(i):
        return chunk_at(i - lag), alive(i - lag) & (i - lag < chunks)

    lag = 2

    def exchange(i):
        @pl.when(alive(i - 1))
        def _():
            q = chunk_at(i - 1)
            slot = lax.rem(q, OWN)
            for way in range(2):
                first(way, q).wait_recv()
            for j, which in ((left, 0), (right, 1)):
                where = part(j, which)
                own_v[slot, where, :] = (own_v[slot, where, :].astype(F32) + all_v[q, where, :].astype(F32)).astype(BF16)

        @pl.when(alive(i))
        def _():
            for way in range(2):
                first(way, chunk_at(i)).start()

        @pl.when(alive(i - lag))
        def _():
            q = chunk_at(i - lag)
            slot = lax.rem(q, OWN)
            for way in range(2):
                second(way, q).wait_recv()
            mine = part(me)
            g = own_v[slot, mine, :].astype(F32) + all_v[q, mine, :].astype(F32) + left_v[q].astype(F32)
            g = g.astype(BF16)
            all_v[q, mine, :] = g
            wide = g.astype(F32)
            ss_v[...] += jnp.sum((wide * wide).reshape(shard // 8, 8, CHUNK), 0)

        @pl.when(alive(i - 1))
        def _():
            for way in range(2):
                second(way, chunk_at(i - 1)).start()

        g2, go2 = gather_at(i - 2)

        @pl.when(go2)
        def _():
            for way in range(2):
                third(way, g2).wait_recv()
            for way in range(2):
                fourth(way, g2).start()

        g1, go1 = gather_at(i)

        @pl.when(go1)
        def _():
            for way in range(2):
                third(way, g1).start()

        @pl.when(alive(i - lag) & (chunk_at(i - lag) >= chunks))
        def _():
            q = chunk_at(i - lag)
            for which in range(2):
                out_shard(q, which).start()
            out_mine(q).start()

        @pl.when(alive(i - 3))
        def _():
            for way in range(2):
                first(way, chunk_at(i - 3)).wait_send()
                second(way, chunk_at(i - 3)).wait_send()

        g3, go3 = gather_at(i - 4)

        @pl.when(go3)
        def _():
            for way in range(2):
                third(way, g3).wait_send()
                fourth(way, g3).wait_send()
                fourth(way, g3).wait_recv()
            out(g3).start()

    tiles, per = tokens // TILE, TILE // FWD

    def keep(t):
        slot = lax.rem(t, 2) * chunks
        return pltpu.make_async_copy(da_v.at[pl.ds(slot, chunks)], kept_hbm.at[t], kept_sem.at[lax.rem(t, 2)])

    def kept(at):
        slot = lax.rem(at, AHEAD + 1)
        where = pl.ds(lax.rem(at, tiles) * per, per)
        return pltpu.make_async_copy(kept_hbm.at[where, at // tiles], da_v.at[pl.ds(slot * per, per)], kept_sem.at[2 + slot])

    def chunk(i, last_layer):
        k = i if last_layer else i - 1
        slot = lax.rem(k, 2)

        @pl.when(k + 1 < total)
        def _():
            for copy in weights(k + 1):
                copy.start()

        for copy in weights(k):
            copy.wait()
        gu_v[...] = jnp.zeros_like(gu_v)
        gd_v[...] = jnp.zeros_like(gd_v)

        def tile(t, _):
            where = pl.ds(pl.multiple_of(t * TILE, TILE), TILE)
            if last_layer:
                w = w_v[slot]
                both = dot(a_v[where, :], w)
            else:
                at = (k - chunks) * tiles + t

                @pl.when(at + AHEAD < chunks * tiles)
                def _():
                    kept(at + AHEAD).start()

                kept(at).wait()
                both = da_v[pl.ds(lax.rem(at, AHEAD + 1) * per, per)].reshape(TILE, 2 * CHUNK)
            dp = dot_t(dy_v[where, :], wd_v[slot]).astype(BF16).astype(F32)
            gate, up = both[:, :CHUNK], both[:, CHUNK:]
            s = sigmoid(gate)
            act = gate * s
            p = (act * up).astype(BF16)
            gd_v[...] += dot(dyt_v[:, where], p)
            dgate = (dp * up * (s + act * (1.0 - s))).astype(BF16)
            dup = (dp * act).astype(BF16)
            dboth = jnp.concatenate([dgate, dup], 1)
            gu_v[...] += dot(at_v[:, where], dboth)
            if last_layer:
                da_v[pl.ds(t * per, per)] += dot_t(dboth, w).reshape(per, FWD, d)
            return 0

        lax.fori_loop(0, tokens // TILE, tile, 0)
        o = lax.rem(k, OWN)
        down = gd_v[...].T
        for j in range(n):
            own_v[o, j * shard : j * shard + pr, :] = gu_v[j * pr : (j + 1) * pr, :CHUNK].astype(BF16)
            own_v[o, j * shard + pr : j * shard + 2 * pr, :] = gu_v[j * pr : (j + 1) * pr, CHUNK:].astype(BF16)
            for b in range(d // CHUNK):
                at = j * shard + 2 * pr + b * pd
                own_v[o, at : at + pd, :] = down[j * pd : (j + 1) * pd, b * CHUNK : (b + 1) * CHUNK].astype(BF16)
        exchange(i)
        return 0

    def drain(i, _):
        exchange(i)
        return 0

    def first_weights(c):
        cols = pl.ds(pl.multiple_of(c * CHUNK, CHUNK), CHUNK)
        held = all_v.at[chunks + c]
        copies = [
            pltpu.make_async_copy(wg_hbm.at[0, :, cols], held.at[pl.ds(0, d)], first_sem.at[0, c]),
            pltpu.make_async_copy(wu_hbm.at[0, :, cols], held.at[pl.ds(d, d)], first_sem.at[1, c]),
        ]
        for b in range(d // CHUNK):
            to = held.at[pl.ds(2 * d + b * CHUNK, CHUNK)]
            copies.append(pltpu.make_async_copy(wd_hbm.at[0, cols, pl.ds(b * CHUNK, CHUNK)], to, first_sem.at[2 + b, c]))
        return copies

    def x_tile(t):
        where = pl.ds(pl.multiple_of(t * FWD, FWD), FWD)
        return pltpu.make_async_copy(x_hbm.at[where], h_v.at[where], in_sem.at[0, t])

    def dy_tile(t):
        where = pl.ds(pl.multiple_of(t * FWD, FWD), FWD)
        return pltpu.make_async_copy(dy_hbm.at[where], dy_v.at[where], in_sem.at[1, t])

    steps = tokens // FWD
    x_tile(0).start()
    for c in range(chunks):
        for copy in first_weights(c):
            copy.start()

    def load_tiles(t, _):
        dy_tile(t).start()

        @pl.when(t > 0)
        def _():
            x_tile(t).start()

        return 0

    lax.fori_loop(0, steps, load_tiles, 0)
    for copy in weights(0):
        copy.start()
    ss_v[...] = jnp.zeros_like(ss_v)

    def tile_at(t):
        return pl.ds(pl.multiple_of(t * FWD, FWD), FWD)

    def after_forward(t):
        a = normed(h_v[tile_at(t), :])
        a_v[tile_at(t), :] = a
        at_v[:, tile_at(t)] = a.T
        dyt_v[:, tile_at(t)] = dy_v[tile_at(t), :].T

    def forward(t, _):
        after = jnp.minimum(t + 1, steps - 1)
        slot = lax.rem(t, 2) * chunks
        dy_tile(t).wait()

        @pl.when(t + 1 < steps)
        def _():
            x_tile(after).wait()

        @pl.when(t >= 2)
        def _():
            keep(t - 2).wait()

        a = a_v[tile_at(t), :]
        after_forward(jnp.maximum(t - 1, 0))
        a_v[tile_at(after), :] = normed(h_v[tile_at(after), :])
        sums = [None] * (d // CHUNK)
        for c in range(0, chunks, 2):
            ps = []
            for b in range(2):
                gate = dot(a, all_v[chunks + c + b, :d, :])
                up = dot(a, all_v[chunks + c + b, d : 2 * d, :])
                da_v[slot + c + b, :, :CHUNK] = gate
                da_v[slot + c + b, :, CHUNK:] = up
                ps.append((gate * sigmoid(gate) * up).astype(BF16))
            p = jnp.concatenate(ps, 1)
            for b in range(d // CHUNK):
                at = 2 * d + b * CHUNK
                term = dot(p, all_v[chunks + c : chunks + c + 2, at : at + CHUNK, :].reshape(2 * CHUNK, CHUNK))
                sums[b] = term if sums[b] is None else sums[b] + term
        out = jnp.concatenate(sums, 1).astype(BF16)
        h_v[tile_at(t), :] = (h_v[tile_at(t), :].astype(F32) + out.astype(F32)).astype(BF16)
        keep(t).start()
        return 0

    x_tile(0).wait()
    a_v[tile_at(0), :] = normed(h_v[tile_at(0), :])
    for c in range(chunks):
        for copy in first_weights(c):
            copy.wait()
    lax.fori_loop(0, steps, forward, 0)
    after_forward(steps - 1)
    for t in (steps - 2, steps - 1):
        keep(t).wait()

    def clear(t, _):
        da_v[t] = jnp.zeros((FWD, d), F32)
        return 0

    lax.fori_loop(0, steps, clear, 0)
    lax.fori_loop(0, chunks, lambda i, _: chunk(i, True), 0)

    load = pltpu.make_async_copy(x_hbm, a_v, again_sem)
    load.start()

    def through_norm(t, _):
        where = pl.ds(pl.multiple_of(t * FTILE, FTILE), FTILE)
        wide = h_v[where, :].astype(F32)
        scale = scale_of(wide)
        g = da_v[pl.ds(t * (FTILE // FWD), FTILE // FWD)].reshape(FTILE, d).astype(BF16).astype(F32)
        along = jnp.sum(g * wide, -1, keepdims=True)
        dh = (scale * g - wide * (scale * scale * scale * along * (1.0 / d))).astype(BF16)
        dy = (dy_v[where, :].astype(F32) + dh.astype(F32)).astype(BF16)
        dy_v[where, :] = dy
        dyt_v[:, where] = dy.T
        return 0

    lax.fori_loop(0, tokens // FTILE, through_norm, 0)
    for at in range(AHEAD):
        kept(at).start()
    lax.fori_loop(chunks, chunks + 1, drain, 0)
    load.wait()

    def prepare_first(t, _):
        where = pl.ds(pl.multiple_of(t * FTILE, FTILE), FTILE)
        at_v[:, where] = normed(a_v[where, :]).T
        return 0

    lax.fori_loop(0, tokens // FTILE, prepare_first, 0)
    lax.fori_loop(chunks + 1, total + 1, lambda i, _: chunk(i, False), 0)

    lax.fori_loop(total + 1, total + 4, drain, 0)

    ssall_v[me] = ss_v[...]

    def squares(i, peer):
        return pltpu.make_async_remote_copy(
            src_ref=ss_v, dst_ref=ssall_v.at[me], send_sem=ss_send.at[i], recv_sem=ss_recv.at[i],
            device_id={"dp": peer}, device_id_type=MESH_ID,
        )

    sends = [squares(i, peer) for i, peer in enumerate((right, left, opposite))]
    for copy in sends:
        copy.start()

    def finish(k, _):
        out_mine(k + chunks).wait()
        for which in range(2):
            out_shard(k + chunks, which).wait()
        return 0

    lax.fori_loop(0, chunks, finish, 0)

    def finish_pair(p, _):
        out(p).wait()
        return 0

    lax.fori_loop(0, chunks, finish_pair, 0)
    for copy in sends:
        copy.wait()
    squares_sum = ssall_v[0]
    for j in range(1, n):
        squares_sum = squares_sum + ssall_v[j]
    ss_out[...] = squares_sum


def train(n, x, dy, wg, wu, wd):
    tokens, d = x.shape
    ff = wg.shape[2]
    chunks = ff // CHUNK
    rows = 3 * d
    assert d == 2 * CHUNK and tokens % TILE == 0 and TILE // FWD * (AHEAD + 1) <= tokens // FWD
    anywhere = pl.BlockSpec(memory_space=pl.ANY)
    dma = pltpu.SemaphoreType.DMA
    return pl.pallas_call(
        functools.partial(train_kernel, n),
        out_shape=(
            jax.ShapeDtypeStruct((2 * chunks, rows, CHUNK), BF16),
            jax.ShapeDtypeStruct((chunks, rows // n // 2, CHUNK), BF16),
            jax.ShapeDtypeStruct((chunks, rows // n // 2, CHUNK), BF16),
            jax.ShapeDtypeStruct((8, CHUNK), F32),
            jax.ShapeDtypeStruct((tokens // FWD, chunks, FWD, 2 * CHUNK), F32),
        ),
        in_specs=[anywhere] * 5,
        out_specs=(anywhere, anywhere, anywhere, pl.BlockSpec(memory_space=pltpu.VMEM), anywhere),
        scratch_shapes=[
            pltpu.VMEM((tokens, d), BF16),
            pltpu.VMEM((tokens, d), BF16),
            pltpu.VMEM((d, tokens), BF16),
            pltpu.VMEM((tokens, d), BF16),
            pltpu.VMEM((d, tokens), BF16),
            pltpu.VMEM((tokens // FWD, FWD, d), F32),
            pltpu.VMEM((2, d, 2 * CHUNK), BF16),
            pltpu.VMEM((2, CHUNK, d), BF16),
            pltpu.VMEM((d, 2 * CHUNK), F32),
            pltpu.VMEM((d, CHUNK), F32),
            pltpu.VMEM((OWN, rows, CHUNK), BF16),
            pltpu.VMEM((2 * chunks, rows, CHUNK), BF16),
            pltpu.VMEM((2 * chunks, rows // n, CHUNK), BF16),
            pltpu.VMEM((8, CHUNK), F32),
            pltpu.VMEM((n, 8, CHUNK), F32),
            dma((2, tokens // FWD)),
            dma,
            dma((2 + AHEAD + 1,)),
            dma((2 + d // CHUNK, chunks)),
            dma((2, 3)),
            dma((4, 2, 2 * chunks)),
            dma((4, 2, 2 * chunks)),
            dma((3, 2 * chunks)),
            dma((3,)),
            dma((3,)),
        ],
        compiler_params=pltpu.CompilerParams(collective_id=0, has_side_effects=True, vmem_limit_bytes=VMEM_LIMIT),
        cost_estimate=pl.CostEstimate(flops=30 * tokens * d * ff, bytes_accessed=12 * tokens * d + 16 * tokens * ff + 24 * d * ff, transcendentals=3 * tokens * ff),
        name="train",
    )(x, dy, wg, wu, wd)


def update_kernel(count, sources, first, unit, me_ref, ss_ref, *refs):
    source = unit(pl.program_id(0), me_ref[0])[3]
    g_refs = []
    for parts in sources:
        g_refs.append(refs[:parts])
        refs = refs[parts:]
    w_refs, m_refs, v_refs = refs[:3], refs[3:6], refs[6:9]
    outs = refs[9:] if first else refs[18:]
    factor = jnp.minimum(1.0, 0.5 * lax.rsqrt(jnp.sum(ss_ref[...], keepdims=True) / count + 1e-30))
    pr, pd = w_refs[0].shape[1], w_refs[2].shape[3]

    def rows(halves, i, lo, hi):
        half = halves[0].shape[1]
        if hi <= half:
            return halves[0][i, lo:hi, :]
        if lo >= half:
            return halves[1][i, lo - half : hi - half, :]
        return jnp.concatenate([halves[0][i, lo:half, :], halves[1][i, 0 : hi - half, :]], 0)

    def step(which, at, g):
        g = g.astype(F32) * factor
        m = 0.9 * m_refs[which][at] + 0.1 * g
        v = 0.95 * v_refs[which][at] + 0.05 * g * g
        w = w_refs[which][at].astype(F32)
        outs[which][at] = (w - 0.02 * (m * lax.rsqrt(v + 1e-8) + 0.1 * w)).astype(BF16)
        outs[3 + which][at] = m
        outs[6 + which][at] = v

    for number, halves in enumerate(g_refs):

        @pl.when(source == number)
        def _(halves=halves):
            for i in range(halves[0].shape[0]):
                cols = slice(i * CHUNK, (i + 1) * CHUNK)
                for which in range(2):
                    step(which, (0, slice(None), cols), rows(halves, i, which * pr, (which + 1) * pr))
                for h in range(w_refs[2].shape[4] // CHUNK):
                    at = (0, i, 0, slice(None), slice(h * CHUNK, (h + 1) * CHUNK))
                    step(2, at, rows(halves, i, 2 * pr + h * pd, 2 * pr + (h + 1) * pd))


def update(n, me, units, unit, block, ss, sources, arrays, outs):
    d, ff = arrays[0].shape[1:]
    first = outs is None
    pr, pd = d // n, CHUNK // n
    count = sum(a.size for a in arrays[:3])

    def side(u, me_ref):
        layer, b, s, _, _ = unit(u, me_ref[0])
        return layer, s, b

    def down(u, me_ref):
        layer, b, s, _, _ = unit(u, me_ref[0])
        return layer, b, s, 0, 0

    def whole_g(u, me_ref):
        _, _, s, _, at = unit(u, me_ref[0])
        return at[0], s, 0

    specs = [pl.BlockSpec((1, pr, block * CHUNK), side)] * 2 + [pl.BlockSpec((1, block, 1, pd, d), down)]
    specs = specs * 3
    g_specs = []
    for i, source in enumerate(sources):
        if len(source) == 1:
            g_specs.append(pl.BlockSpec((block, source[0].shape[1] // n, CHUNK), whole_g))
        else:
            g_specs += [pl.BlockSpec((block, *a.shape[1:]), lambda u, me_ref, i=i: (unit(u, me_ref[0])[4][i], 0, 0)) for a in source]
    gs = [a for source in sources for a in source]
    size = units * 3 * pr * block * CHUNK
    return pl.pallas_call(
        functools.partial(update_kernel, count, tuple(len(source) for source in sources), first, unit),
        out_shape=tuple(jax.ShapeDtypeStruct(a.shape, a.dtype) for a in arrays),
        grid_spec=pltpu.PrefetchScalarGridSpec(
            num_scalar_prefetch=1,
            grid=(units,),
            in_specs=[pl.BlockSpec(ss.shape, lambda u, me_ref: (0, 0)), *g_specs, *specs]
            + ([] if first else [pl.BlockSpec(memory_space=pl.ANY)] * 9),
            out_specs=tuple(specs),
        ),
        input_output_aliases={} if first else {2 + len(gs) + 9 + i: i for i in range(9)},
        compiler_params=pltpu.CompilerParams(vmem_limit_bytes=VMEM_LIMIT),
        cost_estimate=pl.CostEstimate(flops=15 * size, bytes_accessed=22 * size, transcendentals=size),
        name="update",
    )(me, ss, *gs, *arrays, *([] if first else outs))


def solution(mesh):
    n = mesh.shape["dp"]
    assert n == 4

    def step(x, dy, *arrays):
        x, dy = x.reshape(x.shape[1:]), dy.reshape(dy.shape[1:])
        wg, wu, wd = arrays[:3]
        gathered, half_a, half_b, ss, _ = train(n, x, dy, wg, wu, wd)

        to_right = [(i, (i + 1) % n) for i in range(n)]
        to_left = [(i, (i + n - 1) % n) for i in range(n)]
        left_b = lax.ppermute(half_b, "dp", to_right)
        right_a = lax.ppermute(half_a, "dp", to_left)
        left_a = lax.ppermute(half_a, "dp", to_right)
        right_b = lax.ppermute(half_b, "dp", to_left)

        layers, ff, d = wd.shape
        chunks = ff // CHUNK
        cut = (layers, chunks, n, CHUNK // n, d)
        views = [a.reshape(cut) if i % 3 == 2 else a for i, a in enumerate(arrays)]
        me = lax.axis_index("dp").astype(jnp.int32).reshape(1)

        blocks = chunks // 4

        def unit(u, me, blocks=blocks):
            mine = u >= blocks * n
            b = jnp.where(mine, u - blocks * n, u // n)
            return jnp.where(mine, 0, 1), b, jnp.where(mine, me, u % n), 0, (jnp.where(mine, blocks + b, b),)

        outs = update(n, me, blocks * (n + 1), unit, 4, ss, ((gathered,),), views, None)
        left_b, right_a, outs = lax.optimization_barrier((left_b, right_a, outs))
        far_b = lax.ppermute(left_b, "dp", to_right)
        far_a = lax.ppermute(right_a, "dp", to_left)

        def unit(u, me, blocks=blocks):
            on_right = u >= blocks
            b = jnp.where(on_right, u - blocks, u)
            shard = (me + jnp.where(on_right, 1, n - 1)) % n
            return 0, b, shard, jnp.where(on_right, 1, 0), (jnp.where(on_right, blocks - 1, b), jnp.where(on_right, b, 0))

        outs = update(n, me, 2 * blocks, unit, 4, ss, ((left_a, left_b), (right_a, right_b)), views, outs)

        def unit(u, me):
            return 0, u, (me + 2) % n, 0, (u,)

        outs = update(n, me, chunks // 2, unit, 2, ss, ((far_a, far_b),), views, outs)
        return tuple(o.reshape(a.shape) for o, a in zip(outs, arrays, strict=True))

    return jax.shard_map(
        step,
        mesh=mesh,
        in_specs=(P(("rep", "dp"), None, None),) * 2 + (P(None, None, None),) * 9,
        out_specs=(P("rep", None, None),) * 9,
        check_vma=False,
    )
```

```python
import functools

import jax
import jax.numpy as jnp
from jax import lax
from jax.experimental import pallas as pl
from jax.experimental.pallas import tpu as pltpu
from jax.sharding import PartitionSpec as P

F32, BF16 = jnp.float32, jnp.bfloat16
CHUNK = 256
TILE = 1024
FWD = 256
FTILE = 512
AHEAD = 3
OWN = 4
VMEM_LIMIT = 67_043_328
MESH_ID = pl.DeviceIdType.MESH


def dot(a, b):
    return jnp.dot(a, b, preferred_element_type=F32)


def dot_t(a, b):
    return lax.dot_general(a, b, (((1,), (1,)), ((), ())), preferred_element_type=F32)


def sigmoid(x):
    return 0.5 * jnp.tanh(0.5 * x) + 0.5


def scale_of(wide):
    return lax.rsqrt(jnp.mean(wide * wide, -1, keepdims=True) + 1e-6)


def normed(h):
    wide = h.astype(F32)
    return (wide * scale_of(wide)).astype(BF16)


def train_kernel(n, x_hbm, dy_hbm, wg_hbm, wu_hbm, wd_hbm, g_out, sa_out, sb_out, ss_out, kept_hbm,
                 h_v, a_v, at_v, dy_v, dyt_v, da_v, w_v, wd_v, gu_v, gd_v, own_v, all_v, left_v, ss_v, ssall_v,
                 in_sem, again_sem, kept_sem, first_sem, w_sem, send_sem, recv_sem, out_sem, ss_send, ss_recv):
    tokens, d = h_v.shape
    chunks = wg_hbm.shape[2] // CHUNK
    total = 2 * chunks
    rows = own_v.shape[1]
    shard, half = rows // n, rows // n // 2
    pr, pd = d // n, CHUNK // n
    me = lax.axis_index("dp")
    right, left, opposite = lax.rem(me + 1, n), lax.rem(me + n - 1, n), lax.rem(me + 2, n)

    barrier = pltpu.get_barrier_semaphore()
    for peer in (left, right, opposite):
        pl.semaphore_signal(barrier, inc=1, device_id={"dp": peer}, device_id_type=MESH_ID)
    pl.semaphore_wait(barrier, 3)

    def part(j, which=None):
        if which is None:
            return pl.ds(pl.multiple_of(j * shard, half), shard)
        return pl.ds(pl.multiple_of(j * shard + which * half, half), half)

    def weights(k):
        layer, c, slot = 1 - k // chunks, lax.rem(k, chunks), lax.rem(k, 2)
        cols = pl.ds(pl.multiple_of(c * CHUNK, CHUNK), CHUNK)
        return (
            pltpu.make_async_copy(wg_hbm.at[layer, :, cols], w_v.at[slot, :, pl.ds(0, CHUNK)], w_sem.at[slot, 0]),
            pltpu.make_async_copy(wu_hbm.at[layer, :, cols], w_v.at[slot, :, pl.ds(CHUNK, CHUNK)], w_sem.at[slot, 1]),
            pltpu.make_async_copy(wd_hbm.at[layer, cols, :], wd_v.at[slot], w_sem.at[slot, 2]),
        )

    def remote(kind, way, k, src, dst):
        return pltpu.make_async_remote_copy(
            src_ref=src, dst_ref=dst, send_sem=send_sem.at[kind, way, k], recv_sem=recv_sem.at[kind, way, k],
            device_id={"dp": (left, right)[way]}, device_id_type=MESH_ID,
        )

    def first(way, k):
        where = part(opposite, way)
        return remote(0, way, k, own_v.at[lax.rem(k, OWN), where], all_v.at[k, where])

    def second(way, k):
        where = part((left, right)[way])
        return remote(1, way, k, own_v.at[lax.rem(k, OWN), where], all_v.at[k, where] if way == 0 else left_v.at[k])

    def third(way, k):
        return remote(2, way, k, all_v.at[k, part(me)], all_v.at[k, part(me)])

    def fourth(way, k):
        where = part((right, left)[way], way)
        return remote(3, way, k, all_v.at[k, where], all_v.at[k, where])

    def out(k):
        return pltpu.make_async_copy(all_v.at[k], g_out.at[k], out_sem.at[0, k])

    def out_mine(k):
        return pltpu.make_async_copy(all_v.at[k, part(me)], g_out.at[k, part(me)], out_sem.at[0, k])

    def out_shard(k, which):
        return pltpu.make_async_copy(all_v.at[k, part(me, which)], (sa_out, sb_out)[which].at[k - chunks], out_sem.at[1 + which, k])

    def chunk_at(i):
        return jnp.where(i > chunks, i - 1, i)

    def alive(i):
        return (i >= 0) & (i <= total) & (i != chunks)

    def gathered(i):
        return alive(i) & (i < chunks)

    def middle(i):
        @pl.when(alive(i - 1))
        def _():
            q = chunk_at(i - 1)
            slot = lax.rem(q, OWN)
            for way in range(2):
                first(way, q).wait_recv()
            for j, which in ((left, 0), (right, 1)):
                where = part(j, which)
                own_v[slot, where, :] = (own_v[slot, where, :].astype(F32) + all_v[q, where, :].astype(F32)).astype(BF16)

        @pl.when(alive(i - 2))
        def _():
            q = chunk_at(i - 2)
            slot = lax.rem(q, OWN)
            for way in range(2):
                second(way, q).wait_recv()
            mine = part(me)
            g = own_v[slot, mine, :].astype(F32) + all_v[q, mine, :].astype(F32) + left_v[q].astype(F32)
            g = g.astype(BF16)
            all_v[q, mine, :] = g
            wide = g.astype(F32)
            ss_v[...] += jnp.sum((wide * wide).reshape(shard // 8, 8, CHUNK), 0)

        @pl.when(alive(i - 1))
        def _():
            for way in range(2):
                second(way, chunk_at(i - 1)).start()

        @pl.when(gathered(i - 2))
        def _():
            for way in range(2):
                third(way, i - 2).start()

        @pl.when(alive(i - 2) & (i - 2 > chunks))
        def _():
            q = chunk_at(i - 2)
            for which in range(2):
                out_shard(q, which).start()
            out_mine(q).start()

        @pl.when(alive(i - 3))
        def _():
            for way in range(2):
                first(way, chunk_at(i - 3)).wait_send()
                second(way, chunk_at(i - 3)).wait_send()

    def end(i):
        @pl.when(alive(i))
        def _():
            for way in range(2):
                first(way, chunk_at(i)).start()

        @pl.when(gathered(i - 3))
        def _():
            for way in range(2):
                third(way, i - 3).wait_recv()
            for way in range(2):
                fourth(way, i - 3).start()

        @pl.when(gathered(i - 5))
        def _():
            for way in range(2):
                third(way, i - 5).wait_send()
                fourth(way, i - 5).wait_send()
                fourth(way, i - 5).wait_recv()
            out(i - 5).start()

    tiles, per = tokens // TILE, TILE // FWD

    def keep(t):
        slot = lax.rem(t, 2) * chunks
        return pltpu.make_async_copy(da_v.at[pl.ds(slot, chunks)], kept_hbm.at[t], kept_sem.at[lax.rem(t, 2)])

    def kept(at):
        slot = lax.rem(at, AHEAD + 1)
        where = pl.ds(lax.rem(at, tiles) * per, per)
        return pltpu.make_async_copy(kept_hbm.at[where, at // tiles], da_v.at[pl.ds(slot * per, per)], kept_sem.at[2 + slot])

    def chunk(i, last_layer):
        k = i if last_layer else i - 1
        slot = lax.rem(k, 2)

        @pl.when(k + 1 < total)
        def _():
            for copy in weights(k + 1):
                copy.start()

        for copy in weights(k):
            copy.wait()
        gu_v[...] = jnp.zeros_like(gu_v)
        gd_v[...] = jnp.zeros_like(gd_v)

        def tile(t, _):
            @pl.when(t == tiles // 2)
            def _():
                middle(i)

            where = pl.ds(pl.multiple_of(t * TILE, TILE), TILE)
            if last_layer:
                w = w_v[slot]
                both = dot(a_v[where, :], w)
            else:
                at = (k - chunks) * tiles + t

                @pl.when(at + AHEAD < chunks * tiles)
                def _():
                    kept(at + AHEAD).start()

                kept(at).wait()
                both = da_v[pl.ds(lax.rem(at, AHEAD + 1) * per, per)].reshape(TILE, 2 * CHUNK)
            dp = dot_t(dy_v[where, :], wd_v[slot]).astype(BF16).astype(F32)
            gate, up = both[:, :CHUNK], both[:, CHUNK:]
            s = sigmoid(gate)
            act = gate * s
            p = (act * up).astype(BF16)
            gd_v[...] += dot(dyt_v[:, where], p)
            dgate = (dp * up * (s + act * (1.0 - s))).astype(BF16)
            dup = (dp * act).astype(BF16)
            dboth = jnp.concatenate([dgate, dup], 1)
            gu_v[...] += dot(at_v[:, where], dboth)
            if last_layer:
                da_v[pl.ds(t * per, per)] += dot_t(dboth, w).reshape(per, FWD, d)
            return 0

        lax.fori_loop(0, tokens // TILE, tile, 0)
        o = lax.rem(k, OWN)
        down = gd_v[...].T
        for j in range(n):
            own_v[o, j * shard : j * shard + pr, :] = gu_v[j * pr : (j + 1) * pr, :CHUNK].astype(BF16)
            own_v[o, j * shard + pr : j * shard + 2 * pr, :] = gu_v[j * pr : (j + 1) * pr, CHUNK:].astype(BF16)
            for b in range(d // CHUNK):
                at = j * shard + 2 * pr + b * pd
                own_v[o, at : at + pd, :] = down[j * pd : (j + 1) * pd, b * CHUNK : (b + 1) * CHUNK].astype(BF16)
        end(i)
        return 0

    def drain(i, _):
        middle(i)
        end(i)
        return 0

    def first_weights(c):
        cols = pl.ds(pl.multiple_of(c * CHUNK, CHUNK), CHUNK)
        held = all_v.at[chunks + c]
        copies = [
            pltpu.make_async_copy(wg_hbm.at[0, :, cols], held.at[pl.ds(0, d)], first_sem.at[0, c]),
            pltpu.make_async_copy(wu_hbm.at[0, :, cols], held.at[pl.ds(d, d)], first_sem.at[1, c]),
        ]
        for b in range(d // CHUNK):
            to = held.at[pl.ds(2 * d + b * CHUNK, CHUNK)]
            copies.append(pltpu.make_async_copy(wd_hbm.at[0, cols, pl.ds(b * CHUNK, CHUNK)], to, first_sem.at[2 + b, c]))
        return copies

    def x_tile(t):
        where = pl.ds(pl.multiple_of(t * FWD, FWD), FWD)
        return pltpu.make_async_copy(x_hbm.at[where], h_v.at[where], in_sem.at[0, t])

    def dy_tile(t):
        where = pl.ds(pl.multiple_of(t * FWD, FWD), FWD)
        return pltpu.make_async_copy(dy_hbm.at[where], dy_v.at[where], in_sem.at[1, t])

    steps = tokens // FWD
    x_tile(0).start()
    for c in range(chunks):
        for copy in first_weights(c):
            copy.start()

    def load_tiles(t, _):
        dy_tile(t).start()

        @pl.when(t > 0)
        def _():
            x_tile(t).start()

        return 0

    lax.fori_loop(0, steps, load_tiles, 0)
    for copy in weights(0):
        copy.start()
    ss_v[...] = jnp.zeros_like(ss_v)

    def tile_at(t):
        return pl.ds(pl.multiple_of(t * FWD, FWD), FWD)

    def after_forward(t):
        a = normed(h_v[tile_at(t), :])
        a_v[tile_at(t), :] = a
        at_v[:, tile_at(t)] = a.T
        dyt_v[:, tile_at(t)] = dy_v[tile_at(t), :].T

    def forward(t, _):
        after = jnp.minimum(t + 1, steps - 1)
        slot = lax.rem(t, 2) * chunks
        dy_tile(t).wait()

        @pl.when(t + 1 < steps)
        def _():
            x_tile(after).wait()

        @pl.when(t >= 2)
        def _():
            keep(t - 2).wait()

        a = a_v[tile_at(t), :]
        after_forward(jnp.maximum(t - 1, 0))
        a_v[tile_at(after), :] = normed(h_v[tile_at(after), :])
        sums = [None] * (d // CHUNK)
        for c in range(0, chunks, 2):
            ps = []
            for b in range(2):
                gate = dot(a, all_v[chunks + c + b, :d, :])
                up = dot(a, all_v[chunks + c + b, d : 2 * d, :])
                da_v[slot + c + b, :, :CHUNK] = gate
                da_v[slot + c + b, :, CHUNK:] = up
                ps.append((gate * sigmoid(gate) * up).astype(BF16))
            p = jnp.concatenate(ps, 1)
            for b in range(d // CHUNK):
                at = 2 * d + b * CHUNK
                term = dot(p, all_v[chunks + c : chunks + c + 2, at : at + CHUNK, :].reshape(2 * CHUNK, CHUNK))
                sums[b] = term if sums[b] is None else sums[b] + term
        out = jnp.concatenate(sums, 1).astype(BF16)
        h_v[tile_at(t), :] = (h_v[tile_at(t), :].astype(F32) + out.astype(F32)).astype(BF16)
        keep(t).start()
        return 0

    x_tile(0).wait()
    a_v[tile_at(0), :] = normed(h_v[tile_at(0), :])
    for c in range(chunks):
        for copy in first_weights(c):
            copy.wait()
    lax.fori_loop(0, steps, forward, 0)
    after_forward(steps - 1)
    for t in (steps - 2, steps - 1):
        keep(t).wait()

    def clear(t, _):
        da_v[t] = jnp.zeros((FWD, d), F32)
        return 0

    lax.fori_loop(0, steps, clear, 0)
    lax.fori_loop(0, chunks, lambda i, _: chunk(i, True), 0)

    load = pltpu.make_async_copy(x_hbm, a_v, again_sem)
    load.start()

    def through_norm(t, _):
        where = pl.ds(pl.multiple_of(t * FTILE, FTILE), FTILE)
        wide = h_v[where, :].astype(F32)
        scale = scale_of(wide)
        g = da_v[pl.ds(t * (FTILE // FWD), FTILE // FWD)].reshape(FTILE, d).astype(BF16).astype(F32)
        along = jnp.sum(g * wide, -1, keepdims=True)
        dh = (scale * g - wide * (scale * scale * scale * along * (1.0 / d))).astype(BF16)
        dy = (dy_v[where, :].astype(F32) + dh.astype(F32)).astype(BF16)
        dy_v[where, :] = dy
        dyt_v[:, where] = dy.T
        return 0

    lax.fori_loop(0, tokens // FTILE, through_norm, 0)
    for at in range(AHEAD):
        kept(at).start()
    lax.fori_loop(chunks, chunks + 1, drain, 0)
    load.wait()

    def prepare_first(t, _):
        where = pl.ds(pl.multiple_of(t * FTILE, FTILE), FTILE)
        at_v[:, where] = normed(a_v[where, :]).T
        return 0

    lax.fori_loop(0, tokens // FTILE, prepare_first, 0)
    lax.fori_loop(chunks + 1, total + 1, lambda i, _: chunk(i, False), 0)

    lax.fori_loop(total + 1, total + 4, drain, 0)

    ssall_v[me] = ss_v[...]

    def squares(i, peer):
        return pltpu.make_async_remote_copy(
            src_ref=ss_v, dst_ref=ssall_v.at[me], send_sem=ss_send.at[i], recv_sem=ss_recv.at[i],
            device_id={"dp": peer}, device_id_type=MESH_ID,
        )

    sends = [squares(i, peer) for i, peer in enumerate((right, left, opposite))]
    for copy in sends:
        copy.start()

    def finish(k, _):
        out_mine(k + chunks).wait()
        for which in range(2):
            out_shard(k + chunks, which).wait()
        return 0

    lax.fori_loop(0, chunks, finish, 0)

    def finish_pair(p, _):
        out(p).wait()
        return 0

    lax.fori_loop(0, chunks, finish_pair, 0)
    for copy in sends:
        copy.wait()
    squares_sum = ssall_v[0]
    for j in range(1, n):
        squares_sum = squares_sum + ssall_v[j]
    ss_out[...] = squares_sum


def train(n, x, dy, wg, wu, wd):
    tokens, d = x.shape
    ff = wg.shape[2]
    chunks = ff // CHUNK
    rows = 3 * d
    assert d == 2 * CHUNK and tokens % TILE == 0 and TILE // FWD * (AHEAD + 1) <= tokens // FWD
    anywhere = pl.BlockSpec(memory_space=pl.ANY)
    dma = pltpu.SemaphoreType.DMA
    return pl.pallas_call(
        functools.partial(train_kernel, n),
        out_shape=(
            jax.ShapeDtypeStruct((2 * chunks, rows, CHUNK), BF16),
            jax.ShapeDtypeStruct((chunks, rows // n // 2, CHUNK), BF16),
            jax.ShapeDtypeStruct((chunks, rows // n // 2, CHUNK), BF16),
            jax.ShapeDtypeStruct((8, CHUNK), F32),
            jax.ShapeDtypeStruct((tokens // FWD, chunks, FWD, 2 * CHUNK), F32),
        ),
        in_specs=[anywhere] * 5,
        out_specs=(anywhere, anywhere, anywhere, pl.BlockSpec(memory_space=pltpu.VMEM), anywhere),
        scratch_shapes=[
            pltpu.VMEM((tokens, d), BF16),
            pltpu.VMEM((tokens, d), BF16),
            pltpu.VMEM((d, tokens), BF16),
            pltpu.VMEM((tokens, d), BF16),
            pltpu.VMEM((d, tokens), BF16),
            pltpu.VMEM((tokens // FWD, FWD, d), F32),
            pltpu.VMEM((2, d, 2 * CHUNK), BF16),
            pltpu.VMEM((2, CHUNK, d), BF16),
            pltpu.VMEM((d, 2 * CHUNK), F32),
            pltpu.VMEM((d, CHUNK), F32),
            pltpu.VMEM((OWN, rows, CHUNK), BF16),
            pltpu.VMEM((2 * chunks, rows, CHUNK), BF16),
            pltpu.VMEM((2 * chunks, rows // n, CHUNK), BF16),
            pltpu.VMEM((8, CHUNK), F32),
            pltpu.VMEM((n, 8, CHUNK), F32),
            dma((2, tokens // FWD)),
            dma,
            dma((2 + AHEAD + 1,)),
            dma((2 + d // CHUNK, chunks)),
            dma((2, 3)),
            dma((4, 2, 2 * chunks)),
            dma((4, 2, 2 * chunks)),
            dma((3, 2 * chunks)),
            dma((3,)),
            dma((3,)),
        ],
        compiler_params=pltpu.CompilerParams(collective_id=0, has_side_effects=True, vmem_limit_bytes=VMEM_LIMIT),
        cost_estimate=pl.CostEstimate(flops=30 * tokens * d * ff, bytes_accessed=12 * tokens * d + 16 * tokens * ff + 24 * d * ff, transcendentals=3 * tokens * ff),
        name="train",
    )(x, dy, wg, wu, wd)


def update_kernel(count, sources, first, unit, me_ref, ss_ref, *refs):
    source = unit(pl.program_id(0), me_ref[0])[3]
    g_refs = []
    for parts in sources:
        g_refs.append(refs[:parts])
        refs = refs[parts:]
    w_refs, m_refs, v_refs = refs[:3], refs[3:6], refs[6:9]
    outs = refs[9:] if first else refs[18:]
    factor = jnp.minimum(1.0, 0.5 * lax.rsqrt(jnp.sum(ss_ref[...], keepdims=True) / count + 1e-30))
    pr, pd = w_refs[0].shape[1], w_refs[2].shape[3]

    def rows(halves, i, lo, hi):
        half = halves[0].shape[1]
        if hi <= half:
            return halves[0][i, lo:hi, :]
        if lo >= half:
            return halves[1][i, lo - half : hi - half, :]
        return jnp.concatenate([halves[0][i, lo:half, :], halves[1][i, 0 : hi - half, :]], 0)

    def step(which, at, g):
        g = g.astype(F32) * factor
        m = 0.9 * m_refs[which][at] + 0.1 * g
        v = 0.95 * v_refs[which][at] + 0.05 * g * g
        w = w_refs[which][at].astype(F32)
        outs[which][at] = (w - 0.02 * (m * lax.rsqrt(v + 1e-8) + 0.1 * w)).astype(BF16)
        outs[3 + which][at] = m
        outs[6 + which][at] = v

    for number, halves in enumerate(g_refs):

        @pl.when(source == number)
        def _(halves=halves):
            for i in range(halves[0].shape[0]):
                cols = slice(i * CHUNK, (i + 1) * CHUNK)
                for which in range(2):
                    step(which, (0, slice(None), cols), rows(halves, i, which * pr, (which + 1) * pr))
                for h in range(w_refs[2].shape[4] // CHUNK):
                    at = (0, i, 0, slice(None), slice(h * CHUNK, (h + 1) * CHUNK))
                    step(2, at, rows(halves, i, 2 * pr + h * pd, 2 * pr + (h + 1) * pd))


def update(n, me, units, unit, block, ss, sources, arrays, outs):
    d, ff = arrays[0].shape[1:]
    first = outs is None
    pr, pd = d // n, CHUNK // n
    count = sum(a.size for a in arrays[:3])

    def side(u, me_ref):
        layer, b, s, _, _ = unit(u, me_ref[0])
        return layer, s, b

    def down(u, me_ref):
        layer, b, s, _, _ = unit(u, me_ref[0])
        return layer, b, s, 0, 0

    def whole_g(u, me_ref):
        _, _, s, _, at = unit(u, me_ref[0])
        return at[0], s, 0

    specs = [pl.BlockSpec((1, pr, block * CHUNK), side)] * 2 + [pl.BlockSpec((1, block, 1, pd, d), down)]
    specs = specs * 3
    g_specs = []
    for i, source in enumerate(sources):
        if len(source) == 1:
            g_specs.append(pl.BlockSpec((block, source[0].shape[1] // n, CHUNK), whole_g))
        else:
            g_specs += [pl.BlockSpec((block, *a.shape[1:]), lambda u, me_ref, i=i: (unit(u, me_ref[0])[4][i], 0, 0)) for a in source]
    gs = [a for source in sources for a in source]
    size = units * 3 * pr * block * CHUNK
    return pl.pallas_call(
        functools.partial(update_kernel, count, tuple(len(source) for source in sources), first, unit),
        out_shape=tuple(jax.ShapeDtypeStruct(a.shape, a.dtype) for a in arrays),
        grid_spec=pltpu.PrefetchScalarGridSpec(
            num_scalar_prefetch=1,
            grid=(units,),
            in_specs=[pl.BlockSpec(ss.shape, lambda u, me_ref: (0, 0)), *g_specs, *specs]
            + ([] if first else [pl.BlockSpec(memory_space=pl.ANY)] * 9),
            out_specs=tuple(specs),
        ),
        input_output_aliases={} if first else {2 + len(gs) + 9 + i: i for i in range(9)},
        compiler_params=pltpu.CompilerParams(vmem_limit_bytes=VMEM_LIMIT),
        cost_estimate=pl.CostEstimate(flops=15 * size, bytes_accessed=22 * size, transcendentals=size),
        name="update",
    )(me, ss, *gs, *arrays, *([] if first else outs))


def solution(mesh):
    n = mesh.shape["dp"]
    assert n == 4

    def step(x, dy, *arrays):
        x, dy = x.reshape(x.shape[1:]), dy.reshape(dy.shape[1:])
        wg, wu, wd = arrays[:3]
        gathered, half_a, half_b, ss, _ = train(n, x, dy, wg, wu, wd)

        to_right = [(i, (i + 1) % n) for i in range(n)]
        to_left = [(i, (i + n - 1) % n) for i in range(n)]
        left_b = lax.ppermute(half_b, "dp", to_right)
        right_a = lax.ppermute(half_a, "dp", to_left)
        left_a = lax.ppermute(half_a, "dp", to_right)
        right_b = lax.ppermute(half_b, "dp", to_left)

        layers, ff, d = wd.shape
        chunks = ff // CHUNK
        cut = (layers, chunks, n, CHUNK // n, d)
        views = [a.reshape(cut) if i % 3 == 2 else a for i, a in enumerate(arrays)]
        me = lax.axis_index("dp").astype(jnp.int32).reshape(1)

        blocks = chunks // 4

        def unit(u, me, blocks=blocks):
            mine = u >= blocks * n
            b = jnp.where(mine, u - blocks * n, u // n)
            return jnp.where(mine, 0, 1), b, jnp.where(mine, me, u % n), 0, (jnp.where(mine, blocks + b, b),)

        outs = update(n, me, blocks * (n + 1), unit, 4, ss, ((gathered,),), views, None)
        left_b, right_a, outs = lax.optimization_barrier((left_b, right_a, outs))
        far_b = lax.ppermute(left_b, "dp", to_right)
        far_a = lax.ppermute(right_a, "dp", to_left)

        def unit(u, me, blocks=blocks):
            on_right = u >= blocks
            b = jnp.where(on_right, u - blocks, u)
            shard = (me + jnp.where(on_right, 1, n - 1)) % n
            return 0, b, shard, jnp.where(on_right, 1, 0), (jnp.where(on_right, blocks - 1, b), jnp.where(on_right, b, 0))

        outs = update(n, me, 2 * blocks, unit, 4, ss, ((left_a, left_b), (right_a, right_b)), views, outs)

        def unit(u, me):
            return 0, u, (me + 2) % n, 0, (u,)

        outs = update(n, me, chunks // 2, unit, 2, ss, ((far_a, far_b),), views, outs)
        return tuple(o.reshape(a.shape) for o, a in zip(outs, arrays, strict=True))

    return jax.shard_map(
        step,
        mesh=mesh,
        in_specs=(P(("rep", "dp"), None, None),) * 2 + (P(None, None, None),) * 9,
        out_specs=(P("rep", None, None),) * 9,
        check_vma=False,
    )
```

```python
import functools

import jax
import jax.numpy as jnp
from jax import lax
from jax.experimental import pallas as pl
from jax.experimental.pallas import tpu as pltpu
from jax.sharding import PartitionSpec as P

F32, BF16 = jnp.float32, jnp.bfloat16
CHUNK = 256
TILE = 1024
FWD = 256
FTILE = 512
AHEAD = 3
OWN = 4
VMEM_LIMIT = 67_043_328
MESH_ID = pl.DeviceIdType.MESH


def dot(a, b):
    return jnp.dot(a, b, preferred_element_type=F32)


def dot_t(a, b):
    return lax.dot_general(a, b, (((1,), (1,)), ((), ())), preferred_element_type=F32)


def sigmoid(x):
    return 0.5 * jnp.tanh(0.5 * x) + 0.5


def scale_of(wide):
    return lax.rsqrt(jnp.mean(wide * wide, -1, keepdims=True) + 1e-6)


def normed(h):
    wide = h.astype(F32)
    return (wide * scale_of(wide)).astype(BF16)


def train_kernel(n, x_hbm, dy_hbm, wg_hbm, wu_hbm, wd_hbm, g_out, sa_out, sb_out, ss_out, kept_hbm,
                 h_v, a_v, at_v, dy_v, dyt_v, da_v, w_v, wd_v, gu_v, gd_v, own_v, all_v, left_v, ss_v, ssall_v,
                 in_sem, again_sem, kept_sem, keep_sem, first_sem, w_sem, send_sem, recv_sem, out_sem, ss_send, ss_recv):
    tokens, d = h_v.shape
    chunks = wg_hbm.shape[2] // CHUNK
    total = 2 * chunks
    rows = own_v.shape[1]
    shard, half = rows // n, rows // n // 2
    pr, pd = d // n, CHUNK // n
    me = lax.axis_index("dp")
    right, left, opposite = lax.rem(me + 1, n), lax.rem(me + n - 1, n), lax.rem(me + 2, n)

    barrier = pltpu.get_barrier_semaphore()
    for peer in (left, right, opposite):
        pl.semaphore_signal(barrier, inc=1, device_id={"dp": peer}, device_id_type=MESH_ID)
    pl.semaphore_wait(barrier, 3)

    def part(j, which=None):
        if which is None:
            return pl.ds(pl.multiple_of(j * shard, half), shard)
        return pl.ds(pl.multiple_of(j * shard + which * half, half), half)

    def weights(k):
        layer, c, slot = 1 - k // chunks, lax.rem(k, chunks), lax.rem(k, 2)
        cols = pl.ds(pl.multiple_of(c * CHUNK, CHUNK), CHUNK)
        return (
            pltpu.make_async_copy(wg_hbm.at[layer, :, cols], w_v.at[slot, :, pl.ds(0, CHUNK)], w_sem.at[slot, 0]),
            pltpu.make_async_copy(wu_hbm.at[layer, :, cols], w_v.at[slot, :, pl.ds(CHUNK, CHUNK)], w_sem.at[slot, 1]),
            pltpu.make_async_copy(wd_hbm.at[layer, cols, :], wd_v.at[slot], w_sem.at[slot, 2]),
        )

    def remote(kind, way, k, src, dst):
        return pltpu.make_async_remote_copy(
            src_ref=src, dst_ref=dst, send_sem=send_sem.at[kind, way, k], recv_sem=recv_sem.at[kind, way, k],
            device_id={"dp": (left, right)[way]}, device_id_type=MESH_ID,
        )

    def first(way, k):
        where = part(opposite, way)
        return remote(0, way, k, own_v.at[lax.rem(k, OWN), where], all_v.at[k, where])

    def second(way, k):
        where = part((left, right)[way])
        return remote(1, way, k, own_v.at[lax.rem(k, OWN), where], all_v.at[k, where] if way == 0 else left_v.at[k])

    def third(way, k):
        return remote(2, way, k, all_v.at[k, part(me)], all_v.at[k, part(me)])

    def fourth(way, k):
        where = part((right, left)[way], way)
        return remote(3, way, k, all_v.at[k, where], all_v.at[k, where])

    def out(k):
        return pltpu.make_async_copy(all_v.at[k], g_out.at[k], out_sem.at[0, k])

    def out_mine(k):
        return pltpu.make_async_copy(all_v.at[k, part(me)], g_out.at[k, part(me)], out_sem.at[0, k])

    def out_shard(k, which):
        return pltpu.make_async_copy(all_v.at[k, part(me, which)], (sa_out, sb_out)[which].at[k - chunks], out_sem.at[1 + which, k])

    def chunk_at(i):
        return jnp.where(i > chunks, i - 1, i)

    def alive(i):
        return (i >= 0) & (i <= total) & (i != chunks)

    def gather_at(i):
        return chunk_at(i - lag), alive(i - lag) & (i - lag < chunks)

    lag = 2

    def exchange(i):
        @pl.when(alive(i - 1))
        def _():
            q = chunk_at(i - 1)
            slot = lax.rem(q, OWN)
            for way in range(2):
                first(way, q).wait_recv()
            for j, which in ((left, 0), (right, 1)):
                where = part(j, which)
                own_v[slot, where, :] = (own_v[slot, where, :].astype(F32) + all_v[q, where, :].astype(F32)).astype(BF16)

        @pl.when(alive(i))
        def _():
            for way in range(2):
                first(way, chunk_at(i)).start()

        @pl.when(alive(i - lag))
        def _():
            q = chunk_at(i - lag)
            slot = lax.rem(q, OWN)
            for way in range(2):
                second(way, q).wait_recv()
            mine = part(me)
            g = own_v[slot, mine, :].astype(F32) + all_v[q, mine, :].astype(F32) + left_v[q].astype(F32)
            g = g.astype(BF16)
            all_v[q, mine, :] = g
            wide = g.astype(F32)
            ss_v[...] += jnp.sum((wide * wide).reshape(shard // 8, 8, CHUNK), 0)

        @pl.when(alive(i - 1))
        def _():
            for way in range(2):
                second(way, chunk_at(i - 1)).start()

        g2, go2 = gather_at(i - 2)

        @pl.when(go2)
        def _():
            for way in range(2):
                third(way, g2).wait_recv()
            for way in range(2):
                fourth(way, g2).start()

        g1, go1 = gather_at(i)

        @pl.when(go1)
        def _():
            for way in range(2):
                third(way, g1).start()

        @pl.when(alive(i - lag) & (chunk_at(i - lag) >= chunks))
        def _():
            q = chunk_at(i - lag)
            for which in range(2):
                out_shard(q, which).start()
            out_mine(q).start()

        @pl.when(alive(i - 3))
        def _():
            for way in range(2):
                first(way, chunk_at(i - 3)).wait_send()
                second(way, chunk_at(i - 3)).wait_send()

        g3, go3 = gather_at(i - 4)

        @pl.when(go3)
        def _():
            for way in range(2):
                third(way, g3).wait_send()
                fourth(way, g3).wait_send()
                fourth(way, g3).wait_recv()
            out(g3).start()

    tiles, per = tokens // TILE, TILE // FWD

    def keep(t, c):
        slot = lax.rem(t, 2)
        return pltpu.make_async_copy(da_v.at[pl.ds(slot * chunks + c, 2)], kept_hbm.at[t, pl.ds(c, 2)], keep_sem.at[slot, c // 2])

    def kept(at):
        slot = lax.rem(at, AHEAD + 1)
        where = pl.ds(lax.rem(at, tiles) * per, per)
        return pltpu.make_async_copy(kept_hbm.at[where, at // tiles], da_v.at[pl.ds(slot * per, per)], kept_sem.at[slot])

    def chunk(i, last_layer):
        k = i if last_layer else i - 1
        slot = lax.rem(k, 2)

        @pl.when(k + 1 < total)
        def _():
            for copy in weights(k + 1):
                copy.start()

        for copy in weights(k):
            copy.wait()
        gu_v[...] = jnp.zeros_like(gu_v)
        gd_v[...] = jnp.zeros_like(gd_v)

        def tile(t, _):
            where = pl.ds(pl.multiple_of(t * TILE, TILE), TILE)
            if last_layer:
                w = w_v[slot]
                both = dot(a_v[where, :], w)
            else:
                at = (k - chunks) * tiles + t

                @pl.when(at + AHEAD < chunks * tiles)
                def _():
                    kept(at + AHEAD).start()

                kept(at).wait()
                both = da_v[pl.ds(lax.rem(at, AHEAD + 1) * per, per)].reshape(TILE, 2 * CHUNK)
            dp = dot_t(dy_v[where, :], wd_v[slot]).astype(BF16).astype(F32)
            gate, up = both[:, :CHUNK], both[:, CHUNK:]
            s = sigmoid(gate)
            act = gate * s
            p = (act * up).astype(BF16)
            gd_v[...] += dot(dyt_v[:, where], p)
            dgate = (dp * up * (s + act * (1.0 - s))).astype(BF16)
            dup = (dp * act).astype(BF16)
            dboth = jnp.concatenate([dgate, dup], 1)
            gu_v[...] += dot(at_v[:, where], dboth)
            if last_layer:
                da_v[pl.ds(t * per, per)] += dot_t(dboth, w).reshape(per, FWD, d)
            return 0

        lax.fori_loop(0, tokens // TILE, tile, 0)
        o = lax.rem(k, OWN)
        down = gd_v[...].T
        for j in range(n):
            own_v[o, j * shard : j * shard + pr, :] = gu_v[j * pr : (j + 1) * pr, :CHUNK].astype(BF16)
            own_v[o, j * shard + pr : j * shard + 2 * pr, :] = gu_v[j * pr : (j + 1) * pr, CHUNK:].astype(BF16)
            for b in range(d // CHUNK):
                at = j * shard + 2 * pr + b * pd
                own_v[o, at : at + pd, :] = down[j * pd : (j + 1) * pd, b * CHUNK : (b + 1) * CHUNK].astype(BF16)
        exchange(i)
        return 0

    def drain(i, _):
        exchange(i)
        return 0

    def first_weights(c):
        cols = pl.ds(pl.multiple_of(c * CHUNK, CHUNK), CHUNK)
        held = all_v.at[chunks + c]
        copies = [
            pltpu.make_async_copy(wg_hbm.at[0, :, cols], held.at[pl.ds(0, d)], first_sem.at[0, c]),
            pltpu.make_async_copy(wu_hbm.at[0, :, cols], held.at[pl.ds(d, d)], first_sem.at[1, c]),
        ]
        for b in range(d // CHUNK):
            to = held.at[pl.ds(2 * d + b * CHUNK, CHUNK)]
            copies.append(pltpu.make_async_copy(wd_hbm.at[0, cols, pl.ds(b * CHUNK, CHUNK)], to, first_sem.at[2 + b, c]))
        return copies

    def x_tile(t):
        where = pl.ds(pl.multiple_of(t * FWD, FWD), FWD)
        return pltpu.make_async_copy(x_hbm.at[where], h_v.at[where], in_sem.at[0, t])

    def dy_tile(t):
        where = pl.ds(pl.multiple_of(t * FWD, FWD), FWD)
        return pltpu.make_async_copy(dy_hbm.at[where], dy_v.at[where], in_sem.at[1, t])

    steps = tokens // FWD
    x_tile(0).start()
    for c in range(chunks):
        for copy in first_weights(c):
            copy.start()

    def load_tiles(t, _):
        dy_tile(t).start()

        @pl.when(t > 0)
        def _():
            x_tile(t).start()

        return 0

    lax.fori_loop(0, steps, load_tiles, 0)
    for copy in weights(0):
        copy.start()
    ss_v[...] = jnp.zeros_like(ss_v)

    def tile_at(t):
        return pl.ds(pl.multiple_of(t * FWD, FWD), FWD)

    def after_forward(t):
        a = normed(h_v[tile_at(t), :])
        a_v[tile_at(t), :] = a
        at_v[:, tile_at(t)] = a.T
        dyt_v[:, tile_at(t)] = dy_v[tile_at(t), :].T

    def forward(t, _):
        after = jnp.minimum(t + 1, steps - 1)
        slot = lax.rem(t, 2) * chunks
        dy_tile(t).wait()

        @pl.when(t + 1 < steps)
        def _():
            x_tile(after).wait()

        @pl.when(t >= 2)
        def _():
            for c in range(0, chunks, 2):
                keep(t - 2, c).wait()

        a = a_v[tile_at(t), :]
        after_forward(jnp.maximum(t - 1, 0))
        a_v[tile_at(after), :] = normed(h_v[tile_at(after), :])
        sums = [None] * (d // CHUNK)
        for c in range(0, chunks, 2):
            ps = []
            for b in range(2):
                gate = dot(a, all_v[chunks + c + b, :d, :])
                up = dot(a, all_v[chunks + c + b, d : 2 * d, :])
                da_v[slot + c + b, :, :CHUNK] = gate
                da_v[slot + c + b, :, CHUNK:] = up
                ps.append((gate * sigmoid(gate) * up).astype(BF16))
            p = jnp.concatenate(ps, 1)
            for b in range(d // CHUNK):
                at = 2 * d + b * CHUNK
                term = dot(p, all_v[chunks + c : chunks + c + 2, at : at + CHUNK, :].reshape(2 * CHUNK, CHUNK))
                sums[b] = term if sums[b] is None else sums[b] + term
            keep(t, c).start()
        out = jnp.concatenate(sums, 1).astype(BF16)
        h_v[tile_at(t), :] = (h_v[tile_at(t), :].astype(F32) + out.astype(F32)).astype(BF16)
        return 0

    x_tile(0).wait()
    a_v[tile_at(0), :] = normed(h_v[tile_at(0), :])
    for c in range(chunks):
        for copy in first_weights(c):
            copy.wait()
    lax.fori_loop(0, steps, forward, 0)
    after_forward(steps - 1)
    for t in (steps - 2, steps - 1):
        for c in range(0, chunks, 2):
            keep(t, c).wait()

    def clear(t, _):
        da_v[t] = jnp.zeros((FWD, d), F32)
        return 0

    lax.fori_loop(0, steps, clear, 0)
    lax.fori_loop(0, chunks, lambda i, _: chunk(i, True), 0)

    load = pltpu.make_async_copy(x_hbm, a_v, again_sem)
    load.start()

    def through_norm(t, _):
        where = pl.ds(pl.multiple_of(t * FTILE, FTILE), FTILE)
        wide = h_v[where, :].astype(F32)
        scale = scale_of(wide)
        g = da_v[pl.ds(t * (FTILE // FWD), FTILE // FWD)].reshape(FTILE, d).astype(BF16).astype(F32)
        along = jnp.sum(g * wide, -1, keepdims=True)
        dh = (scale * g - wide * (scale * scale * scale * along * (1.0 / d))).astype(BF16)
        dy = (dy_v[where, :].astype(F32) + dh.astype(F32)).astype(BF16)
        dy_v[where, :] = dy
        dyt_v[:, where] = dy.T
        return 0

    lax.fori_loop(0, tokens // FTILE, through_norm, 0)
    for at in range(AHEAD):
        kept(at).start()
    lax.fori_loop(chunks, chunks + 1, drain, 0)
    load.wait()

    def prepare_first(t, _):
        where = pl.ds(pl.multiple_of(t * FTILE, FTILE), FTILE)
        at_v[:, where] = normed(a_v[where, :]).T
        return 0

    lax.fori_loop(0, tokens // FTILE, prepare_first, 0)
    lax.fori_loop(chunks + 1, total + 1, lambda i, _: chunk(i, False), 0)

    lax.fori_loop(total + 1, total + 4, drain, 0)

    ssall_v[me] = ss_v[...]

    def squares(i, peer):
        return pltpu.make_async_remote_copy(
            src_ref=ss_v, dst_ref=ssall_v.at[me], send_sem=ss_send.at[i], recv_sem=ss_recv.at[i],
            device_id={"dp": peer}, device_id_type=MESH_ID,
        )

    sends = [squares(i, peer) for i, peer in enumerate((right, left, opposite))]
    for copy in sends:
        copy.start()

    def finish(k, _):
        out_mine(k + chunks).wait()
        for which in range(2):
            out_shard(k + chunks, which).wait()
        return 0

    lax.fori_loop(0, chunks, finish, 0)

    def finish_pair(p, _):
        out(p).wait()
        return 0

    lax.fori_loop(0, chunks, finish_pair, 0)
    for copy in sends:
        copy.wait()
    squares_sum = ssall_v[0]
    for j in range(1, n):
        squares_sum = squares_sum + ssall_v[j]
    ss_out[...] = squares_sum


def train(n, x, dy, wg, wu, wd):
    tokens, d = x.shape
    ff = wg.shape[2]
    chunks = ff // CHUNK
    rows = 3 * d
    assert d == 2 * CHUNK and tokens % TILE == 0 and TILE // FWD * (AHEAD + 1) <= tokens // FWD
    anywhere = pl.BlockSpec(memory_space=pl.ANY)
    dma = pltpu.SemaphoreType.DMA
    return pl.pallas_call(
        functools.partial(train_kernel, n),
        out_shape=(
            jax.ShapeDtypeStruct((2 * chunks, rows, CHUNK), BF16),
            jax.ShapeDtypeStruct((chunks, rows // n // 2, CHUNK), BF16),
            jax.ShapeDtypeStruct((chunks, rows // n // 2, CHUNK), BF16),
            jax.ShapeDtypeStruct((8, CHUNK), F32),
            jax.ShapeDtypeStruct((tokens // FWD, chunks, FWD, 2 * CHUNK), F32),
        ),
        in_specs=[anywhere] * 5,
        out_specs=(anywhere, anywhere, anywhere, pl.BlockSpec(memory_space=pltpu.VMEM), anywhere),
        scratch_shapes=[
            pltpu.VMEM((tokens, d), BF16),
            pltpu.VMEM((tokens, d), BF16),
            pltpu.VMEM((d, tokens), BF16),
            pltpu.VMEM((tokens, d), BF16),
            pltpu.VMEM((d, tokens), BF16),
            pltpu.VMEM((tokens // FWD, FWD, d), F32),
            pltpu.VMEM((2, d, 2 * CHUNK), BF16),
            pltpu.VMEM((2, CHUNK, d), BF16),
            pltpu.VMEM((d, 2 * CHUNK), F32),
            pltpu.VMEM((d, CHUNK), F32),
            pltpu.VMEM((OWN, rows, CHUNK), BF16),
            pltpu.VMEM((2 * chunks, rows, CHUNK), BF16),
            pltpu.VMEM((2 * chunks, rows // n, CHUNK), BF16),
            pltpu.VMEM((8, CHUNK), F32),
            pltpu.VMEM((n, 8, CHUNK), F32),
            dma((2, tokens // FWD)),
            dma,
            dma((AHEAD + 1,)),
            dma((2, chunks // 2)),
            dma((2 + d // CHUNK, chunks)),
            dma((2, 3)),
            dma((4, 2, 2 * chunks)),
            dma((4, 2, 2 * chunks)),
            dma((3, 2 * chunks)),
            dma((3,)),
            dma((3,)),
        ],
        compiler_params=pltpu.CompilerParams(collective_id=0, has_side_effects=True, vmem_limit_bytes=VMEM_LIMIT),
        cost_estimate=pl.CostEstimate(flops=30 * tokens * d * ff, bytes_accessed=12 * tokens * d + 16 * tokens * ff + 24 * d * ff, transcendentals=3 * tokens * ff),
        name="train",
    )(x, dy, wg, wu, wd)


def update_kernel(count, sources, first, unit, me_ref, ss_ref, *refs):
    source = unit(pl.program_id(0), me_ref[0])[3]
    g_refs = []
    for parts in sources:
        g_refs.append(refs[:parts])
        refs = refs[parts:]
    w_refs, m_refs, v_refs = refs[:3], refs[3:6], refs[6:9]
    outs = refs[9:] if first else refs[18:]
    factor = jnp.minimum(1.0, 0.5 * lax.rsqrt(jnp.sum(ss_ref[...], keepdims=True) / count + 1e-30))
    pr, pd = w_refs[0].shape[1], w_refs[2].shape[3]

    def rows(halves, i, lo, hi):
        half = halves[0].shape[1]
        if hi <= half:
            return halves[0][i, lo:hi, :]
        if lo >= half:
            return halves[1][i, lo - half : hi - half, :]
        return jnp.concatenate([halves[0][i, lo:half, :], halves[1][i, 0 : hi - half, :]], 0)

    def step(which, at, g):
        g = g.astype(F32) * factor
        m = 0.9 * m_refs[which][at] + 0.1 * g
        v = 0.95 * v_refs[which][at] + 0.05 * g * g
        w = w_refs[which][at].astype(F32)
        outs[which][at] = (w - 0.02 * (m * lax.rsqrt(v + 1e-8) + 0.1 * w)).astype(BF16)
        outs[3 + which][at] = m
        outs[6 + which][at] = v

    for number, halves in enumerate(g_refs):

        @pl.when(source == number)
        def _(halves=halves):
            for i in range(halves[0].shape[0]):
                cols = slice(i * CHUNK, (i + 1) * CHUNK)
                for which in range(2):
                    step(which, (0, slice(None), cols), rows(halves, i, which * pr, (which + 1) * pr))
                for h in range(w_refs[2].shape[4] // CHUNK):
                    at = (0, i, 0, slice(None), slice(h * CHUNK, (h + 1) * CHUNK))
                    step(2, at, rows(halves, i, 2 * pr + h * pd, 2 * pr + (h + 1) * pd))


def update(n, me, units, unit, block, ss, sources, arrays, outs):
    d, ff = arrays[0].shape[1:]
    first = outs is None
    pr, pd = d // n, CHUNK // n
    count = sum(a.size for a in arrays[:3])

    def side(u, me_ref):
        layer, b, s, _, _ = unit(u, me_ref[0])
        return layer, s, b

    def down(u, me_ref):
        layer, b, s, _, _ = unit(u, me_ref[0])
        return layer, b, s, 0, 0

    def whole_g(u, me_ref):
        _, _, s, _, at = unit(u, me_ref[0])
        return at[0], s, 0

    specs = [pl.BlockSpec((1, pr, block * CHUNK), side)] * 2 + [pl.BlockSpec((1, block, 1, pd, d), down)]
    specs = specs * 3
    g_specs = []
    for i, source in enumerate(sources):
        if len(source) == 1:
            g_specs.append(pl.BlockSpec((block, source[0].shape[1] // n, CHUNK), whole_g))
        else:
            g_specs += [pl.BlockSpec((block, *a.shape[1:]), lambda u, me_ref, i=i: (unit(u, me_ref[0])[4][i], 0, 0)) for a in source]
    gs = [a for source in sources for a in source]
    size = units * 3 * pr * block * CHUNK
    return pl.pallas_call(
        functools.partial(update_kernel, count, tuple(len(source) for source in sources), first, unit),
        out_shape=tuple(jax.ShapeDtypeStruct(a.shape, a.dtype) for a in arrays),
        grid_spec=pltpu.PrefetchScalarGridSpec(
            num_scalar_prefetch=1,
            grid=(units,),
            in_specs=[pl.BlockSpec(ss.shape, lambda u, me_ref: (0, 0)), *g_specs, *specs]
            + ([] if first else [pl.BlockSpec(memory_space=pl.ANY)] * 9),
            out_specs=tuple(specs),
        ),
        input_output_aliases={} if first else {2 + len(gs) + 9 + i: i for i in range(9)},
        compiler_params=pltpu.CompilerParams(vmem_limit_bytes=VMEM_LIMIT),
        cost_estimate=pl.CostEstimate(flops=15 * size, bytes_accessed=22 * size, transcendentals=size),
        name="update",
    )(me, ss, *gs, *arrays, *([] if first else outs))


def solution(mesh):
    n = mesh.shape["dp"]
    assert n == 4

    def step(x, dy, *arrays):
        x, dy = x.reshape(x.shape[1:]), dy.reshape(dy.shape[1:])
        wg, wu, wd = arrays[:3]
        gathered, half_a, half_b, ss, _ = train(n, x, dy, wg, wu, wd)

        to_right = [(i, (i + 1) % n) for i in range(n)]
        to_left = [(i, (i + n - 1) % n) for i in range(n)]
        left_b = lax.ppermute(half_b, "dp", to_right)
        right_a = lax.ppermute(half_a, "dp", to_left)
        left_a = lax.ppermute(half_a, "dp", to_right)
        right_b = lax.ppermute(half_b, "dp", to_left)

        layers, ff, d = wd.shape
        chunks = ff // CHUNK
        cut = (layers, chunks, n, CHUNK // n, d)
        views = [a.reshape(cut) if i % 3 == 2 else a for i, a in enumerate(arrays)]
        me = lax.axis_index("dp").astype(jnp.int32).reshape(1)

        blocks = chunks // 4

        def unit(u, me, blocks=blocks):
            mine = u >= blocks * n
            b = jnp.where(mine, u - blocks * n, u // n)
            return jnp.where(mine, 0, 1), b, jnp.where(mine, me, u % n), 0, (jnp.where(mine, blocks + b, b),)

        outs = update(n, me, blocks * (n + 1), unit, 4, ss, ((gathered,),), views, None)
        left_b, right_a, outs = lax.optimization_barrier((left_b, right_a, outs))
        far_b = lax.ppermute(left_b, "dp", to_right)
        far_a = lax.ppermute(right_a, "dp", to_left)

        def unit(u, me, blocks=blocks):
            on_right = u >= blocks
            b = jnp.where(on_right, u - blocks, u)
            shard = (me + jnp.where(on_right, 1, n - 1)) % n
            return 0, b, shard, jnp.where(on_right, 1, 0), (jnp.where(on_right, blocks - 1, b), jnp.where(on_right, b, 0))

        outs = update(n, me, 2 * blocks, unit, 4, ss, ((left_a, left_b), (right_a, right_b)), views, outs)

        def unit(u, me):
            return 0, u, (me + 2) % n, 0, (u,)

        outs = update(n, me, chunks // 2, unit, 2, ss, ((far_a, far_b),), views, outs)
        return tuple(o.reshape(a.shape) for o, a in zip(outs, arrays, strict=True))

    return jax.shard_map(
        step,
        mesh=mesh,
        in_specs=(P(("rep", "dp"), None, None),) * 2 + (P(None, None, None),) * 9,
        out_specs=(P("rep", None, None),) * 9,
        check_vma=False,
    )
```

```python
import functools

import jax
import jax.numpy as jnp
from jax import lax
from jax.experimental import pallas as pl
from jax.experimental.pallas import tpu as pltpu
from jax.sharding import PartitionSpec as P

F32, BF16 = jnp.float32, jnp.bfloat16
CHUNK = 256
TILE = 1024
FWD = 256
FTILE = 512
AHEAD = 3
LATER = (0, 0, 0, 0, 0, 2, 2, 5)
OWN = 4
VMEM_LIMIT = 67_043_328
MESH_ID = pl.DeviceIdType.MESH


def dot(a, b):
    return jnp.dot(a, b, preferred_element_type=F32)


def dot_t(a, b):
    return lax.dot_general(a, b, (((1,), (1,)), ((), ())), preferred_element_type=F32)


def sigmoid(x):
    return 0.5 * jnp.tanh(0.5 * x) + 0.5


def scale_of(wide):
    return lax.rsqrt(jnp.mean(wide * wide, -1, keepdims=True) + 1e-6)


def normed(h):
    wide = h.astype(F32)
    return (wide * scale_of(wide)).astype(BF16)


def train_kernel(n, x_hbm, dy_hbm, wg_hbm, wu_hbm, wd_hbm, g_out, sa_out, sb_out, ss_out, kept_hbm,
                 h_v, a_v, at_v, dy_v, dyt_v, da_v, w_v, wd_v, gu_v, gd_v, own_v, all_v, left_v, ss_v, ssall_v,
                 in_sem, again_sem, kept_sem, keep_sem, first_sem, w_sem, send_sem, recv_sem, out_sem, ss_send, ss_recv):
    tokens, d = h_v.shape
    chunks = wg_hbm.shape[2] // CHUNK
    total = 2 * chunks
    rows = own_v.shape[1]
    shard, half = rows // n, rows // n // 2
    pr, pd = d // n, CHUNK // n
    me = lax.axis_index("dp")
    right, left, opposite = lax.rem(me + 1, n), lax.rem(me + n - 1, n), lax.rem(me + 2, n)

    barrier = pltpu.get_barrier_semaphore()
    for peer in (left, right, opposite):
        pl.semaphore_signal(barrier, inc=1, device_id={"dp": peer}, device_id_type=MESH_ID)
    pl.semaphore_wait(barrier, 3)

    def part(j, which=None):
        if which is None:
            return pl.ds(pl.multiple_of(j * shard, half), shard)
        return pl.ds(pl.multiple_of(j * shard + which * half, half), half)

    def weights(k):
        layer, c, slot = 1 - k // chunks, lax.rem(k, chunks), lax.rem(k, 2)
        cols = pl.ds(pl.multiple_of(c * CHUNK, CHUNK), CHUNK)
        return (
            pltpu.make_async_copy(wg_hbm.at[layer, :, cols], w_v.at[slot, :, pl.ds(0, CHUNK)], w_sem.at[slot, 0]),
            pltpu.make_async_copy(wu_hbm.at[layer, :, cols], w_v.at[slot, :, pl.ds(CHUNK, CHUNK)], w_sem.at[slot, 1]),
            pltpu.make_async_copy(wd_hbm.at[layer, cols, :], wd_v.at[slot], w_sem.at[slot, 2]),
        )

    def remote(kind, way, k, src, dst):
        return pltpu.make_async_remote_copy(
            src_ref=src, dst_ref=dst, send_sem=send_sem.at[kind, way, k], recv_sem=recv_sem.at[kind, way, k],
            device_id={"dp": (left, right)[way]}, device_id_type=MESH_ID,
        )

    def first(way, k):
        where = part(opposite, way)
        return remote(0, way, k, own_v.at[lax.rem(k, OWN), where], all_v.at[k, where])

    def second(way, k):
        where = part((left, right)[way])
        return remote(1, way, k, own_v.at[lax.rem(k, OWN), where], all_v.at[k, where] if way == 0 else left_v.at[k])

    def third(way, k):
        return remote(2, way, k, all_v.at[k, part(me)], all_v.at[k, part(me)])

    def fourth(way, k):
        where = part((right, left)[way], way)
        return remote(3, way, k, all_v.at[k, where], all_v.at[k, where])

    def out(k):
        return pltpu.make_async_copy(all_v.at[k], g_out.at[k], out_sem.at[0, k])

    def out_mine(k):
        return pltpu.make_async_copy(all_v.at[k, part(me)], g_out.at[k, part(me)], out_sem.at[0, k])

    def out_shard(k, which):
        return pltpu.make_async_copy(all_v.at[k, part(me, which)], (sa_out, sb_out)[which].at[k - chunks], out_sem.at[1 + which, k])

    def chunk_at(i):
        return jnp.where(i > chunks, i - 1, i)

    def alive(i):
        return (i >= 0) & (i <= total) & (i != chunks)

    def gather_at(i):
        k, found = 0, False
        for q in range(chunks):
            here = i == q + lag + LATER[q]
            k, found = k + jnp.where(here, q, 0), here | found
        return k, found

    lag = 2

    def exchange(i):
        @pl.when(alive(i - 1))
        def _():
            q = chunk_at(i - 1)
            slot = lax.rem(q, OWN)
            for way in range(2):
                first(way, q).wait_recv()
            for j, which in ((left, 0), (right, 1)):
                where = part(j, which)
                own_v[slot, where, :] = (own_v[slot, where, :].astype(F32) + all_v[q, where, :].astype(F32)).astype(BF16)

        @pl.when(alive(i))
        def _():
            for way in range(2):
                first(way, chunk_at(i)).start()

        @pl.when(alive(i - lag))
        def _():
            q = chunk_at(i - lag)
            slot = lax.rem(q, OWN)
            for way in range(2):
                second(way, q).wait_recv()
            mine = part(me)
            g = own_v[slot, mine, :].astype(F32) + all_v[q, mine, :].astype(F32) + left_v[q].astype(F32)
            g = g.astype(BF16)
            all_v[q, mine, :] = g
            wide = g.astype(F32)
            ss_v[...] += jnp.sum((wide * wide).reshape(shard // 8, 8, CHUNK), 0)

        @pl.when(alive(i - 1))
        def _():
            for way in range(2):
                second(way, chunk_at(i - 1)).start()

        g2, go2 = gather_at(i - 2)

        @pl.when(go2)
        def _():
            for way in range(2):
                third(way, g2).wait_recv()
            for way in range(2):
                fourth(way, g2).start()

        g1, go1 = gather_at(i)

        @pl.when(go1)
        def _():
            for way in range(2):
                third(way, g1).start()

        @pl.when(alive(i - lag) & (chunk_at(i - lag) >= chunks))
        def _():
            q = chunk_at(i - lag)
            for which in range(2):
                out_shard(q, which).start()
            out_mine(q).start()

        @pl.when(alive(i - 3))
        def _():
            for way in range(2):
                first(way, chunk_at(i - 3)).wait_send()
                second(way, chunk_at(i - 3)).wait_send()

        g3, go3 = gather_at(i - 4)

        @pl.when(go3)
        def _():
            for way in range(2):
                third(way, g3).wait_send()
                fourth(way, g3).wait_send()
                fourth(way, g3).wait_recv()
            out(g3).start()

    tiles, per = tokens // TILE, TILE // FWD

    def keep(t, c):
        slot = lax.rem(t, 2)
        return pltpu.make_async_copy(da_v.at[pl.ds(slot * chunks + c, 2)], kept_hbm.at[t, pl.ds(c, 2)], keep_sem.at[slot, c // 2])

    def kept(at):
        slot = lax.rem(at, AHEAD + 1)
        where = pl.ds(lax.rem(at, tiles) * per, per)
        return pltpu.make_async_copy(kept_hbm.at[where, at // tiles], da_v.at[pl.ds(slot * per, per)], kept_sem.at[slot])

    def chunk(i, last_layer):
        k = i if last_layer else i - 1
        slot = lax.rem(k, 2)

        @pl.when(k + 1 < total)
        def _():
            for copy in weights(k + 1):
                copy.start()

        for copy in weights(k):
            copy.wait()
        gu_v[...] = jnp.zeros_like(gu_v)
        gd_v[...] = jnp.zeros_like(gd_v)

        def tile(t, _):
            where = pl.ds(pl.multiple_of(t * TILE, TILE), TILE)
            if last_layer:
                w = w_v[slot]
                both = dot(a_v[where, :], w)
            else:
                at = (k - chunks) * tiles + t

                @pl.when(at + AHEAD < chunks * tiles)
                def _():
                    kept(at + AHEAD).start()

                kept(at).wait()
                both = da_v[pl.ds(lax.rem(at, AHEAD + 1) * per, per)].reshape(TILE, 2 * CHUNK)
            dp = dot_t(dy_v[where, :], wd_v[slot]).astype(BF16).astype(F32)
            gate, up = both[:, :CHUNK], both[:, CHUNK:]
            s = sigmoid(gate)
            act = gate * s
            p = (act * up).astype(BF16)
            gd_v[...] += dot(dyt_v[:, where], p)
            dgate = (dp * up * (s + act * (1.0 - s))).astype(BF16)
            dup = (dp * act).astype(BF16)
            dboth = jnp.concatenate([dgate, dup], 1)
            gu_v[...] += dot(at_v[:, where], dboth)
            if last_layer:
                da_v[pl.ds(t * per, per)] += dot_t(dboth, w).reshape(per, FWD, d)
            return 0

        lax.fori_loop(0, tokens // TILE, tile, 0)
        o = lax.rem(k, OWN)
        down = gd_v[...].T
        for j in range(n):
            own_v[o, j * shard : j * shard + pr, :] = gu_v[j * pr : (j + 1) * pr, :CHUNK].astype(BF16)
            own_v[o, j * shard + pr : j * shard + 2 * pr, :] = gu_v[j * pr : (j + 1) * pr, CHUNK:].astype(BF16)
            for b in range(d // CHUNK):
                at = j * shard + 2 * pr + b * pd
                own_v[o, at : at + pd, :] = down[j * pd : (j + 1) * pd, b * CHUNK : (b + 1) * CHUNK].astype(BF16)
        exchange(i)
        return 0

    def drain(i, _):
        exchange(i)
        return 0

    def first_weights(c):
        cols = pl.ds(pl.multiple_of(c * CHUNK, CHUNK), CHUNK)
        held = all_v.at[chunks + c]
        copies = [
            pltpu.make_async_copy(wg_hbm.at[0, :, cols], held.at[pl.ds(0, d)], first_sem.at[0, c]),
            pltpu.make_async_copy(wu_hbm.at[0, :, cols], held.at[pl.ds(d, d)], first_sem.at[1, c]),
        ]
        for b in range(d // CHUNK):
            to = held.at[pl.ds(2 * d + b * CHUNK, CHUNK)]
            copies.append(pltpu.make_async_copy(wd_hbm.at[0, cols, pl.ds(b * CHUNK, CHUNK)], to, first_sem.at[2 + b, c]))
        return copies

    def x_tile(t):
        where = pl.ds(pl.multiple_of(t * FWD, FWD), FWD)
        return pltpu.make_async_copy(x_hbm.at[where], h_v.at[where], in_sem.at[0, t])

    def dy_tile(t):
        where = pl.ds(pl.multiple_of(t * FWD, FWD), FWD)
        return pltpu.make_async_copy(dy_hbm.at[where], dy_v.at[where], in_sem.at[1, t])

    steps = tokens // FWD
    x_tile(0).start()
    for c in range(chunks):
        for copy in first_weights(c):
            copy.start()

    def load_tiles(t, _):
        dy_tile(t).start()

        @pl.when(t > 0)
        def _():
            x_tile(t).start()

        return 0

    lax.fori_loop(0, steps, load_tiles, 0)
    for copy in weights(0):
        copy.start()
    ss_v[...] = jnp.zeros_like(ss_v)

    def tile_at(t):
        return pl.ds(pl.multiple_of(t * FWD, FWD), FWD)

    def after_forward(t):
        a = normed(h_v[tile_at(t), :])
        a_v[tile_at(t), :] = a
        at_v[:, tile_at(t)] = a.T
        dyt_v[:, tile_at(t)] = dy_v[tile_at(t), :].T

    def forward(t, _):
        after = jnp.minimum(t + 1, steps - 1)
        slot = lax.rem(t, 2) * chunks
        dy_tile(t).wait()

        @pl.when(t + 1 < steps)
        def _():
            x_tile(after).wait()

        @pl.when(t >= 2)
        def _():
            for c in range(0, chunks, 2):
                keep(t - 2, c).wait()

        a = a_v[tile_at(t), :]
        after_forward(jnp.maximum(t - 1, 0))
        a_v[tile_at(after), :] = normed(h_v[tile_at(after), :])
        sums = [None] * (d // CHUNK)
        for c in range(0, chunks, 2):
            ps = []
            for b in range(2):
                gate = dot(a, all_v[chunks + c + b, :d, :])
                up = dot(a, all_v[chunks + c + b, d : 2 * d, :])
                da_v[slot + c + b, :, :CHUNK] = gate
                da_v[slot + c + b, :, CHUNK:] = up
                ps.append((gate * sigmoid(gate) * up).astype(BF16))
            p = jnp.concatenate(ps, 1)
            for b in range(d // CHUNK):
                at = 2 * d + b * CHUNK
                term = dot(p, all_v[chunks + c : chunks + c + 2, at : at + CHUNK, :].reshape(2 * CHUNK, CHUNK))
                sums[b] = term if sums[b] is None else sums[b] + term
            keep(t, c).start()
        out = jnp.concatenate(sums, 1).astype(BF16)
        h_v[tile_at(t), :] = (h_v[tile_at(t), :].astype(F32) + out.astype(F32)).astype(BF16)
        return 0

    x_tile(0).wait()
    a_v[tile_at(0), :] = normed(h_v[tile_at(0), :])
    for c in range(chunks):
        for copy in first_weights(c):
            copy.wait()
    lax.fori_loop(0, steps, forward, 0)
    after_forward(steps - 1)
    for t in (steps - 2, steps - 1):
        for c in range(0, chunks, 2):
            keep(t, c).wait()

    def clear(t, _):
        da_v[t] = jnp.zeros((FWD, d), F32)
        return 0

    lax.fori_loop(0, steps, clear, 0)
    lax.fori_loop(0, chunks, lambda i, _: chunk(i, True), 0)

    load = pltpu.make_async_copy(x_hbm, a_v, again_sem)
    load.start()

    def through_norm(t, _):
        where = pl.ds(pl.multiple_of(t * FTILE, FTILE), FTILE)
        wide = h_v[where, :].astype(F32)
        scale = scale_of(wide)
        g = da_v[pl.ds(t * (FTILE // FWD), FTILE // FWD)].reshape(FTILE, d).astype(BF16).astype(F32)
        along = jnp.sum(g * wide, -1, keepdims=True)
        dh = (scale * g - wide * (scale * scale * scale * along * (1.0 / d))).astype(BF16)
        dy = (dy_v[where, :].astype(F32) + dh.astype(F32)).astype(BF16)
        dy_v[where, :] = dy
        dyt_v[:, where] = dy.T
        return 0

    lax.fori_loop(0, tokens // FTILE, through_norm, 0)
    for at in range(AHEAD):
        kept(at).start()
    lax.fori_loop(chunks, chunks + 1, drain, 0)
    load.wait()

    def prepare_first(t, _):
        where = pl.ds(pl.multiple_of(t * FTILE, FTILE), FTILE)
        at_v[:, where] = normed(a_v[where, :]).T
        return 0

    lax.fori_loop(0, tokens // FTILE, prepare_first, 0)
    lax.fori_loop(chunks + 1, total + 1, lambda i, _: chunk(i, False), 0)

    lax.fori_loop(total + 1, total + 4, drain, 0)

    ssall_v[me] = ss_v[...]

    def squares(i, peer):
        return pltpu.make_async_remote_copy(
            src_ref=ss_v, dst_ref=ssall_v.at[me], send_sem=ss_send.at[i], recv_sem=ss_recv.at[i],
            device_id={"dp": peer}, device_id_type=MESH_ID,
        )

    sends = [squares(i, peer) for i, peer in enumerate((right, left, opposite))]
    for copy in sends:
        copy.start()

    def finish(k, _):
        out_mine(k + chunks).wait()
        for which in range(2):
            out_shard(k + chunks, which).wait()
        return 0

    lax.fori_loop(0, chunks, finish, 0)

    def finish_pair(p, _):
        out(p).wait()
        return 0

    lax.fori_loop(0, chunks, finish_pair, 0)
    for copy in sends:
        copy.wait()
    squares_sum = ssall_v[0]
    for j in range(1, n):
        squares_sum = squares_sum + ssall_v[j]
    ss_out[...] = squares_sum


def train(n, x, dy, wg, wu, wd):
    tokens, d = x.shape
    ff = wg.shape[2]
    chunks = ff // CHUNK
    rows = 3 * d
    assert d == 2 * CHUNK and tokens % TILE == 0 and TILE // FWD * (AHEAD + 1) <= tokens // FWD
    anywhere = pl.BlockSpec(memory_space=pl.ANY)
    dma = pltpu.SemaphoreType.DMA
    return pl.pallas_call(
        functools.partial(train_kernel, n),
        out_shape=(
            jax.ShapeDtypeStruct((2 * chunks, rows, CHUNK), BF16),
            jax.ShapeDtypeStruct((chunks, rows // n // 2, CHUNK), BF16),
            jax.ShapeDtypeStruct((chunks, rows // n // 2, CHUNK), BF16),
            jax.ShapeDtypeStruct((8, CHUNK), F32),
            jax.ShapeDtypeStruct((tokens // FWD, chunks, FWD, 2 * CHUNK), F32),
        ),
        in_specs=[anywhere] * 5,
        out_specs=(anywhere, anywhere, anywhere, pl.BlockSpec(memory_space=pltpu.VMEM), anywhere),
        scratch_shapes=[
            pltpu.VMEM((tokens, d), BF16),
            pltpu.VMEM((tokens, d), BF16),
            pltpu.VMEM((d, tokens), BF16),
            pltpu.VMEM((tokens, d), BF16),
            pltpu.VMEM((d, tokens), BF16),
            pltpu.VMEM((tokens // FWD, FWD, d), F32),
            pltpu.VMEM((2, d, 2 * CHUNK), BF16),
            pltpu.VMEM((2, CHUNK, d), BF16),
            pltpu.VMEM((d, 2 * CHUNK), F32),
            pltpu.VMEM((d, CHUNK), F32),
            pltpu.VMEM((OWN, rows, CHUNK), BF16),
            pltpu.VMEM((2 * chunks, rows, CHUNK), BF16),
            pltpu.VMEM((2 * chunks, rows // n, CHUNK), BF16),
            pltpu.VMEM((8, CHUNK), F32),
            pltpu.VMEM((n, 8, CHUNK), F32),
            dma((2, tokens // FWD)),
            dma,
            dma((AHEAD + 1,)),
            dma((2, chunks // 2)),
            dma((2 + d // CHUNK, chunks)),
            dma((2, 3)),
            dma((4, 2, 2 * chunks)),
            dma((4, 2, 2 * chunks)),
            dma((3, 2 * chunks)),
            dma((3,)),
            dma((3,)),
        ],
        compiler_params=pltpu.CompilerParams(collective_id=0, has_side_effects=True, vmem_limit_bytes=VMEM_LIMIT),
        cost_estimate=pl.CostEstimate(flops=30 * tokens * d * ff, bytes_accessed=12 * tokens * d + 16 * tokens * ff + 24 * d * ff, transcendentals=3 * tokens * ff),
        name="train",
    )(x, dy, wg, wu, wd)


def update_kernel(count, sources, first, unit, me_ref, ss_ref, *refs):
    source = unit(pl.program_id(0), me_ref[0])[3]
    g_refs = []
    for parts in sources:
        g_refs.append(refs[:parts])
        refs = refs[parts:]
    w_refs, m_refs, v_refs = refs[:3], refs[3:6], refs[6:9]
    outs = refs[9:] if first else refs[18:]
    factor = jnp.minimum(1.0, 0.5 * lax.rsqrt(jnp.sum(ss_ref[...], keepdims=True) / count + 1e-30))
    pr, pd = w_refs[0].shape[1], w_refs[2].shape[3]

    def rows(halves, i, lo, hi):
        half = halves[0].shape[1]
        if hi <= half:
            return halves[0][i, lo:hi, :]
        if lo >= half:
            return halves[1][i, lo - half : hi - half, :]
        return jnp.concatenate([halves[0][i, lo:half, :], halves[1][i, 0 : hi - half, :]], 0)

    def step(which, at, g):
        g = g.astype(F32) * factor
        m = 0.9 * m_refs[which][at] + 0.1 * g
        v = 0.95 * v_refs[which][at] + 0.05 * g * g
        w = w_refs[which][at].astype(F32)
        outs[which][at] = (w - 0.02 * (m * lax.rsqrt(v + 1e-8) + 0.1 * w)).astype(BF16)
        outs[3 + which][at] = m
        outs[6 + which][at] = v

    for number, halves in enumerate(g_refs):

        @pl.when(source == number)
        def _(halves=halves):
            for i in range(halves[0].shape[0]):
                cols = slice(i * CHUNK, (i + 1) * CHUNK)
                for which in range(2):
                    step(which, (0, slice(None), cols), rows(halves, i, which * pr, (which + 1) * pr))
                for h in range(w_refs[2].shape[4] // CHUNK):
                    at = (0, i, 0, slice(None), slice(h * CHUNK, (h + 1) * CHUNK))
                    step(2, at, rows(halves, i, 2 * pr + h * pd, 2 * pr + (h + 1) * pd))


def update(n, me, units, unit, block, ss, sources, arrays, outs):
    d, ff = arrays[0].shape[1:]
    first = outs is None
    pr, pd = d // n, CHUNK // n
    count = sum(a.size for a in arrays[:3])

    def side(u, me_ref):
        layer, b, s, _, _ = unit(u, me_ref[0])
        return layer, s, b

    def down(u, me_ref):
        layer, b, s, _, _ = unit(u, me_ref[0])
        return layer, b, s, 0, 0

    def whole_g(u, me_ref):
        _, _, s, _, at = unit(u, me_ref[0])
        return at[0], s, 0

    specs = [pl.BlockSpec((1, pr, block * CHUNK), side)] * 2 + [pl.BlockSpec((1, block, 1, pd, d), down)]
    specs = specs * 3
    g_specs = []
    for i, source in enumerate(sources):
        if len(source) == 1:
            g_specs.append(pl.BlockSpec((block, source[0].shape[1] // n, CHUNK), whole_g))
        else:
            g_specs += [pl.BlockSpec((block, *a.shape[1:]), lambda u, me_ref, i=i: (unit(u, me_ref[0])[4][i], 0, 0)) for a in source]
    gs = [a for source in sources for a in source]
    size = units * 3 * pr * block * CHUNK
    return pl.pallas_call(
        functools.partial(update_kernel, count, tuple(len(source) for source in sources), first, unit),
        out_shape=tuple(jax.ShapeDtypeStruct(a.shape, a.dtype) for a in arrays),
        grid_spec=pltpu.PrefetchScalarGridSpec(
            num_scalar_prefetch=1,
            grid=(units,),
            in_specs=[pl.BlockSpec(ss.shape, lambda u, me_ref: (0, 0)), *g_specs, *specs]
            + ([] if first else [pl.BlockSpec(memory_space=pl.ANY)] * 9),
            out_specs=tuple(specs),
        ),
        input_output_aliases={} if first else {2 + len(gs) + 9 + i: i for i in range(9)},
        compiler_params=pltpu.CompilerParams(vmem_limit_bytes=VMEM_LIMIT),
        cost_estimate=pl.CostEstimate(flops=15 * size, bytes_accessed=22 * size, transcendentals=size),
        name="update",
    )(me, ss, *gs, *arrays, *([] if first else outs))


def solution(mesh):
    n = mesh.shape["dp"]
    assert n == 4

    def step(x, dy, *arrays):
        x, dy = x.reshape(x.shape[1:]), dy.reshape(dy.shape[1:])
        wg, wu, wd = arrays[:3]
        gathered, half_a, half_b, ss, _ = train(n, x, dy, wg, wu, wd)

        to_right = [(i, (i + 1) % n) for i in range(n)]
        to_left = [(i, (i + n - 1) % n) for i in range(n)]
        left_b = lax.ppermute(half_b, "dp", to_right)
        right_a = lax.ppermute(half_a, "dp", to_left)
        left_a = lax.ppermute(half_a, "dp", to_right)
        right_b = lax.ppermute(half_b, "dp", to_left)

        layers, ff, d = wd.shape
        chunks = ff // CHUNK
        cut = (layers, chunks, n, CHUNK // n, d)
        views = [a.reshape(cut) if i % 3 == 2 else a for i, a in enumerate(arrays)]
        me = lax.axis_index("dp").astype(jnp.int32).reshape(1)

        blocks = chunks // 4

        def unit(u, me, blocks=blocks):
            mine = u >= blocks * n
            b = jnp.where(mine, u - blocks * n, u // n)
            return jnp.where(mine, 0, 1), b, jnp.where(mine, me, u % n), 0, (jnp.where(mine, blocks + b, b),)

        outs = update(n, me, blocks * (n + 1), unit, 4, ss, ((gathered,),), views, None)
        left_b, right_a, outs = lax.optimization_barrier((left_b, right_a, outs))
        far_b = lax.ppermute(left_b, "dp", to_right)
        far_a = lax.ppermute(right_a, "dp", to_left)

        def unit(u, me, blocks=blocks):
            on_right = u >= blocks
            b = jnp.where(on_right, u - blocks, u)
            shard = (me + jnp.where(on_right, 1, n - 1)) % n
            return 0, b, shard, jnp.where(on_right, 1, 0), (jnp.where(on_right, blocks - 1, b), jnp.where(on_right, b, 0))

        outs = update(n, me, 2 * blocks, unit, 4, ss, ((left_a, left_b), (right_a, right_b)), views, outs)

        def unit(u, me):
            return 0, u, (me + 2) % n, 0, (u,)

        outs = update(n, me, chunks // 2, unit, 2, ss, ((far_a, far_b),), views, outs)
        return tuple(o.reshape(a.shape) for o, a in zip(outs, arrays, strict=True))

    return jax.shard_map(
        step,
        mesh=mesh,
        in_specs=(P(("rep", "dp"), None, None),) * 2 + (P(None, None, None),) * 9,
        out_specs=(P("rep", None, None),) * 9,
        check_vma=False,
    )
```
